32 devices in a mesh: dp: 2 (over x), tp: 4 (over z), sp: 4 (over y, core).
Axes of the slice: x: 2, y: 2, z: 4, core: 2. Of those that a mesh axis runs over, the one named last changes fastest.
Arguments:
- hidden: bfloat16 [4, 128, 2048], P(None, 'dp'), parts along dimension 1
- start_pos: int32 [128], P('dp'), parts along dimension 0
- k_cache: bfloat16 [128, 1024, 8, 128], P('dp', 'sp', 'tp'), parts along dimension 0
- v_cache: bfloat16 [128, 1024, 8, 128], P('dp', 'sp', 'tp'), parts along dimension 0
- w_q: bfloat16 [2048, 2048], P(None, 'tp')
- w_k: bfloat16 [2048, 1024], P(None, 'tp')
- w_v: bfloat16 [2048, 1024], P(None, 'tp')
- w_o: bfloat16 [2048, 2048], P('tp')
- w_gate: bfloat16 [2048, 6144], P(None, 'tp')
- w_up: bfloat16 [2048, 6144], P(None, 'tp')
- w_down: bfloat16 [6144, 2048], P('tp')
- attn_norm: bfloat16 [2048], replicated
- mlp_norm: bfloat16 [2048], replicated
- q_gain: bfloat16 [128], replicated
- k_gain: bfloat16 [128], replicated
Outputs:
- output 1: bfloat16 [4, 128, 2048], P(None, 'dp'), parts along dimension 1
- output 2: bfloat16 [128, 1024, 8, 128], P('dp', 'sp', 'tp'), parts along dimension 0
- output 3: bfloat16 [128, 1024, 8, 128], P('dp', 'sp', 'tp'), parts along dimension 0
There are 2 independent parts. The reference program is written for one: setup_inputs(seed, part) draws one part's arguments, and reference() takes and returns one part's arrays. A program takes and returns all parts, laid end to end along the dimension named above; an argument that names none is the same for every part.
All inputs are finite; a program needn't handle non-finite values.
Results may differ from the reference program's by a relative error of at most 0.00853494.
Values sent between devices are 32-bit elements.
A program may use at most 1 GiB of HBM per device.

```python
import math
import jax
import jax.numpy as jnp
from jax import lax

D_MODEL = 2048
HEADS = 16
KV_HEADS = 8
FFN_DIM = 6144
HEAD_DIM = 128
STEPS = 4
BATCH = 64
SEQ_DEV = 256
SEQ_LEN = 1024
ROPE_BASE = 1000000.0
NORM_EPS = 1e-06


def rms_scale(values, gain_vec):
    wide_vals = values.astype(jnp.float32)
    inv_rms = lax.rsqrt(jnp.mean(wide_vals * wide_vals, axis=-1, keepdims=True) + NORM_EPS)
    return wide_vals * inv_rms * gain_vec.astype(jnp.float32)


def apply_rope(vector, tok_pos):
    head_dim = vector.shape[-1]
    half_dim = head_dim // 2
    freqs = ROPE_BASE ** (-(jnp.arange(half_dim, dtype=jnp.float32) * (2.0 / head_dim)))
    angles = tok_pos.astype(jnp.float32)[:, None] * freqs[None, :]
    cos_tab = jnp.cos(angles)[:, None, :]
    sin_tab = jnp.sin(angles)[:, None, :]
    lower_half = vector[..., :half_dim]
    upper_half = vector[..., half_dim:]
    return jnp.concatenate([lower_half * cos_tab - upper_half * sin_tab, upper_half * cos_tab + lower_half * sin_tab], axis=-1)


def setup_inputs(seed: int = 0, part: int = 0) -> dict:
    w_keys = jax.random.split(jax.random.key(seed), 11)
    part_keys = jax.random.split(jax.random.fold_in(jax.random.key(seed + 1), part), 5)
    q_width = HEADS * HEAD_DIM
    kv_width = KV_HEADS * HEAD_DIM
    q_scale = math.sqrt(math.log(SEQ_LEN / 16.0))
    k_scale = math.sqrt(2.0 * math.log(SEQ_LEN)) / 1.5

    def normal_draw(key_in, shape, scale):
        return (jax.random.normal(key_in, shape, jnp.float32) * scale).astype(jnp.bfloat16)

    def gain_draw(key_in, shape, scale):
        return (scale * (1.0 + 0.2 * jax.random.normal(key_in, shape, jnp.float32))).astype(jnp.bfloat16)

    drawn_pos = jax.random.randint(part_keys[1], (BATCH,), SEQ_DEV, SEQ_LEN - STEPS + 1, dtype=jnp.int32)
    order = jax.random.permutation(part_keys[2], BATCH)
    start_pos = drawn_pos.at[order[0]].set(SEQ_LEN - STEPS).at[order[1]].set(SEQ_DEV)
    filled = (jnp.arange(SEQ_LEN)[None, :] < start_pos[:, None])[:, :, None, None]
    cache_shape = (BATCH, SEQ_LEN, KV_HEADS, HEAD_DIM)
    k_cache = jnp.where(filled, jax.random.normal(part_keys[3], cache_shape, jnp.float32), 0.0).astype(jnp.bfloat16)
    v_cache = jnp.where(filled, jax.random.normal(part_keys[4], cache_shape, jnp.float32), 0.0).astype(jnp.bfloat16)
    return {
        'hidden': normal_draw(part_keys[0], (STEPS, BATCH, D_MODEL), 1.0),
        'start_pos': start_pos,
        'k_cache': k_cache,
        'v_cache': v_cache,
        'w_q': normal_draw(w_keys[0], (D_MODEL, q_width), D_MODEL ** -0.5),
        'w_k': normal_draw(w_keys[1], (D_MODEL, kv_width), D_MODEL ** -0.5),
        'w_v': normal_draw(w_keys[2], (D_MODEL, kv_width), D_MODEL ** -0.5),
        'w_o': normal_draw(w_keys[3], (q_width, D_MODEL), 2.0 * q_width ** -0.5),
        'w_gate': normal_draw(w_keys[4], (D_MODEL, FFN_DIM), D_MODEL ** -0.5),
        'w_up': normal_draw(w_keys[5], (D_MODEL, FFN_DIM), D_MODEL ** -0.5),
        'w_down': normal_draw(w_keys[6], (FFN_DIM, D_MODEL), FFN_DIM ** -0.5),
        'attn_norm': gain_draw(w_keys[7], (D_MODEL,), 1.0),
        'mlp_norm': gain_draw(w_keys[8], (D_MODEL,), 1.0),
        'q_gain': gain_draw(w_keys[9], (HEAD_DIM,), q_scale),
        'k_gain': gain_draw(w_keys[10], (HEAD_DIM,), k_scale),
    }


def reference(hidden, start_pos, k_cache, v_cache, w_q, w_k, w_v, w_o, w_gate, w_up, w_down, attn_norm, mlp_norm, q_gain, k_gain):
    groups = HEADS // KV_HEADS
    score_scale = HEAD_DIM ** -0.5
    seq_pos = jnp.arange(SEQ_LEN)

    def attend_one(request):
        q_one, k_one, v_one, pos_one = request
        scores = jnp.einsum('kgh,lkh->kgl', q_one.astype(jnp.float32), k_one.astype(jnp.float32)) * score_scale
        scores = jnp.where(seq_pos <= pos_one, scores, -jnp.inf)
        probs = jax.nn.softmax(scores, axis=-1)
        return jnp.einsum('kgl,lkh->kgh', probs, v_one.astype(jnp.float32))

    def decode_step(caches, step_in):
        k_all, v_all = caches
        x_tok, step_idx = step_in
        tok_pos = start_pos + step_idx
        normed = rms_scale(x_tok, attn_norm).astype(jnp.bfloat16)
        q_raw = jnp.dot(normed, w_q, preferred_element_type=jnp.float32).reshape(BATCH, HEADS, HEAD_DIM)
        k_raw = jnp.dot(normed, w_k, preferred_element_type=jnp.float32).reshape(BATCH, KV_HEADS, HEAD_DIM)
        v_new = jnp.dot(normed, w_v, preferred_element_type=jnp.float32).astype(jnp.bfloat16).reshape(BATCH, KV_HEADS, HEAD_DIM)
        q_rot = apply_rope(rms_scale(q_raw, q_gain), tok_pos).astype(jnp.bfloat16).reshape(BATCH, KV_HEADS, groups, HEAD_DIM)
        k_new = apply_rope(rms_scale(k_raw, k_gain), tok_pos).astype(jnp.bfloat16)
        hit = (seq_pos[None, :] == tok_pos[:, None])[:, :, None, None]
        k_all = jnp.where(hit, k_new[:, None], k_all)
        v_all = jnp.where(hit, v_new[:, None], v_all)
        attn_vals = lax.map(attend_one, (q_rot, k_all, v_all, tok_pos))
        attn_in = attn_vals.reshape(BATCH, HEADS * HEAD_DIM).astype(jnp.bfloat16)
        attn_out = jnp.dot(attn_in, w_o, preferred_element_type=jnp.float32)
        residual = (x_tok.astype(jnp.float32) + attn_out).astype(jnp.bfloat16)
        mlp_in = rms_scale(residual, mlp_norm).astype(jnp.bfloat16)
        gate_act = jnp.dot(mlp_in, w_gate, preferred_element_type=jnp.float32)
        up_proj = jnp.dot(mlp_in, w_up, preferred_element_type=jnp.float32)
        mlp_act = (jax.nn.silu(gate_act) * up_proj).astype(jnp.bfloat16)
        down_out = jnp.dot(mlp_act, w_down, preferred_element_type=jnp.float32)
        out_tok = (residual.astype(jnp.float32) + down_out).astype(jnp.bfloat16)
        return (k_all, v_all), out_tok

    final_caches, outputs = lax.scan(decode_step, (k_cache, v_cache), (hidden, jnp.arange(STEPS)))
    return outputs, final_caches[0], final_caches[1]
```

```python
import jax
import jax.numpy as jnp
from jax import lax
from jax.sharding import PartitionSpec as P

ROPE_BASE = 1000000.0
NORM_EPS = 1e-06
NEG_BIG = -1e30


def rms_scale(values, gain_vec):
    wide_vals = values.astype(jnp.float32)
    inv_rms = lax.rsqrt(jnp.mean(wide_vals * wide_vals, axis=-1, keepdims=True) + NORM_EPS)
    return wide_vals * inv_rms * gain_vec.astype(jnp.float32)


def apply_rope(vector, tok_pos):
    head_dim = vector.shape[-1]
    half_dim = head_dim // 2
    freqs = ROPE_BASE ** (-(jnp.arange(half_dim, dtype=jnp.float32) * (2.0 / head_dim)))
    angles = tok_pos.astype(jnp.float32)[:, None] * freqs[None, :]
    cos_tab = jnp.cos(angles)[:, None, :]
    sin_tab = jnp.sin(angles)[:, None, :]
    lower_half = vector[..., :half_dim]
    upper_half = vector[..., half_dim:]
    return jnp.concatenate([lower_half * cos_tab - upper_half * sin_tab, upper_half * cos_tab + lower_half * sin_tab], axis=-1)


def solution(mesh):
    cache_spec = P('dp', 'sp', 'tp', None)
    col_spec = P(None, 'tp')
    row_spec = P('tp', None)
    in_specs = (P(None, 'dp', None), P('dp'), cache_spec, cache_spec, col_spec, col_spec, col_spec, row_spec,
                col_spec, col_spec, row_spec, P(), P(), P(), P())
    out_specs = (P(None, 'dp', None), cache_spec, cache_spec)

    def shard_body(hidden, start_pos, k_cache, v_cache, w_q, w_k, w_v, w_o, w_gate, w_up, w_down, attn_norm, mlp_norm, q_gain, k_gain):
        n_steps, n_batch = hidden.shape[0], hidden.shape[1]
        seq_blk, kv_loc, head_dim = k_cache.shape[1], k_cache.shape[2], k_cache.shape[3]
        heads_loc = w_q.shape[1] // head_dim
        groups = heads_loc // kv_loc
        n_tok = n_steps * n_batch
        score_scale = head_dim ** -0.5
        blk_start = lax.axis_index('sp') * seq_blk
        blk_pos = blk_start + jnp.arange(seq_blk)
        tok_pos = (start_pos[None, :] + jnp.arange(n_steps, dtype=jnp.int32)[:, None]).reshape(n_tok)
        x_tok = hidden.reshape(n_tok, hidden.shape[2])
        normed = rms_scale(x_tok, attn_norm).astype(jnp.bfloat16)
        q_raw = jnp.dot(normed, w_q, preferred_element_type=jnp.float32).reshape(n_tok, heads_loc, head_dim)
        k_raw = jnp.dot(normed, w_k, preferred_element_type=jnp.float32).reshape(n_tok, kv_loc, head_dim)
        v_new = jnp.dot(normed, w_v, preferred_element_type=jnp.float32).astype(jnp.bfloat16).reshape(n_steps, n_batch, kv_loc, head_dim)
        q_rot = apply_rope(rms_scale(q_raw, q_gain), tok_pos).astype(jnp.bfloat16).reshape(n_steps, n_batch, kv_loc, groups, head_dim)
        k_new = apply_rope(rms_scale(k_raw, k_gain), tok_pos).astype(jnp.bfloat16).reshape(n_steps, n_batch, kv_loc, head_dim)
        new_keys, new_vals = k_new, v_new
        old_mask = (blk_pos[None, :] < start_pos[:, None])[:, None, None, None, :]
        step_ids = jnp.arange(n_steps)
        owned = (start_pos[:, None] + step_ids[None, :]) // seq_blk == lax.axis_index('sp')
        new_mask = (owned[:, None, :] & (step_ids[None, :] <= step_ids[:, None])[None])[:, None, :, None, :]
        old_scores = jnp.einsum('ibkgh,bskh->bkigs', q_rot, k_cache, preferred_element_type=jnp.float32) * score_scale
        old_scores = jnp.where(old_mask, old_scores, NEG_BIG)
        new_scores = jnp.einsum('ibkgh,jbkh->bkigj', q_rot, k_new, preferred_element_type=jnp.float32) * score_scale
        new_scores = jnp.where(new_mask, new_scores, NEG_BIG)
        blk_max = jnp.maximum(old_scores.max(axis=-1), new_scores.max(axis=-1))
        old_probs = jnp.where(old_mask, jnp.exp(old_scores - blk_max[..., None]), 0.0)
        new_probs = jnp.where(new_mask, jnp.exp(new_scores - blk_max[..., None]), 0.0)
        blk_sum = old_probs.sum(axis=-1) + new_probs.sum(axis=-1)
        blk_out = (jnp.einsum('bkigs,bskh->bkigh', old_probs.astype(jnp.bfloat16), v_cache, preferred_element_type=jnp.float32)
                   + jnp.einsum('bkigj,jbkh->bkigh', new_probs.astype(jnp.bfloat16), v_new, preferred_element_type=jnp.float32))
        top_max = lax.pmax(blk_max, 'sp')
        weights = jnp.exp(blk_max - top_max)
        packed = jnp.concatenate([blk_out * weights[..., None], (blk_sum * weights)[..., None]], axis=-1)
        summed = lax.psum(packed, 'sp')
        attn_vals = summed[..., :head_dim] / summed[..., head_dim:]
        attn_in = attn_vals.transpose(2, 0, 1, 3, 4).reshape(n_tok, heads_loc * head_dim).astype(jnp.bfloat16)
        attn_out = lax.psum(jnp.dot(attn_in, w_o, preferred_element_type=jnp.float32), 'tp')
        residual = (x_tok.astype(jnp.float32) + attn_out).astype(jnp.bfloat16)
        mlp_in = rms_scale(residual, mlp_norm).astype(jnp.bfloat16)
        gate_act = jnp.dot(mlp_in, w_gate, preferred_element_type=jnp.float32)
        up_proj = jnp.dot(mlp_in, w_up, preferred_element_type=jnp.float32)
        mlp_act = (jax.nn.silu(gate_act) * up_proj).astype(jnp.bfloat16)
        down_sum = lax.psum(jnp.dot(mlp_act, w_down, preferred_element_type=jnp.float32), 'tp')
        outputs = (residual.astype(jnp.float32) + down_sum).astype(jnp.bfloat16)
        offsets = blk_pos[None, :] - start_pos[:, None]
        k_out = k_cache
        v_out = v_cache
        for step_idx in range(n_steps):
            hit = (offsets == step_idx)[:, :, None, None]
            k_out = jnp.where(hit, new_keys[step_idx][:, None], k_out)
            v_out = jnp.where(hit, new_vals[step_idx][:, None], v_out)
        return outputs.reshape(hidden.shape), k_out, v_out

    return jax.shard_map(shard_body, mesh=mesh, in_specs=in_specs, out_specs=out_specs, check_vma=False)
```

```python
import functools
import jax
import jax.numpy as jnp
import numpy as np
from jax import lax
from jax.experimental import pallas as pl
from jax.experimental.pallas import tpu as pltpu
from jax.sharding import PartitionSpec as P

ROPE_BASE = 1000000.0
NORM_EPS = 1e-06
NEG_BIG = -1e30
HEAD = 128
CHUNK = 4


def gain_row(ref):
    g = ref[...].astype(jnp.float32)
    return jnp.concatenate([g[j:j + 1] for j in range(g.shape[0])], axis=1)


def attend_kernel(start_ref, hid_hbm, wq_hbm, wk_hbm, wv_hbm, kc_hbm, vc_hbm, an_ref, qg_ref, kg_ref, freq_ref,
                  o_ref, ml_ref, ko_hbm, vo_hbm,
                  hid, wq, wk, wv, kbuf, vbuf, nrm, raw, q_s, k_s, v_s, pos_s, ml_s, key_s,
                  w_sem, h_sem, kin_sem, vin_sem, kout_sem, vout_sem):
    n_steps, n_batch, width = hid.shape
    rows = kbuf.shape[1]
    seq_blk = rows // 2
    n_chunk = n_batch // CHUNK
    n_q = wq.shape[1] // HEAD
    n_kv = wk.shape[1] // HEAD
    blk_start = lax.axis_index('sp') * seq_blk
    scale = HEAD ** -0.5

    hid_cp = pltpu.make_async_copy(hid_hbm, hid, h_sem)
    hid_cp.start()
    w_cps = [pltpu.make_async_copy(a, b, w_sem.at[j]) for j, (a, b) in enumerate(((wq_hbm, wq), (wk_hbm, wk), (wv_hbm, wv)))]
    for cp in w_cps:
        cp.start()

    def kv_in(c):
        sl = pl.ds(c * CHUNK, CHUNK)
        return (pltpu.make_async_copy(kc_hbm.at[sl], kbuf.at[sl], kin_sem.at[c]),
                pltpu.make_async_copy(vc_hbm.at[sl], vbuf.at[sl], vin_sem.at[c]))

    def kv_out(c):
        sl = pl.ds(c * CHUNK, CHUNK)
        return (pltpu.make_async_copy(kbuf.at[sl], ko_hbm.at[sl], kout_sem.at[c]),
                pltpu.make_async_copy(vbuf.at[sl], vo_hbm.at[sl], vout_sem.at[c]))

    @pl.loop(0, n_chunk)
    def _(c):
        a, b = kv_in(c)
        a.start()
        b.start()

    @pl.loop(0, n_batch)
    def _(b):
        pos_s[pl.ds(b, 1), :] = jnp.full((1, HEAD), start_ref[b].astype(jnp.float32), jnp.float32)

    freq = freq_ref[0:1, :]
    sign = freq_ref[1:2, :]
    ang = pos_s[...] * freq
    cos0 = jnp.cos(ang)
    sin0 = jnp.sin(ang)

    r_id = lax.broadcasted_iota(jnp.int32, (16, rows), 0)
    c_id = lax.broadcasted_iota(jnp.int32, (16, rows), 1)
    same = ((r_id % 4) // 2) == (c_id % 2)
    key_s[...] = jnp.where(same, c_id // 2 - r_id // 4, 1 << 20)

    hid_cp.wait()
    gain = gain_row(an_ref)
    for i in range(n_steps):
        for h in range(0, n_batch, 32):
            x = hid[i, h:h + 32, :].astype(jnp.float32)
            inv = lax.rsqrt(jnp.mean(x * x, axis=-1, keepdims=True) + NORM_EPS)
            nrm[i * n_batch + h:i * n_batch + h + 32, :] = (x * inv * gain).astype(jnp.bfloat16)

    def rope(x, g, cos, sin):
        inv = lax.rsqrt(jnp.mean(x * x, axis=-1, keepdims=True) + NORM_EPS)
        y = x * inv * g
        return y * cos + pltpu.roll(y, HEAD // 2, 1) * sin

    tabs = []
    for i in range(n_steps):
        if i == 0:
            c, s = cos0, sin0
        else:
            ci, si = jnp.cos(freq * float(i)), jnp.sin(freq * float(i))
            c, s = cos0 * ci - sin0 * si, sin0 * ci + cos0 * si
        pos_s_c, pos_s_s = c, s * sign
        tabs.append((pos_s_c, pos_s_s))

    for cp in w_cps:
        cp.wait()
    qg = qg_ref[...].astype(jnp.float32)
    kg = kg_ref[...].astype(jnp.float32)
    nq = n_q * HEAD
    nk = n_kv * HEAD
    raw[:, :nq] = jnp.dot(nrm[...], wq[...], preferred_element_type=jnp.float32)
    raw[:, nq:nq + nk] = jnp.dot(nrm[...], wk[...], preferred_element_type=jnp.float32)
    raw[:, nq + nk:] = jnp.dot(nrm[...], wv[...], preferred_element_type=jnp.float32)
    for i in range(n_steps):
        rs = slice(i * n_batch, (i + 1) * n_batch)
        cos, sin = tabs[i]
        for h in range(n_q):
            q_s[pl.ds(i * n_q + h, n_batch, stride=n_steps * n_q), :] = rope(raw[rs, h * HEAD:(h + 1) * HEAD], qg, cos, sin)
        for h in range(n_kv):
            k_s[pl.ds(i * n_kv + h, n_batch, stride=n_steps * n_kv), :] = rope(
                raw[rs, nq + h * HEAD:nq + (h + 1) * HEAD], kg, cos, sin)
            v_s[pl.ds(i * n_kv + h, n_batch, stride=n_steps * n_kv), :] = raw[rs, nq + nk + h * HEAD:nq + nk + (h + 1) * HEAD]

    row32 = lax.broadcasted_iota(jnp.int32, (32, HEAD), 0)
    eye_r = lax.broadcasted_iota(jnp.int32, (16, HEAD), 0)
    eye_c = lax.broadcasted_iota(jnp.int32, (16, HEAD), 1)
    eye_m = eye_r == eye_c
    eye_l = eye_r + 16 == eye_c
    zero24 = jnp.zeros((24, HEAD), jnp.float32)

    @pl.loop(0, n_chunk)
    def _(c):
        a, b = kv_in(c)
        a.wait()
        b.wait()
        lps = []
        for u in range(CHUNK):
            bb = c * CHUNK + u
            lp = start_ref[bb] - blk_start
            lps.append(lp)
            base = jnp.clip((lp // 8) * 8, 0, seq_blk - 16)
            rel = (lp - base) * 2
            shift = jnp.bitwise_and(rel, 31)
            hit = (row32 >= rel) & (row32 < rel + 8)
            win = pl.ds(pl.multiple_of(base * 2, 16), 32)
            for src, dst in ((k_s, kbuf), (v_s, vbuf)):
                new = src[pl.ds(pl.multiple_of(bb * 8, 8), 8), :]
                new = pltpu.roll(jnp.concatenate([new, zero24], axis=0), shift, 0)
                old = dst[bb, win, :].astype(jnp.float32)
                dst[bb, win, :] = jnp.where(hit, new, old).astype(jnp.bfloat16)
        for u in range(CHUNK):
            bb = c * CHUNK + u
            q = q_s[pl.ds(pl.multiple_of(bb * 16, 16), 16), :].astype(jnp.bfloat16)
            s = lax.dot_general(q, kbuf[bb], (((1,), (1,)), ((), ())), preferred_element_type=jnp.float32) * scale
            valid = key_s[...] <= lps[u]
            s = jnp.where(valid, s, NEG_BIG)
            m = jnp.max(s, axis=-1, keepdims=True)
            p = jnp.where(valid, jnp.exp(s - m), 0.0)
            l = jnp.sum(p, axis=-1, keepdims=True)
            o = jnp.dot(p.astype(jnp.bfloat16), vbuf[bb], preferred_element_type=jnp.float32)
            o_ref[pl.ds(bb, 16, stride=n_batch), :] = o
            ml = jnp.where(eye_m, m, 0.0) + jnp.where(eye_l, l, 0.0)
            ml_s[pl.ds(bb, 1), :] = jnp.sum(ml, axis=0, keepdims=True)
        a, b = kv_out(c)
        a.start()
        b.start()

    for i in range(n_steps):
        ml = ml_s[...]
        ml_ref[i] = ml if i == 0 else pltpu.roll(ml, HEAD - 4 * i, 1)

    @pl.loop(0, n_chunk)
    def _(c):
        a, b = kv_out(c)
        a.wait()
        b.wait()


def attend(start_pos, hidden, w_q, w_k, w_v, k_cache, v_cache, attn_norm, q_gain, k_gain):
    n_steps, n_batch, width = hidden.shape
    rows = k_cache.shape[1]
    n_chunk = n_batch // CHUNK
    nq, nk = w_q.shape[1], w_k.shape[1]
    half = HEAD // 2
    f = ROPE_BASE ** (-(np.arange(half, dtype=np.float64) * (2.0 / HEAD)))
    freq = np.stack([np.concatenate([f, f]), np.concatenate([-np.ones(half), np.ones(half)])]).astype(np.float32)
    vm = pl.BlockSpec(memory_space=pltpu.VMEM)
    anyspec = pl.BlockSpec(memory_space=pltpu.HBM)
    return pl.pallas_call(
        attend_kernel,
        name='attend',
        out_shape=(jax.ShapeDtypeStruct((16 * n_batch, HEAD), jnp.float32),
                   jax.ShapeDtypeStruct((n_steps, n_batch, HEAD), jnp.float32),
                   jax.ShapeDtypeStruct(k_cache.shape, jnp.bfloat16),
                   jax.ShapeDtypeStruct(v_cache.shape, jnp.bfloat16)),
        in_specs=[pl.BlockSpec(memory_space=pltpu.SMEM)] + [anyspec] * 6 + [vm] * 4,
        out_specs=(vm, vm, anyspec, anyspec),
        scratch_shapes=[
            pltpu.VMEM(hidden.shape, jnp.bfloat16),
            pltpu.VMEM(w_q.shape, jnp.bfloat16),
            pltpu.VMEM(w_k.shape, jnp.bfloat16),
            pltpu.VMEM(w_v.shape, jnp.bfloat16),
            pltpu.VMEM(k_cache.shape, jnp.bfloat16),
            pltpu.VMEM(v_cache.shape, jnp.bfloat16),
            pltpu.VMEM((n_steps * n_batch, width), jnp.bfloat16),
            pltpu.VMEM((n_steps * n_batch, nq + 2 * nk), jnp.float32),
            pltpu.VMEM((n_batch * 16, HEAD), jnp.float32),
            pltpu.VMEM((n_batch * 8, HEAD), jnp.float32),
            pltpu.VMEM((n_batch * 8, HEAD), jnp.float32),
            pltpu.VMEM((n_batch, HEAD), jnp.float32),
            pltpu.VMEM((n_batch, HEAD), jnp.float32),
            pltpu.VMEM((16, rows), jnp.int32),
            pltpu.SemaphoreType.DMA((3,)),
            pltpu.SemaphoreType.DMA,
            pltpu.SemaphoreType.DMA((n_chunk,)),
            pltpu.SemaphoreType.DMA((n_chunk,)),
            pltpu.SemaphoreType.DMA((n_chunk,)),
            pltpu.SemaphoreType.DMA((n_chunk,)),
        ],
        compiler_params=pltpu.CompilerParams(vmem_limit_bytes=67043328),
        cost_estimate=pl.CostEstimate(flops=2 * 10 ** 9, bytes_accessed=40 * 10 ** 6, transcendentals=10 ** 6),
    )(start_pos, hidden, w_q, w_k, w_v, k_cache, v_cache, attn_norm.reshape(-1, HEAD), q_gain.reshape(1, -1), k_gain.reshape(1, -1), jnp.asarray(freq))


N_COL = 8
N_HALF = 2
LAG = 3
LAG_Y = 3


def layer_kernel(o_hbm, ml_hbm, hid_hbm, wo_hbm, wg_hbm, wu_hbm, wd_hbm, mn_ref, out_ref,
                 o_own, ml_own, oa, mla, om, mlm, oy, mly, own, ml_mine, attn, hid, wo, wg, wu, wd,
                 p1, e1, x1, r1, m_s, act, p2, e2, x2, ob, yb, pb, pf,
                 ld_sem, w_sem, a1_snd, a1_rcv, a2_snd, a2_rcv, es1, er1, xs1, xr1, ts1, tr1,
                 es2, er2, xs2, xr2, ts2, tr2, ps, pr, ys, yr, fs, fr):
    n_steps, n_batch, width = hid_hbm.shape
    n_half = n_batch // N_HALF
    n_col = width // N_COL
    n_piece = N_COL * N_HALF
    tp = lax.axis_index('tp')
    sp = lax.axis_index('sp')
    core = sp % 2
    row = sp // 2
    partner = {'sp': row * 2 + 1 - core}
    across = {'sp': (1 - row) * 2 + core}
    is_mid = (tp % 3) != 0
    is_end = (tp % 3) == 0
    to_mid = {'tp': (tp + 3) // 3}
    to_end = {'tp': (tp - 1) * 3}
    to_other = {'tp': 3 - tp}
    mesh_id = pl.DeviceIdType.MESH

    def remote(src, dst, ssem, rsem, dev):
        return pltpu.make_async_remote_copy(src_ref=src, dst_ref=dst, send_sem=ssem, recv_sem=rsem, device_id=dev, device_id_type=mesh_id)

    lds = [pltpu.make_async_copy(o_hbm, o_own, ld_sem.at[0]), pltpu.make_async_copy(ml_hbm, ml_own, ld_sem.at[1]),
           pltpu.make_async_copy(hid_hbm.at[sp], hid, ld_sem.at[2])]
    wts = [pltpu.make_async_copy(a, b, w_sem.at[j]) for j, (a, b) in enumerate(((wo_hbm, wo), (wg_hbm, wg), (wu_hbm, wu), (wd_hbm, wd)))]
    for cp in lds + wts:
        cp.start()

    barrier = pltpu.get_barrier_semaphore()
    for dev in (partner, across):
        pl.semaphore_signal(barrier, inc=1, device_id=dev, device_id_type=mesh_id)

    @pl.when(is_mid)
    def _():
        pl.semaphore_signal(barrier, inc=1, device_id=to_end, device_id_type=mesh_id)
        pl.semaphore_signal(barrier, inc=1, device_id=to_other, device_id_type=mesh_id)
        pl.semaphore_wait(barrier, 4)

    @pl.when(is_end)
    def _():
        pl.semaphore_signal(barrier, inc=1, device_id=to_mid, device_id_type=mesh_id)
        pl.semaphore_wait(barrier, 3)

    for cp in lds:
        cp.wait()
    a1 = []
    for q, jy in enumerate((1 - row, row)):
        step = jy * 2 + 1 - core
        a1.append((remote(ml_own.at[step], mla.at[q], a1_snd.at[2 * q], a1_rcv.at[2 * q], partner),
                   remote(o_own.at[pl.ds(step * 4, 4)], oa.at[q], a1_snd.at[2 * q + 1], a1_rcv.at[2 * q + 1], partner)))
        for cp in a1[-1]:
            cp.start()

    lane = lax.broadcasted_iota(jnp.int32, (n_half, HEAD), 1)

    def weigh(ma, mb):
        top = jnp.maximum(ma, mb)
        wa, wb = jnp.exp(ma - top), jnp.exp(mb - top)
        tot = pltpu.roll(ma, HEAD - 16, 1) * wa + pltpu.roll(mb, HEAD - 16, 1) * wb
        return top, wa, wb, tot

    def merge_core(q, step, dst, mldst):
        for cp in a1[q]:
            cp.wait()
        for h in range(N_HALF):
            rs = pl.ds(h * n_half, n_half)
            top, wa, wb, tot = weigh(ml_own[step, rs, :], mla[q, rs, :])
            mldst[h] = jnp.where(lane < 16, top, pltpu.roll(tot, 16, 1))
            for k in range(4):
                dst[h, k] = o_own[step * 4 + k, rs, :] * wa[:, k:k + 1] + oa[q, k, rs, :] * wb[:, k:k + 1]

    merge_core(0, (1 - row) * 2 + core, om, mlm)
    a2 = []
    for h in range(N_HALF):
        a2.append((remote(mlm.at[h], mly.at[h], a2_snd.at[2 * h], a2_rcv.at[2 * h], across),
                   remote(om.at[h], oy.at[h], a2_snd.at[2 * h + 1], a2_rcv.at[2 * h + 1], across)))
        for cp in a2[-1]:
            cp.start()
    merge_core(1, row * 2 + core, own, ml_mine)
    wts[0].wait()

    e1_cp = lambda t: remote(p1.at[t], e1.at[t], es1.at[t], er1.at[t], to_mid)
    x1_cp = lambda t: remote(p1.at[t], x1.at[t], xs1.at[t], xr1.at[t], to_other)
    t1_cp = lambda t: remote(r1.at[t], r1.at[t], ts1.at[t], tr1.at[t], to_end)
    e2_cp = lambda t: remote(p2.at[t], e2.at[t], es2.at[t], er2.at[t], to_mid)
    x2_cp = lambda t: remote(p2.at[t], x2.at[t], xs2.at[t], xr2.at[t], to_other)
    t2_cp = lambda t: remote(ob.at[t], ob.at[t], ts2.at[t], tr2.at[t], to_end)
    p_cp = lambda t: remote(ob.at[t], pb.at[t], ps.at[t], pr.at[t], partner)
    y_cp = lambda t: remote(ob.at[t], yb.at[t], ys.at[t], yr.at[t], across)
    f_cp = lambda t: remote(yb.at[t], pf.at[t], fs.at[t], fr.at[t], partner)

    for h in range(N_HALF):
        for cp in a2[h]:
            cp.wait()
        _, wa, wb, tot = weigh(ml_mine[h], mly[h])
        inv = 1.0 / tot
        for k in range(4):
            val = (own[h, k] * wa[:, k:k + 1] + oy[h, k] * wb[:, k:k + 1]) * inv[:, k:k + 1]
            attn[h, :, k * HEAD:(k + 1) * HEAD] = val.astype(jnp.bfloat16)

        @pl.loop(0, N_COL)
        def _(n):
            cs = pl.ds(pl.multiple_of(n * n_col, n_col), n_col)
            t = h * N_COL + n
            p1[t] = jnp.dot(attn[h], wo[:, cs], preferred_element_type=jnp.float32)

            @pl.when(is_end)
            def _():
                e1_cp(t).start()

    @pl.when(is_mid)
    def _():
        @pl.loop(0, n_piece + LAG)
        def _(s):
            @pl.when(s < n_piece)
            def _():
                e1_cp(s).wait_recv()
                p1[s] = p1[s] + e1[s]
                x1_cp(s).start()

            @pl.when(s >= LAG)
            def _():
                t = s - LAG
                h = t // N_COL
                rs = pl.ds(pl.multiple_of(h * n_half, n_half), n_half)
                cs = pl.ds(pl.multiple_of((t - h * N_COL) * n_col, n_col), n_col)
                x1_cp(t).wait_recv()
                r = hid[rs, cs].astype(jnp.float32) + (p1[t] + x1[t])
                r1[t] = r.astype(jnp.bfloat16).astype(jnp.float32)
                t1_cp(t).start()

    @pl.when(is_end)
    def _():
        @pl.loop(0, n_piece)
        def _(t):
            t1_cp(t).wait_recv()

    gain = gain_row(mn_ref)
    for h in range(N_HALF):
        sq = jnp.zeros((n_half, 1), jnp.float32)
        for n in range(N_COL):
            r = r1[h * N_COL + n]
            sq = sq + jnp.sum(r * r, axis=-1, keepdims=True)
        inv = lax.rsqrt(sq / width + NORM_EPS)
        for n in range(N_COL):
            m_s[h * n_half:(h + 1) * n_half, n * n_col:(n + 1) * n_col] = (
                r1[h * N_COL + n] * inv * gain[:, n * n_col:(n + 1) * n_col]).astype(jnp.bfloat16)

    wts[1].wait()
    wts[2].wait()
    ffn = wg.shape[1]
    blk = 512
    for n in range(ffn // blk):
        cs = slice(n * blk, (n + 1) * blk)
        g = jnp.dot(m_s[...], wg[:, cs], preferred_element_type=jnp.float32)
        u = jnp.dot(m_s[...], wu[:, cs], preferred_element_type=jnp.float32)
        act[:, cs] = (jax.nn.silu(g) * u).astype(jnp.bfloat16)

    wts[3].wait()

    @pl.loop(0, N_COL)
    def _(n):
        cs = pl.ds(pl.multiple_of(n * n_col, n_col), n_col)
        d = jnp.dot(act[...], wd[:, cs], preferred_element_type=jnp.float32)
        for h in range(N_HALF):
            t = n * N_HALF + h
            p2[t] = d[h * n_half:(h + 1) * n_half]

            @pl.when(is_end)
            def _():
                e2_cp(t).start()

    def share(t):
        p_cp(t).start()
        y_cp(t).start()

    def relay(t):
        y_cp(t).wait_recv()
        f_cp(t).start()

    @pl.when(is_mid)
    def _():
        @pl.loop(0, n_piece + LAG + LAG_Y)
        def _(s):
            @pl.when(s < n_piece)
            def _():
                e2_cp(s).wait_recv()
                p2[s] = p2[s] + e2[s]
                x2_cp(s).start()

            @pl.when((s >= LAG) & (s < n_piece + LAG))
            def _():
                t = s - LAG
                n = t // N_HALF
                h = t - n * N_HALF
                x2_cp(t).wait_recv()
                o = r1[h * N_COL + n] + (p2[t] + x2[t])
                ob[t] = o.astype(jnp.bfloat16).astype(jnp.float32)
                t2_cp(t).start()
                share(t)

            @pl.when(s >= LAG + LAG_Y)
            def _():
                relay(s - LAG - LAG_Y)

    @pl.when(is_end)
    def _():
        @pl.loop(0, n_piece + LAG_Y)
        def _(s):
            @pl.when(s < n_piece)
            def _():
                t2_cp(s).wait_recv()
                share(s)

            @pl.when(s >= LAG_Y)
            def _():
                relay(s - LAG_Y)

    @pl.loop(0, n_piece)
    def _(t):
        n = t // N_HALF
        rs = pl.ds(pl.multiple_of((t - n * N_HALF) * n_half, n_half), n_half)
        cs = pl.ds(pl.multiple_of(n * n_col, n_col), n_col)
        out_ref[sp, rs, cs] = ob[t].astype(jnp.bfloat16)
        out_ref[(1 - row) * 2 + core, rs, cs] = yb[t].astype(jnp.bfloat16)
        p_cp(t).wait_recv()
        out_ref[row * 2 + 1 - core, rs, cs] = pb[t].astype(jnp.bfloat16)
        f_cp(t).wait_recv()
        out_ref[(1 - row) * 2 + 1 - core, rs, cs] = pf[t].astype(jnp.bfloat16)
        p_cp(t).wait_send()
        y_cp(t).wait_send()
        f_cp(t).wait_send()

        @pl.when(is_mid)
        def _():
            x1_cp(t).wait_send()
            t1_cp(t).wait_send()
            x2_cp(t).wait_send()
            t2_cp(t).wait_send()

        @pl.when(is_end)
        def _():
            e1_cp(t).wait_send()
            e2_cp(t).wait_send()


def layer(o, ml, hidden, w_o, w_gate, w_up, w_down, mlp_norm):
    n_steps, n_batch, width = hidden.shape
    n_half = n_batch // N_HALF
    n_col = width // N_COL
    n_piece = N_COL * N_HALF
    vm = pl.BlockSpec(memory_space=pltpu.VMEM)
    anyspec = pl.BlockSpec(memory_space=pltpu.HBM)
    f32, bf16 = jnp.float32, jnp.bfloat16
    piece = pltpu.VMEM((n_piece, n_half, n_col), f32)
    dma = pltpu.SemaphoreType.DMA
    return pl.pallas_call(
        layer_kernel,
        name='layer',
        out_shape=jax.ShapeDtypeStruct(hidden.shape, bf16),
        in_specs=[anyspec] * 7 + [vm],
        out_specs=vm,
        scratch_shapes=[
            pltpu.VMEM((16, n_batch, HEAD), f32),
            pltpu.VMEM((4, n_batch, HEAD), f32),
            pltpu.VMEM((2, 4, n_batch, HEAD), f32),
            pltpu.VMEM((2, n_batch, HEAD), f32),
            pltpu.VMEM((N_HALF, 4, n_half, HEAD), f32),
            pltpu.VMEM((N_HALF, n_half, HEAD), f32),
            pltpu.VMEM((N_HALF, 4, n_half, HEAD), f32),
            pltpu.VMEM((N_HALF, n_half, HEAD), f32),
            pltpu.VMEM((N_HALF, 4, n_half, HEAD), f32),
            pltpu.VMEM((N_HALF, n_half, HEAD), f32),
            pltpu.VMEM((N_HALF, n_half, 4 * HEAD), bf16),
            pltpu.VMEM((n_batch, width), bf16),
            pltpu.VMEM(w_o.shape, bf16),
            pltpu.VMEM(w_gate.shape, bf16),
            pltpu.VMEM(w_up.shape, bf16),
            pltpu.VMEM(w_down.shape, bf16),
            piece, piece, piece, piece,
            pltpu.VMEM((n_batch, width), bf16),
            pltpu.VMEM((n_batch, w_gate.shape[1]), bf16),
            piece, piece, piece, piece, piece, piece, piece,
            dma((3,)), dma((4,)), dma((4,)), dma((4,)), dma((2 * N_HALF,)), dma((2 * N_HALF,)),
        ] + [dma((n_piece,))] * 18,
        compiler_params=pltpu.CompilerParams(collective_id=0, has_side_effects=True, vmem_limit_bytes=67043328),
        cost_estimate=pl.CostEstimate(flops=2 * 10 ** 9, bytes_accessed=30 * 10 ** 6, transcendentals=10 ** 6),
    )(o.reshape(16, n_batch, HEAD), ml, hidden, w_o, w_gate, w_up, w_down, mlp_norm.reshape(-1, HEAD))


def solution(mesh):
    cache_spec = P('dp', 'sp', 'tp', None)
    col_spec = P(None, 'tp')
    row_spec = P('tp', None)
    in_specs = (P(None, 'dp', None), P('dp'), cache_spec, cache_spec, col_spec, col_spec, col_spec, row_spec,
                col_spec, col_spec, row_spec, P(), P(), P(), P())
    out_specs = (P(None, 'dp', None), cache_spec, cache_spec)

    def shard_body(hidden, start_pos, k_cache, v_cache, w_q, w_k, w_v, w_o, w_gate, w_up, w_down, attn_norm, mlp_norm, q_gain, k_gain):
        flat = (k_cache.shape[0], k_cache.shape[1] * k_cache.shape[2], k_cache.shape[3])
        o, ml, k_out, v_out = attend(start_pos, hidden, w_q, w_k, w_v, k_cache.reshape(flat), v_cache.reshape(flat), attn_norm, q_gain, k_gain)
        out = layer(o, ml, hidden, w_o, w_gate, w_up, w_down, mlp_norm)
        return out, k_out.reshape(k_cache.shape), v_out.reshape(v_cache.shape)

    return jax.shard_map(shard_body, mesh=mesh, in_specs=in_specs, out_specs=out_specs, check_vma=False)
```

```python
import functools
import jax
import jax.numpy as jnp
import numpy as np
from jax import lax
from jax.experimental import pallas as pl
from jax.experimental.pallas import tpu as pltpu
from jax.sharding import PartitionSpec as P

ROPE_BASE = 1000000.0
NORM_EPS = 1e-06
NEG_BIG = -1e30
HEAD = 128
CHUNK = 8


def gain_row(ref):
    g = ref[...].astype(jnp.float32)
    return jnp.concatenate([g[j:j + 1] for j in range(g.shape[0])], axis=1)


def attend_kernel(start_ref, hid_hbm, wq_hbm, wk_hbm, wv_hbm, kc_hbm, vc_hbm, an_ref, qg_ref, kg_ref, freq_ref,
                  o_ref, ml_ref, ko_hbm, vo_hbm,
                  hid, wq, wk, wv, kbuf, vbuf, nrm, raw, q_s, k_s, v_s, pos_s, ml_s, key_s, sc_s, pr_s,
                  w_sem, h_sem, kin_sem, vin_sem, kout_sem, vout_sem):
    n_steps, n_batch, width = hid.shape
    rows = kbuf.shape[1]
    seq_blk = rows // 2
    n_chunk = n_batch // CHUNK
    n_q = wq.shape[1] // HEAD
    n_kv = wk.shape[1] // HEAD
    blk_start = lax.axis_index('sp') * seq_blk
    scale = HEAD ** -0.5

    hid_cp = pltpu.make_async_copy(hid_hbm, hid, h_sem)
    hid_cp.start()
    w_cps = [pltpu.make_async_copy(a, b, w_sem.at[j]) for j, (a, b) in enumerate(((wq_hbm, wq), (wk_hbm, wk), (wv_hbm, wv)))]
    for cp in w_cps:
        cp.start()

    def kv_in(c):
        sl = pl.ds(c * CHUNK, CHUNK)
        return (pltpu.make_async_copy(kc_hbm.at[sl], kbuf.at[sl], kin_sem.at[c]),
                pltpu.make_async_copy(vc_hbm.at[sl], vbuf.at[sl], vin_sem.at[c]))

    def kv_out(c):
        sl = pl.ds(c * CHUNK, CHUNK)
        return (pltpu.make_async_copy(kbuf.at[sl], ko_hbm.at[sl], kout_sem.at[c]),
                pltpu.make_async_copy(vbuf.at[sl], vo_hbm.at[sl], vout_sem.at[c]))

    @pl.loop(0, n_chunk)
    def _(c):
        a, b = kv_in(c)
        a.start()
        b.start()

    @pl.loop(0, n_batch)
    def _(b):
        pos_s[pl.ds(b, 1), :] = jnp.full((1, HEAD), start_ref[b].astype(jnp.float32), jnp.float32)

    freq = freq_ref[0:1, :]
    sign = freq_ref[1:2, :]
    ang = pos_s[...] * freq
    cos0 = jnp.cos(ang)
    sin0 = jnp.sin(ang)

    r_id = lax.broadcasted_iota(jnp.int32, (16, rows), 0)
    c_id = lax.broadcasted_iota(jnp.int32, (16, rows), 1)
    same = ((r_id % 4) // 2) == (c_id % 2)
    key_s[...] = jnp.where(same, c_id // 2 - r_id // 4, 1 << 20)

    hid_cp.wait()
    gain = gain_row(an_ref)
    for i in range(n_steps):
        for h in range(0, n_batch, 32):
            x = hid[i, h:h + 32, :].astype(jnp.float32)
            inv = lax.rsqrt(jnp.mean(x * x, axis=-1, keepdims=True) + NORM_EPS)
            nrm[i * n_batch + h:i * n_batch + h + 32, :] = (x * inv * gain).astype(jnp.bfloat16)

    def rope(x, g, cos, sin):
        inv = lax.rsqrt(jnp.mean(x * x, axis=-1, keepdims=True) + NORM_EPS)
        y = x * inv * g
        return y * cos + pltpu.roll(y, HEAD // 2, 1) * sin

    tabs = []
    for i in range(n_steps):
        if i == 0:
            c, s = cos0, sin0
        else:
            ci, si = jnp.cos(freq * float(i)), jnp.sin(freq * float(i))
            c, s = cos0 * ci - sin0 * si, sin0 * ci + cos0 * si
        pos_s_c, pos_s_s = c, s * sign
        tabs.append((pos_s_c, pos_s_s))

    for cp in w_cps:
        cp.wait()
    qg = qg_ref[...].astype(jnp.float32)
    kg = kg_ref[...].astype(jnp.float32)
    nq = n_q * HEAD
    nk = n_kv * HEAD
    raw[:, :nq] = jnp.dot(nrm[...], wq[...], preferred_element_type=jnp.float32)
    raw[:, nq:nq + nk] = jnp.dot(nrm[...], wk[...], preferred_element_type=jnp.float32)
    raw[:, nq + nk:] = jnp.dot(nrm[...], wv[...], preferred_element_type=jnp.float32)
    for i in range(n_steps):
        rs = slice(i * n_batch, (i + 1) * n_batch)
        cos, sin = tabs[i]
        for h in range(n_q):
            q_s[pl.ds(i * n_q + h, n_batch, stride=n_steps * n_q), :] = rope(raw[rs, h * HEAD:(h + 1) * HEAD], qg, cos, sin)
        for h in range(n_kv):
            k_s[pl.ds(i * n_kv + h, n_batch, stride=n_steps * n_kv), :] = rope(
                raw[rs, nq + h * HEAD:nq + (h + 1) * HEAD], kg, cos, sin)
            v_s[pl.ds(i * n_kv + h, n_batch, stride=n_steps * n_kv), :] = raw[rs, nq + nk + h * HEAD:nq + nk + (h + 1) * HEAD]

    row32 = lax.broadcasted_iota(jnp.int32, (32, HEAD), 0)
    eye_r = lax.broadcasted_iota(jnp.int32, (16, HEAD), 0)
    eye_c = lax.broadcasted_iota(jnp.int32, (16, HEAD), 1)
    eye_m = eye_r == eye_c
    eye_l = eye_r + 16 == eye_c
    zero24 = jnp.zeros((24, HEAD), jnp.float32)

    @pl.loop(0, n_chunk)
    def _(c):
        a, b = kv_in(c)
        a.wait()
        b.wait()
        lps = []
        for u in range(CHUNK):
            bb = c * CHUNK + u
            lp = start_ref[bb] - blk_start
            lps.append(lp)
            base = jnp.clip((lp // 8) * 8, 0, seq_blk - 16)
            rel = (lp - base) * 2
            shift = jnp.bitwise_and(rel, 31)
            hit = (row32 >= rel) & (row32 < rel + 8)
            win = pl.ds(pl.multiple_of(base * 2, 16), 32)
            for src, dst in ((k_s, kbuf), (v_s, vbuf)):
                new = src[pl.ds(pl.multiple_of(bb * 8, 8), 8), :]
                new = pltpu.roll(jnp.concatenate([new, zero24], axis=0), shift, 0)
                old = dst[bb, win, :].astype(jnp.float32)
                dst[bb, win, :] = jnp.where(hit, new, old).astype(jnp.bfloat16)
        for u in range(CHUNK):
            bb = c * CHUNK + u
            q = q_s[pl.ds(pl.multiple_of(bb * 16, 16), 16), :].astype(jnp.bfloat16)
            sc_s[u] = lax.dot_general(q, kbuf[bb], (((1,), (1,)), ((), ())), preferred_element_type=jnp.float32)
        tops = []
        for u in range(CHUNK):
            s = jnp.where(key_s[...] <= lps[u], sc_s[u] * scale, NEG_BIG)
            sc_s[u] = s
            tops.append(jnp.maximum(jnp.max(s, axis=-1, keepdims=True), 0.5 * NEG_BIG))
        sums = []
        for u in range(CHUNK):
            p = jnp.exp(sc_s[u] - tops[u])
            sums.append(jnp.sum(p, axis=-1, keepdims=True))
            pr_s[u] = p.astype(jnp.bfloat16)
        for u in range(CHUNK):
            bb = c * CHUNK + u
            o_ref[pl.ds(bb, 16, stride=n_batch), :] = jnp.dot(pr_s[u], vbuf[bb], preferred_element_type=jnp.float32)
        for u in range(CHUNK):
            ml = jnp.where(eye_m, tops[u], 0.0) + jnp.where(eye_l, sums[u], 0.0)
            ml_s[pl.ds(c * CHUNK + u, 1), :] = jnp.sum(ml, axis=0, keepdims=True)
        a, b = kv_out(c)
        a.start()
        b.start()

    for i in range(n_steps):
        ml = ml_s[...]
        ml_ref[i] = ml if i == 0 else pltpu.roll(ml, HEAD - 4 * i, 1)

    @pl.loop(0, n_chunk)
    def _(c):
        a, b = kv_out(c)
        a.wait()
        b.wait()


def attend(start_pos, hidden, w_q, w_k, w_v, k_cache, v_cache, attn_norm, q_gain, k_gain):
    n_steps, n_batch, width = hidden.shape
    rows = k_cache.shape[1]
    n_chunk = n_batch // CHUNK
    nq, nk = w_q.shape[1], w_k.shape[1]
    half = HEAD // 2
    f = ROPE_BASE ** (-(np.arange(half, dtype=np.float64) * (2.0 / HEAD)))
    freq = np.stack([np.concatenate([f, f]), np.concatenate([-np.ones(half), np.ones(half)])]).astype(np.float32)
    vm = pl.BlockSpec(memory_space=pltpu.VMEM)
    anyspec = pl.BlockSpec(memory_space=pltpu.HBM)
    return pl.pallas_call(
        attend_kernel,
        name='attend',
        out_shape=(jax.ShapeDtypeStruct((16 * n_batch, HEAD), jnp.float32),
                   jax.ShapeDtypeStruct((n_steps, n_batch, HEAD), jnp.float32),
                   jax.ShapeDtypeStruct(k_cache.shape, jnp.bfloat16),
                   jax.ShapeDtypeStruct(v_cache.shape, jnp.bfloat16)),
        in_specs=[pl.BlockSpec(memory_space=pltpu.SMEM)] + [anyspec] * 6 + [vm] * 4,
        out_specs=(vm, vm, anyspec, anyspec),
        scratch_shapes=[
            pltpu.VMEM(hidden.shape, jnp.bfloat16),
            pltpu.VMEM(w_q.shape, jnp.bfloat16),
            pltpu.VMEM(w_k.shape, jnp.bfloat16),
            pltpu.VMEM(w_v.shape, jnp.bfloat16),
            pltpu.VMEM(k_cache.shape, jnp.bfloat16),
            pltpu.VMEM(v_cache.shape, jnp.bfloat16),
            pltpu.VMEM((n_steps * n_batch, width), jnp.bfloat16),
            pltpu.VMEM((n_steps * n_batch, nq + 2 * nk), jnp.float32),
            pltpu.VMEM((n_batch * 16, HEAD), jnp.float32),
            pltpu.VMEM((n_batch * 8, HEAD), jnp.float32),
            pltpu.VMEM((n_batch * 8, HEAD), jnp.float32),
            pltpu.VMEM((n_batch, HEAD), jnp.float32),
            pltpu.VMEM((n_batch, HEAD), jnp.float32),
            pltpu.VMEM((16, rows), jnp.int32),
            pltpu.VMEM((CHUNK, 16, rows), jnp.float32),
            pltpu.VMEM((CHUNK, 16, rows), jnp.bfloat16),
            pltpu.SemaphoreType.DMA((3,)),
            pltpu.SemaphoreType.DMA,
            pltpu.SemaphoreType.DMA((n_chunk,)),
            pltpu.SemaphoreType.DMA((n_chunk,)),
            pltpu.SemaphoreType.DMA((n_chunk,)),
            pltpu.SemaphoreType.DMA((n_chunk,)),
        ],
        compiler_params=pltpu.CompilerParams(vmem_limit_bytes=67043328),
        cost_estimate=pl.CostEstimate(flops=2 * 10 ** 9, bytes_accessed=40 * 10 ** 6, transcendentals=10 ** 6),
    )(start_pos, hidden, w_q, w_k, w_v, k_cache, v_cache, attn_norm.reshape(-1, HEAD), q_gain.reshape(1, -1), k_gain.reshape(1, -1), jnp.asarray(freq))


N_COL = 8
N_HALF = 2
LAG = 5
LAG_Y = 8


def layer_kernel(o_own, ml_own, hid_hbm, wo_hbm, wg_hbm, wu_hbm, wd_hbm, mn_ref, out_ref,
                 oa, mla, om, mlm, oy, mly, own, ml_mine, attn, hid, wo, wg, wu, wd,
                 p1, e1, x1, r1, m_s, act, p2, e2, x2, ob, yb, pb, pf,
                 ld_sem, w_sem, a1_snd, a1_rcv, a2_snd, a2_rcv, es1, er1, xs1, xr1, ts1, tr1,
                 es2, er2, xs2, xr2, ts2, tr2, ps, pr, ys, yr, fs, fr):
    n_steps, n_batch, width = hid_hbm.shape
    n_half = n_batch // N_HALF
    n_col = width // N_COL
    n_piece = N_COL * N_HALF
    tp = lax.axis_index('tp')
    sp = lax.axis_index('sp')
    core = sp % 2
    row = sp // 2
    partner = {'sp': row * 2 + 1 - core}
    across = {'sp': (1 - row) * 2 + core}
    is_mid = (tp % 3) != 0
    is_end = (tp % 3) == 0
    to_mid = {'tp': (tp + 3) // 3}
    to_end = {'tp': (tp - 1) * 3}
    to_other = {'tp': 3 - tp}
    mesh_id = pl.DeviceIdType.MESH

    def remote(src, dst, ssem, rsem, dev):
        return pltpu.make_async_remote_copy(src_ref=src, dst_ref=dst, send_sem=ssem, recv_sem=rsem, device_id=dev, device_id_type=mesh_id)

    lds = [pltpu.make_async_copy(hid_hbm.at[sp], hid, ld_sem)]
    wts = [pltpu.make_async_copy(a, b, w_sem.at[j]) for j, (a, b) in enumerate(((wo_hbm, wo), (wg_hbm, wg), (wu_hbm, wu), (wd_hbm, wd)))]
    for cp in lds:
        cp.start()

    barrier = pltpu.get_barrier_semaphore()
    for dev in (partner, across):
        pl.semaphore_signal(barrier, inc=1, device_id=dev, device_id_type=mesh_id)

    @pl.when(is_mid)
    def _():
        pl.semaphore_signal(barrier, inc=1, device_id=to_end, device_id_type=mesh_id)
        pl.semaphore_signal(barrier, inc=1, device_id=to_other, device_id_type=mesh_id)
        pl.semaphore_wait(barrier, 4)

    @pl.when(is_end)
    def _():
        pl.semaphore_signal(barrier, inc=1, device_id=to_mid, device_id_type=mesh_id)
        pl.semaphore_wait(barrier, 3)

    for cp in lds:
        cp.wait()
    a1 = []
    for q, jy in enumerate((1 - row, row)):
        step = jy * 2 + 1 - core
        a1.append((remote(ml_own.at[step], mla.at[q], a1_snd.at[2 * q], a1_rcv.at[2 * q], partner),
                   remote(o_own.at[pl.ds(step * 4, 4)], oa.at[q], a1_snd.at[2 * q + 1], a1_rcv.at[2 * q + 1], partner)))
        for cp in a1[-1]:
            cp.start()

    lane = lax.broadcasted_iota(jnp.int32, (n_half, HEAD), 1)

    def weigh(ma, mb):
        top = jnp.maximum(ma, mb)
        wa, wb = jnp.exp(ma - top), jnp.exp(mb - top)
        tot = pltpu.roll(ma, HEAD - 16, 1) * wa + pltpu.roll(mb, HEAD - 16, 1) * wb
        return top, wa, wb, tot

    def merge_core(q, step, dst, mldst):
        for cp in a1[q]:
            cp.wait()
        for h in range(N_HALF):
            rs = pl.ds(h * n_half, n_half)
            top, wa, wb, tot = weigh(ml_own[step, rs, :], mla[q, rs, :])
            mldst[h] = jnp.where(lane < 16, top, pltpu.roll(tot, 16, 1))
            for k in range(4):
                dst[h, k] = o_own[step * 4 + k, rs, :] * wa[:, k:k + 1] + oa[q, k, rs, :] * wb[:, k:k + 1]

    merge_core(0, (1 - row) * 2 + core, om, mlm)
    a2 = []
    for h in range(N_HALF):
        a2.append((remote(mlm.at[h], mly.at[h], a2_snd.at[2 * h], a2_rcv.at[2 * h], across),
                   remote(om.at[h], oy.at[h], a2_snd.at[2 * h + 1], a2_rcv.at[2 * h + 1], across)))
        for cp in a2[-1]:
            cp.start()
    for cp in wts:
        cp.start()
    merge_core(1, row * 2 + core, own, ml_mine)
    wts[0].wait()

    e1_cp = lambda t: remote(p1.at[t], e1.at[t], es1.at[t], er1.at[t], to_mid)
    x1_cp = lambda t: remote(p1.at[t], x1.at[t], xs1.at[t], xr1.at[t], to_other)
    t1_cp = lambda t: remote(r1.at[t], r1.at[t], ts1.at[t], tr1.at[t], to_end)
    e2_cp = lambda t: remote(p2.at[t], e2.at[t], es2.at[t], er2.at[t], to_mid)
    x2_cp = lambda t: remote(p2.at[t], x2.at[t], xs2.at[t], xr2.at[t], to_other)
    t2_cp = lambda t: remote(ob.at[t], ob.at[t], ts2.at[t], tr2.at[t], to_end)
    p_cp = lambda t: remote(ob.at[t], pb.at[t], ps.at[t], pr.at[t], partner)
    y_cp = lambda t: remote(ob.at[t], yb.at[t], ys.at[t], yr.at[t], across)
    f_cp = lambda t: remote(yb.at[t], pf.at[t], fs.at[t], fr.at[t], partner)

    def spread(h, lhs, w, dst, cp):
        wide = width // 2
        per = N_COL // 2
        for j in range(2):
            d = jnp.dot(lhs, w[:, j * wide:(j + 1) * wide], preferred_element_type=jnp.float32)
            for n in range(per):
                dst[h * N_COL + j * per + n] = d[:, n * n_col:(n + 1) * n_col]

            @pl.when(is_end)
            def _():
                @pl.loop(h * N_COL + j * per, h * N_COL + (j + 1) * per)
                def _(t):
                    cp(t).start()

    for h in range(N_HALF):
        for cp in a2[h]:
            cp.wait()
        _, wa, wb, tot = weigh(ml_mine[h], mly[h])
        inv = 1.0 / tot
        for k in range(4):
            val = (own[h, k] * wa[:, k:k + 1] + oy[h, k] * wb[:, k:k + 1]) * inv[:, k:k + 1]
            attn[h, :, k * HEAD:(k + 1) * HEAD] = val.astype(jnp.bfloat16)

        spread(h, attn[h], wo, p1, e1_cp)

    def sum_step(s):
        @pl.when(s < n_piece)
        def _():
            e1_cp(s).wait_recv()
            p1[s] = p1[s] + e1[s]
            x1_cp(s).start()

        @pl.when(s >= LAG)
        def _():
            t = s - LAG
            h = t // N_COL
            rs = pl.ds(pl.multiple_of(h * n_half, n_half), n_half)
            cs = pl.ds(pl.multiple_of((t - h * N_COL) * n_col, n_col), n_col)
            x1_cp(t).wait_recv()
            r = hid[rs, cs].astype(jnp.float32) + (p1[t] + x1[t])
            r1[t] = r.astype(jnp.bfloat16).astype(jnp.float32)
            t1_cp(t).start()

    def sum_steps(lo, hi):
        @pl.when(is_mid)
        def _():
            pl.loop(lo, hi)(sum_step)

    def end_recv(lo, hi):
        @pl.when(is_end)
        def _():
            @pl.loop(lo, hi)
            def _(t):
                t1_cp(t).wait_recv()

    gain = gain_row(mn_ref)
    ffn = wg.shape[1]
    blk = ffn // 3
    done = 0
    for h in range(N_HALF):
        stop = (h + 1) * N_COL + LAG
        sum_steps(done, stop)
        done = stop
        end_recv(h * N_COL, (h + 1) * N_COL)
        sq = jnp.zeros((n_half, 1), jnp.float32)
        for n in range(N_COL):
            r = r1[h * N_COL + n]
            sq = sq + jnp.sum(r * r, axis=-1, keepdims=True)
        inv = lax.rsqrt(sq / width + NORM_EPS)
        for n in range(N_COL):
            m_s[:, n * n_col:(n + 1) * n_col] = (r1[h * N_COL + n] * inv * gain[:, n * n_col:(n + 1) * n_col]).astype(jnp.bfloat16)
        if h == 0:
            wts[1].wait()
            wts[2].wait()
        for n in range(3):
            cs = slice(n * blk, (n + 1) * blk)
            g = jnp.dot(m_s[...], wg[:, cs], preferred_element_type=jnp.float32)
            u = jnp.dot(m_s[...], wu[:, cs], preferred_element_type=jnp.float32)
            act[:, cs] = (jax.nn.silu(g) * u).astype(jnp.bfloat16)
            if h + 1 < N_HALF:
                sum_steps(done, done + 2)
                done += 2
        if h == 0:
            wts[3].wait()
        spread(h, act[...], wd, p2, e2_cp)

    def share(t):
        p_cp(t).start()
        y_cp(t).start()

    def relay(t):
        y_cp(t).wait_recv()
        f_cp(t).start()

    @pl.when(is_mid)
    def _():
        @pl.loop(0, n_piece + LAG + LAG_Y)
        def _(s):
            @pl.when(s < n_piece)
            def _():
                e2_cp(s).wait_recv()
                p2[s] = p2[s] + e2[s]
                x2_cp(s).start()

            @pl.when((s >= LAG) & (s < n_piece + LAG))
            def _():
                t = s - LAG
                x2_cp(t).wait_recv()
                o = r1[t] + (p2[t] + x2[t])
                ob[t] = o.astype(jnp.bfloat16).astype(jnp.float32)
                t2_cp(t).start()
                share(t)

            @pl.when(s >= LAG + LAG_Y)
            def _():
                relay(s - LAG - LAG_Y)

    @pl.when(is_end)
    def _():
        @pl.loop(0, n_piece + LAG_Y)
        def _(s):
            @pl.when(s < n_piece)
            def _():
                t2_cp(s).wait_recv()
                share(s)

            @pl.when(s >= LAG_Y)
            def _():
                relay(s - LAG_Y)

    @pl.loop(0, n_piece)
    def _(t):
        h = t // N_COL
        rs = pl.ds(pl.multiple_of(h * n_half, n_half), n_half)
        cs = pl.ds(pl.multiple_of((t - h * N_COL) * n_col, n_col), n_col)
        out_ref[sp, rs, cs] = ob[t].astype(jnp.bfloat16)
        out_ref[(1 - row) * 2 + core, rs, cs] = yb[t].astype(jnp.bfloat16)
        p_cp(t).wait_recv()
        out_ref[row * 2 + 1 - core, rs, cs] = pb[t].astype(jnp.bfloat16)
        f_cp(t).wait_recv()
        out_ref[(1 - row) * 2 + 1 - core, rs, cs] = pf[t].astype(jnp.bfloat16)
        p_cp(t).wait_send()
        y_cp(t).wait_send()
        f_cp(t).wait_send()

        @pl.when(is_mid)
        def _():
            x1_cp(t).wait_send()
            t1_cp(t).wait_send()
            x2_cp(t).wait_send()
            t2_cp(t).wait_send()

        @pl.when(is_end)
        def _():
            e1_cp(t).wait_send()
            e2_cp(t).wait_send()


def layer(o, ml, hidden, w_o, w_gate, w_up, w_down, mlp_norm):
    n_steps, n_batch, width = hidden.shape
    n_half = n_batch // N_HALF
    n_col = width // N_COL
    n_piece = N_COL * N_HALF
    vm = pl.BlockSpec(memory_space=pltpu.VMEM)
    anyspec = pl.BlockSpec(memory_space=pltpu.HBM)
    f32, bf16 = jnp.float32, jnp.bfloat16
    piece = pltpu.VMEM((n_piece, n_half, n_col), f32)
    dma = pltpu.SemaphoreType.DMA
    return pl.pallas_call(
        layer_kernel,
        name='layer',
        out_shape=jax.ShapeDtypeStruct(hidden.shape, bf16),
        in_specs=[vm] * 2 + [anyspec] * 5 + [vm],
        out_specs=vm,
        scratch_shapes=[
            pltpu.VMEM((2, 4, n_batch, HEAD), f32),
            pltpu.VMEM((2, n_batch, HEAD), f32),
            pltpu.VMEM((N_HALF, 4, n_half, HEAD), f32),
            pltpu.VMEM((N_HALF, n_half, HEAD), f32),
            pltpu.VMEM((N_HALF, 4, n_half, HEAD), f32),
            pltpu.VMEM((N_HALF, n_half, HEAD), f32),
            pltpu.VMEM((N_HALF, 4, n_half, HEAD), f32),
            pltpu.VMEM((N_HALF, n_half, HEAD), f32),
            pltpu.VMEM((N_HALF, n_half, 4 * HEAD), bf16),
            pltpu.VMEM((n_batch, width), bf16),
            pltpu.VMEM(w_o.shape, bf16),
            pltpu.VMEM(w_gate.shape, bf16),
            pltpu.VMEM(w_up.shape, bf16),
            pltpu.VMEM(w_down.shape, bf16),
            piece, piece, piece, piece,
            pltpu.VMEM((n_half, width), bf16),
            pltpu.VMEM((n_half, w_gate.shape[1]), bf16),
            piece, piece, piece, piece, piece, piece, piece,
            dma, dma((4,)), dma((4,)), dma((4,)), dma((2 * N_HALF,)), dma((2 * N_HALF,)),
        ] + [dma((n_piece,))] * 18,
        compiler_params=pltpu.CompilerParams(collective_id=0, has_side_effects=True, vmem_limit_bytes=67043328),
        cost_estimate=pl.CostEstimate(flops=2 * 10 ** 9, bytes_accessed=30 * 10 ** 6, transcendentals=10 ** 6),
    )(o.reshape(16, n_batch, HEAD), ml, hidden, w_o, w_gate, w_up, w_down, mlp_norm.reshape(-1, HEAD))


def solution(mesh):
    cache_spec = P('dp', 'sp', 'tp', None)
    col_spec = P(None, 'tp')
    row_spec = P('tp', None)
    in_specs = (P(None, 'dp', None), P('dp'), cache_spec, cache_spec, col_spec, col_spec, col_spec, row_spec,
                col_spec, col_spec, row_spec, P(), P(), P(), P())
    out_specs = (P(None, 'dp', None), cache_spec, cache_spec)

    def shard_body(hidden, start_pos, k_cache, v_cache, w_q, w_k, w_v, w_o, w_gate, w_up, w_down, attn_norm, mlp_norm, q_gain, k_gain):
        flat = (k_cache.shape[0], k_cache.shape[1] * k_cache.shape[2], k_cache.shape[3])
        o, ml, k_out, v_out = attend(start_pos, hidden, w_q, w_k, w_v, k_cache.reshape(flat), v_cache.reshape(flat), attn_norm, q_gain, k_gain)
        out = layer(o, ml, hidden, w_o, w_gate, w_up, w_down, mlp_norm)
        return out, k_out.reshape(k_cache.shape), v_out.reshape(v_cache.shape)

    return jax.shard_map(shard_body, mesh=mesh, in_specs=in_specs, out_specs=out_specs, check_vma=False)
```

```python
import functools
import jax
import jax.numpy as jnp
import numpy as np
from jax import lax
from jax.experimental import pallas as pl
from jax.experimental.pallas import tpu as pltpu
from jax.sharding import PartitionSpec as P

ROPE_BASE = 1000000.0
NORM_EPS = 1e-06
NEG_BIG = -1e30
HEAD = 128
CHUNK = 8


def gain_row(ref):
    g = ref[...].astype(jnp.float32)
    return jnp.concatenate([g[j:j + 1] for j in range(g.shape[0])], axis=1)


def attend_kernel(start_ref, hid_hbm, wq_hbm, wk_hbm, wv_hbm, kc_hbm, vc_hbm, an_ref, qg_ref, kg_ref, freq_ref,
                  o_ref, ml_ref, ko_hbm, vo_hbm,
                  hid, wq, wk, wv, kbuf, vbuf, nrm, raw, q_s, k_s, v_s, pos_s, ml_s, key_s, sc_s, pr_s,
                  w_sem, h_sem, kin_sem, vin_sem, kout_sem, vout_sem):
    n_steps, n_batch, width = hid.shape
    rows = kbuf.shape[1]
    seq_blk = rows // 2
    n_chunk = n_batch // CHUNK
    n_q = wq.shape[1] // HEAD
    n_kv = wk.shape[1] // HEAD
    blk_start = lax.axis_index('sp') * seq_blk
    scale = HEAD ** -0.5

    hid_cp = pltpu.make_async_copy(hid_hbm, hid, h_sem)
    hid_cp.start()
    w_cps = [pltpu.make_async_copy(a, b, w_sem.at[j]) for j, (a, b) in enumerate(((wq_hbm, wq), (wk_hbm, wk), (wv_hbm, wv)))]
    for cp in w_cps:
        cp.start()

    def kv_in(c):
        sl = pl.ds(c * CHUNK, CHUNK)
        return (pltpu.make_async_copy(kc_hbm.at[sl], kbuf.at[sl], kin_sem.at[c]),
                pltpu.make_async_copy(vc_hbm.at[sl], vbuf.at[sl], vin_sem.at[c]))

    def kv_out(c):
        sl = pl.ds(c * CHUNK, CHUNK)
        return (pltpu.make_async_copy(kbuf.at[sl], ko_hbm.at[sl], kout_sem.at[c]),
                pltpu.make_async_copy(vbuf.at[sl], vo_hbm.at[sl], vout_sem.at[c]))

    @pl.loop(0, n_chunk)
    def _(c):
        a, b = kv_in(c)
        a.start()
        b.start()

    @pl.loop(0, n_batch)
    def _(b):
        pos_s[pl.ds(b, 1), :] = jnp.full((1, HEAD), start_ref[b].astype(jnp.float32), jnp.float32)

    freq = freq_ref[0:1, :]
    sign = freq_ref[1:2, :]
    ang = pos_s[...] * freq
    cos0 = jnp.cos(ang)
    sin0 = jnp.sin(ang)

    r_id = lax.broadcasted_iota(jnp.int32, (16, rows), 0)
    c_id = lax.broadcasted_iota(jnp.int32, (16, rows), 1)
    same = ((r_id % 4) // 2) == (c_id % 2)
    key_s[...] = jnp.where(same, c_id // 2 - r_id // 4, 1 << 20)

    hid_cp.wait()
    gain = gain_row(an_ref)
    for i in range(n_steps):
        for h in range(0, n_batch, 32):
            x = hid[i, h:h + 32, :].astype(jnp.float32)
            inv = lax.rsqrt(jnp.mean(x * x, axis=-1, keepdims=True) + NORM_EPS)
            nrm[i * n_batch + h:i * n_batch + h + 32, :] = (x * inv * gain).astype(jnp.bfloat16)

    def rope(x, g, cos, sin):
        inv = lax.rsqrt(jnp.mean(x * x, axis=-1, keepdims=True) + NORM_EPS)
        y = x * inv * g
        return y * cos + pltpu.roll(y, HEAD // 2, 1) * sin

    tabs = []
    for i in range(n_steps):
        if i == 0:
            c, s = cos0, sin0
        else:
            ci, si = jnp.cos(freq * float(i)), jnp.sin(freq * float(i))
            c, s = cos0 * ci - sin0 * si, sin0 * ci + cos0 * si
        pos_s_c, pos_s_s = c, s * sign
        tabs.append((pos_s_c, pos_s_s))

    for cp in w_cps:
        cp.wait()
    qg = qg_ref[...].astype(jnp.float32)
    kg = kg_ref[...].astype(jnp.float32)
    nq = n_q * HEAD
    nk = n_kv * HEAD
    raw[:, :nq] = jnp.dot(nrm[...], wq[...], preferred_element_type=jnp.float32)
    raw[:, nq:nq + nk] = jnp.dot(nrm[...], wk[...], preferred_element_type=jnp.float32)
    raw[:, nq + nk:] = jnp.dot(nrm[...], wv[...], preferred_element_type=jnp.float32)
    for i in range(n_steps):
        rs = slice(i * n_batch, (i + 1) * n_batch)
        cos, sin = tabs[i]
        for h in range(n_q):
            q_s[pl.ds(i * n_q + h, n_batch, stride=n_steps * n_q), :] = rope(raw[rs, h * HEAD:(h + 1) * HEAD], qg, cos, sin)
        for h in range(n_kv):
            k_s[pl.ds(i * n_kv + h, n_batch, stride=n_steps * n_kv), :] = rope(
                raw[rs, nq + h * HEAD:nq + (h + 1) * HEAD], kg, cos, sin)
            v_s[pl.ds(i * n_kv + h, n_batch, stride=n_steps * n_kv), :] = raw[rs, nq + nk + h * HEAD:nq + nk + (h + 1) * HEAD]

    row32 = lax.broadcasted_iota(jnp.int32, (32, HEAD), 0)
    eye_r = lax.broadcasted_iota(jnp.int32, (16, HEAD), 0)
    eye_c = lax.broadcasted_iota(jnp.int32, (16, HEAD), 1)
    eye_m = eye_r == eye_c
    eye_l = eye_r + 16 == eye_c
    zero24 = jnp.zeros((24, HEAD), jnp.float32)

    @pl.loop(0, n_chunk)
    def _(c):
        a, b = kv_in(c)
        a.wait()
        b.wait()
        lps = []
        for u in range(CHUNK):
            bb = c * CHUNK + u
            lp = start_ref[bb] - blk_start
            lps.append(lp)
            base = jnp.clip((lp // 8) * 8, 0, seq_blk - 16)
            rel = (lp - base) * 2
            shift = jnp.bitwise_and(rel, 31)
            hit = (row32 >= rel) & (row32 < rel + 8)
            win = pl.ds(pl.multiple_of(base * 2, 16), 32)
            for src, dst in ((k_s, kbuf), (v_s, vbuf)):
                new = src[pl.ds(pl.multiple_of(bb * 8, 8), 8), :]
                new = pltpu.roll(jnp.concatenate([new, zero24], axis=0), shift, 0)
                old = dst[bb, win, :].astype(jnp.float32)
                dst[bb, win, :] = jnp.where(hit, new, old).astype(jnp.bfloat16)
        for u in range(CHUNK):
            bb = c * CHUNK + u
            q = q_s[pl.ds(pl.multiple_of(bb * 16, 16), 16), :].astype(jnp.bfloat16)
            sc_s[u] = lax.dot_general(q, kbuf[bb], (((1,), (1,)), ((), ())), preferred_element_type=jnp.float32)
        tops = []
        for u in range(CHUNK):
            s = jnp.where(key_s[...] <= lps[u], sc_s[u] * scale, NEG_BIG)
            sc_s[u] = s
            tops.append(jnp.maximum(jnp.max(s, axis=-1, keepdims=True), 0.5 * NEG_BIG))
        sums = []
        for u in range(CHUNK):
            p = jnp.exp(sc_s[u] - tops[u])
            sums.append(jnp.sum(p, axis=-1, keepdims=True))
            pr_s[u] = p.astype(jnp.bfloat16)
        for u in range(CHUNK):
            bb = c * CHUNK + u
            o_ref[pl.ds(bb, 16, stride=n_batch), :] = jnp.dot(pr_s[u], vbuf[bb], preferred_element_type=jnp.float32)
        for u in range(CHUNK):
            ml = jnp.where(eye_m, tops[u], 0.0) + jnp.where(eye_l, sums[u], 0.0)
            ml_s[pl.ds(c * CHUNK + u, 1), :] = jnp.sum(ml, axis=0, keepdims=True)
        a, b = kv_out(c)
        a.start()
        b.start()

    for i in range(n_steps):
        ml = ml_s[...]
        ml_ref[i] = ml if i == 0 else pltpu.roll(ml, HEAD - 4 * i, 1)

    @pl.loop(0, n_chunk)
    def _(c):
        a, b = kv_out(c)
        a.wait()
        b.wait()


def attend(start_pos, hidden, w_q, w_k, w_v, k_cache, v_cache, attn_norm, q_gain, k_gain):
    n_steps, n_batch, width = hidden.shape
    rows = k_cache.shape[1]
    n_chunk = n_batch // CHUNK
    nq, nk = w_q.shape[1], w_k.shape[1]
    half = HEAD // 2
    f = ROPE_BASE ** (-(np.arange(half, dtype=np.float64) * (2.0 / HEAD)))
    freq = np.stack([np.concatenate([f, f]), np.concatenate([-np.ones(half), np.ones(half)])]).astype(np.float32)
    vm = pl.BlockSpec(memory_space=pltpu.VMEM)
    anyspec = pl.BlockSpec(memory_space=pltpu.HBM)
    return pl.pallas_call(
        attend_kernel,
        name='attend',
        out_shape=(jax.ShapeDtypeStruct((16 * n_batch, HEAD), jnp.float32),
                   jax.ShapeDtypeStruct((n_steps, n_batch, HEAD), jnp.float32),
                   jax.ShapeDtypeStruct(k_cache.shape, jnp.bfloat16),
                   jax.ShapeDtypeStruct(v_cache.shape, jnp.bfloat16)),
        in_specs=[pl.BlockSpec(memory_space=pltpu.SMEM)] + [anyspec] * 6 + [vm] * 4,
        out_specs=(vm, vm, anyspec, anyspec),
        scratch_shapes=[
            pltpu.VMEM(hidden.shape, jnp.bfloat16),
            pltpu.VMEM(w_q.shape, jnp.bfloat16),
            pltpu.VMEM(w_k.shape, jnp.bfloat16),
            pltpu.VMEM(w_v.shape, jnp.bfloat16),
            pltpu.VMEM(k_cache.shape, jnp.bfloat16),
            pltpu.VMEM(v_cache.shape, jnp.bfloat16),
            pltpu.VMEM((n_steps * n_batch, width), jnp.bfloat16),
            pltpu.VMEM((n_steps * n_batch, nq + 2 * nk), jnp.float32),
            pltpu.VMEM((n_batch * 16, HEAD), jnp.float32),
            pltpu.VMEM((n_batch * 8, HEAD), jnp.float32),
            pltpu.VMEM((n_batch * 8, HEAD), jnp.float32),
            pltpu.VMEM((n_batch, HEAD), jnp.float32),
            pltpu.VMEM((n_batch, HEAD), jnp.float32),
            pltpu.VMEM((16, rows), jnp.int32),
            pltpu.VMEM((CHUNK, 16, rows), jnp.float32),
            pltpu.VMEM((CHUNK, 16, rows), jnp.bfloat16),
            pltpu.SemaphoreType.DMA((3,)),
            pltpu.SemaphoreType.DMA,
            pltpu.SemaphoreType.DMA((n_chunk,)),
            pltpu.SemaphoreType.DMA((n_chunk,)),
            pltpu.SemaphoreType.DMA((n_chunk,)),
            pltpu.SemaphoreType.DMA((n_chunk,)),
        ],
        compiler_params=pltpu.CompilerParams(vmem_limit_bytes=67043328),
        cost_estimate=pl.CostEstimate(flops=2 * 10 ** 9, bytes_accessed=40 * 10 ** 6, transcendentals=10 ** 6),
    )(start_pos, hidden, w_q, w_k, w_v, k_cache, v_cache, attn_norm.reshape(-1, HEAD), q_gain.reshape(1, -1), k_gain.reshape(1, -1), jnp.asarray(freq))


N_COL = 4
N_HALF = 4
LAG = 5
LAG_Y = 8
TILES = 3
SERVE = 1


def layer_kernel(o_hbm, ml_hbm, hid_hbm, wo_hbm, wg_hbm, wu_hbm, wd_hbm, mn_hbm, out_hbm,
                 o_own, ml_own, mn_ref, out_ref, oa, mla, om, mlm, oy, mly, own, ml_mine, attn, hid, wo, wg, wu, wd,
                 p1, e1, x1, r1, m_s, act, p2, e2, x2, ob, yb, pb, pf,
                 ld_sem, out_sem, w_sem, a1_snd, a1_rcv, a2_snd, a2_rcv, es1, er1, xs1, xr1, ts1, tr1,
                 es2, er2, xs2, xr2, ts2, tr2, ps, pr, ys, yr, fs, fr):
    n_steps, n_batch, width = hid_hbm.shape
    n_half = n_batch // N_HALF
    n_col = width // N_COL
    n_piece = N_COL * N_HALF
    tp = lax.axis_index('tp')
    sp = lax.axis_index('sp')
    core = sp % 2
    row = sp // 2
    partner = {'sp': row * 2 + 1 - core}
    across = {'sp': (1 - row) * 2 + core}
    is_mid = (tp % 3) != 0
    is_end = (tp % 3) == 0
    to_mid = {'tp': (tp + 3) // 3}
    to_end = {'tp': (tp - 1) * 3}
    to_other = {'tp': 3 - tp}
    mesh_id = pl.DeviceIdType.MESH

    def remote(src, dst, ssem, rsem, dev):
        return pltpu.make_async_remote_copy(src_ref=src, dst_ref=dst, send_sem=ssem, recv_sem=rsem, device_id=dev, device_id_type=mesh_id)

    send_to = 1 - core
    o_cps, ml_cps = [], []
    for q, step in enumerate(((1 - row) * 2 + send_to, row * 2 + send_to, (1 - row) * 2 + core, row * 2 + core)):
        o_cps.append(pltpu.make_async_copy(o_hbm.at[pl.ds(step * 4, 4)], o_own.at[pl.ds(step * 4, 4)], ld_sem.at[q]))
    ml_cp = pltpu.make_async_copy(ml_hbm, ml_own, ld_sem.at[4])
    hid_cp = pltpu.make_async_copy(hid_hbm.at[sp], hid, ld_sem.at[5])
    mn_cp = pltpu.make_async_copy(mn_hbm, mn_ref, ld_sem.at[6])
    lds = [ml_cp] + o_cps + [hid_cp, mn_cp]
    wts = [pltpu.make_async_copy(a, b, w_sem.at[j]) for j, (a, b) in enumerate(((wo_hbm, wo), (wg_hbm, wg), (wu_hbm, wu), (wd_hbm, wd)))]
    for cp in lds:
        cp.start()

    barrier = pltpu.get_barrier_semaphore()
    for dev in (partner, across):
        pl.semaphore_signal(barrier, inc=1, device_id=dev, device_id_type=mesh_id)

    @pl.when(is_mid)
    def _():
        pl.semaphore_signal(barrier, inc=1, device_id=to_end, device_id_type=mesh_id)
        pl.semaphore_signal(barrier, inc=1, device_id=to_other, device_id_type=mesh_id)
        pl.semaphore_wait(barrier, 4)

    @pl.when(is_end)
    def _():
        pl.semaphore_signal(barrier, inc=1, device_id=to_mid, device_id_type=mesh_id)
        pl.semaphore_wait(barrier, 3)

    ml_cp.wait()
    a1 = []
    for q, jy in enumerate((1 - row, row)):
        step = jy * 2 + 1 - core
        o_cps[q].wait()
        a1.append((remote(ml_own.at[step], mla.at[q], a1_snd.at[2 * q], a1_rcv.at[2 * q], partner),
                   remote(o_own.at[pl.ds(step * 4, 4)], oa.at[q], a1_snd.at[2 * q + 1], a1_rcv.at[2 * q + 1], partner)))
        for cp in a1[-1]:
            cp.start()

    lane = lax.broadcasted_iota(jnp.int32, (n_half, HEAD), 1)

    def weigh(ma, mb):
        top = jnp.maximum(ma, mb)
        wa, wb = jnp.exp(ma - top), jnp.exp(mb - top)
        tot = pltpu.roll(ma, HEAD - 16, 1) * wa + pltpu.roll(mb, HEAD - 16, 1) * wb
        return top, wa, wb, tot

    def merge_core(q, step, dst, mldst):
        for cp in a1[q]:
            cp.wait()
        for h in range(N_HALF):
            rs = pl.ds(h * n_half, n_half)
            top, wa, wb, tot = weigh(ml_own[step, rs, :], mla[q, rs, :])
            mldst[h] = jnp.where(lane < 16, top, pltpu.roll(tot, 16, 1))
            for k in range(4):
                dst[h, k] = o_own[step * 4 + k, rs, :] * wa[:, k:k + 1] + oa[q, k, rs, :] * wb[:, k:k + 1]

    for cp in lds[3:]:
        cp.wait()
    merge_core(0, (1 - row) * 2 + core, om, mlm)
    a2 = []
    for h in range(N_HALF):
        a2.append((remote(mlm.at[h], mly.at[h], a2_snd.at[2 * h], a2_rcv.at[2 * h], across),
                   remote(om.at[h], oy.at[h], a2_snd.at[2 * h + 1], a2_rcv.at[2 * h + 1], across)))
        for cp in a2[-1]:
            cp.start()
    for cp in wts:
        cp.start()
    merge_core(1, row * 2 + core, own, ml_mine)
    wts[0].wait()

    e1_cp = lambda t: remote(p1.at[t], e1.at[t], es1.at[t], er1.at[t], to_mid)
    x1_cp = lambda t: remote(p1.at[t], x1.at[t], xs1.at[t], xr1.at[t], to_other)
    t1_cp = lambda t: remote(r1.at[t], r1.at[t], ts1.at[t], tr1.at[t], to_end)
    e2_cp = lambda t: remote(p2.at[t], e2.at[t], es2.at[t], er2.at[t], to_mid)
    x2_cp = lambda t: remote(p2.at[t], x2.at[t], xs2.at[t], xr2.at[t], to_other)
    t2_cp = lambda t: remote(ob.at[t], ob.at[t], ts2.at[t], tr2.at[t], to_end)
    p_cp = lambda t: remote(ob.at[t], pb.at[t], ps.at[t], pr.at[t], partner)
    y_cp = lambda t: remote(ob.at[t], yb.at[t], ys.at[t], yr.at[t], across)
    f_cp = lambda t: remote(yb.at[t], pf.at[t], fs.at[t], fr.at[t], partner)

    def spread(h, lhs, w, dst, cp, after=None):
        wide = width // 2
        per = N_COL // 2
        for j in range(2):
            d = jnp.dot(lhs, w[:, j * wide:(j + 1) * wide], preferred_element_type=jnp.float32)
            for n in range(per):
                dst[h * N_COL + j * per + n] = d[:, n * n_col:(n + 1) * n_col]

            @pl.when(is_end)
            def _():
                @pl.loop(h * N_COL + j * per, h * N_COL + (j + 1) * per)
                def _(t):
                    cp(t).start()

            if after is not None:
                after(h)

    for h in range(N_HALF):
        for cp in a2[h]:
            cp.wait()
        _, wa, wb, tot = weigh(ml_mine[h], mly[h])
        inv = 1.0 / tot
        for k in range(4):
            val = (own[h, k] * wa[:, k:k + 1] + oy[h, k] * wb[:, k:k + 1]) * inv[:, k:k + 1]
            attn[h, :, k * HEAD:(k + 1) * HEAD] = val.astype(jnp.bfloat16)

        spread(h, attn[h], wo, p1, e1_cp)

    def sum_step(s):
        @pl.when(s < n_piece)
        def _():
            e1_cp(s).wait_recv()
            p1[s] = p1[s] + e1[s]
            x1_cp(s).start()

        @pl.when(s >= LAG)
        def _():
            t = s - LAG
            h = t // N_COL
            rs = pl.ds(pl.multiple_of(h * n_half, n_half), n_half)
            cs = pl.ds(pl.multiple_of((t - h * N_COL) * n_col, n_col), n_col)
            x1_cp(t).wait_recv()
            r = hid[rs, cs].astype(jnp.float32) + (p1[t] + x1[t])
            r1[t] = r.astype(jnp.bfloat16).astype(jnp.float32)
            t1_cp(t).start()

    def sum_steps(lo, hi):
        @pl.when(is_mid)
        def _():
            pl.loop(lo, hi)(sum_step)

    def end_recv(lo, hi):
        @pl.when(is_end)
        def _():
            @pl.loop(lo, hi)
            def _(t):
                t1_cp(t).wait_recv()

    def share(t):
        p_cp(t).start()
        y_cp(t).start()

    def relay(t):
        y_cp(t).wait_recv()
        f_cp(t).start()

    def share_step(s):
        @pl.when(s < n_piece)
        def _():
            e2_cp(s).wait_recv()
            p2[s] = p2[s] + e2[s]
            x2_cp(s).start()

        @pl.when((s >= LAG) & (s < n_piece + LAG))
        def _():
            t = s - LAG
            x2_cp(t).wait_recv()
            o = r1[t] + (p2[t] + x2[t])
            ob[t] = o.astype(jnp.bfloat16).astype(jnp.float32)
            t2_cp(t).start()
            share(t)

        @pl.when(s >= LAG + LAG_Y)
        def _():
            relay(s - LAG - LAG_Y)


    def share_steps(lo, hi):
        @pl.when(is_mid)
        def _():
            pl.loop(lo, hi)(share_step)

    gain = gain_row(mn_ref)
    ffn = wg.shape[1]
    blk = ffn // TILES
    done = [0, 0]

    def serve(h):
        for _ in range(SERVE):
            if done[0] < n_piece + LAG:
                sum_steps(done[0], done[0] + 1)
                done[0] += 1
            elif done[1] < h * N_COL:
                share_steps(done[1], done[1] + 1)
                done[1] += 1

    for h in range(N_HALF):
        stop = max(done[0], (h + 1) * N_COL + LAG)
        if stop > done[0]:
            sum_steps(done[0], stop)
            done[0] = stop
        end_recv(h * N_COL, (h + 1) * N_COL)
        sq = jnp.zeros((n_half, 1), jnp.float32)
        for n in range(N_COL):
            r = r1[h * N_COL + n]
            sq = sq + jnp.sum(r * r, axis=-1, keepdims=True)
        inv = lax.rsqrt(sq / width + NORM_EPS)
        for n in range(N_COL):
            m_s[:, n * n_col:(n + 1) * n_col] = (r1[h * N_COL + n] * inv * gain[:, n * n_col:(n + 1) * n_col]).astype(jnp.bfloat16)
        if h == 0:
            wts[1].wait()
            wts[2].wait()
        for n in range(TILES):
            cs = slice(n * blk, (n + 1) * blk)
            g = jnp.dot(m_s[...], wg[:, cs], preferred_element_type=jnp.float32)
            u = jnp.dot(m_s[...], wu[:, cs], preferred_element_type=jnp.float32)
            act[:, cs] = (jax.nn.silu(g) * u).astype(jnp.bfloat16)
            serve(h)
        if h == 0:
            wts[3].wait()
        spread(h, act[...], wd, p2, e2_cp, serve)

    share_steps(done[1], n_piece + LAG + LAG_Y)

    @pl.when(is_end)
    def _():
        @pl.loop(0, n_piece + LAG_Y)
        def _(s):
            @pl.when(s < n_piece)
            def _():
                t2_cp(s).wait_recv()
                share(s)

            @pl.when(s >= LAG_Y)
            def _():
                relay(s - LAG_Y)

    def put(j, t, val):
        h = t // N_COL
        rs = pl.ds(pl.multiple_of(h * n_half, n_half), n_half)
        cs = pl.ds(pl.multiple_of((t - h * N_COL) * n_col, n_col), n_col)
        out_ref[j, rs, cs] = val.astype(jnp.bfloat16)

    def leave(j, h, k):
        rs = pl.ds(h * n_half, n_half)
        return pltpu.make_async_copy(out_ref.at[j, rs], out_hbm.at[j, rs], out_sem.at[h * 4 + k])

    homes = (sp, row * 2 + 1 - core, (1 - row) * 2 + core, (1 - row) * 2 + 1 - core)
    for h in range(N_HALF):
        @pl.loop(h * N_COL, (h + 1) * N_COL)
        def _(t):
            put(homes[0], t, ob[t])
            p_cp(t).wait_recv()
            put(homes[1], t, pb[t])
            put(homes[2], t, yb[t])
            f_cp(t).wait_recv()
            put(homes[3], t, pf[t])

        for k in range(4):
            leave(homes[k], h, k).start()

    @pl.loop(0, n_piece)
    def _(t):
        p_cp(t).wait_send()
        y_cp(t).wait_send()
        f_cp(t).wait_send()

        @pl.when(is_mid)
        def _():
            x1_cp(t).wait_send()
            t1_cp(t).wait_send()
            x2_cp(t).wait_send()
            t2_cp(t).wait_send()

        @pl.when(is_end)
        def _():
            e1_cp(t).wait_send()
            e2_cp(t).wait_send()

    for h in range(N_HALF):
        for k in range(4):
            leave(homes[k], h, k).wait()


def layer(o, ml, hidden, w_o, w_gate, w_up, w_down, mlp_norm):
    n_steps, n_batch, width = hidden.shape
    n_half = n_batch // N_HALF
    n_col = width // N_COL
    n_piece = N_COL * N_HALF
    vm = pl.BlockSpec(memory_space=pltpu.VMEM)
    anyspec = pl.BlockSpec(memory_space=pltpu.HBM)
    f32, bf16 = jnp.float32, jnp.bfloat16
    piece = pltpu.VMEM((n_piece, n_half, n_col), f32)
    dma = pltpu.SemaphoreType.DMA
    return pl.pallas_call(
        layer_kernel,
        name='layer',
        out_shape=jax.ShapeDtypeStruct(hidden.shape, bf16),
        in_specs=[anyspec] * 8,
        out_specs=anyspec,
        scratch_shapes=[
            pltpu.VMEM((16, n_batch, HEAD), f32),
            pltpu.VMEM((4, n_batch, HEAD), f32),
            pltpu.VMEM((width // HEAD, HEAD), bf16),
            pltpu.VMEM(hidden.shape, bf16),
            pltpu.VMEM((2, 4, n_batch, HEAD), f32),
            pltpu.VMEM((2, n_batch, HEAD), f32),
            pltpu.VMEM((N_HALF, 4, n_half, HEAD), f32),
            pltpu.VMEM((N_HALF, n_half, HEAD), f32),
            pltpu.VMEM((N_HALF, 4, n_half, HEAD), f32),
            pltpu.VMEM((N_HALF, n_half, HEAD), f32),
            pltpu.VMEM((N_HALF, 4, n_half, HEAD), f32),
            pltpu.VMEM((N_HALF, n_half, HEAD), f32),
            pltpu.VMEM((N_HALF, n_half, 4 * HEAD), bf16),
            pltpu.VMEM((n_batch, width), bf16),
            pltpu.VMEM(w_o.shape, bf16),
            pltpu.VMEM(w_gate.shape, bf16),
            pltpu.VMEM(w_up.shape, bf16),
            pltpu.VMEM(w_down.shape, bf16),
            piece, piece, piece, piece,
            pltpu.VMEM((n_half, width), bf16),
            pltpu.VMEM((n_half, w_gate.shape[1]), bf16),
            piece, piece, piece, piece, piece, piece, piece,
            dma((7,)), dma((4 * N_HALF,)), dma((4,)), dma((4,)), dma((4,)), dma((2 * N_HALF,)), dma((2 * N_HALF,)),
        ] + [dma((n_piece,))] * 18,
        compiler_params=pltpu.CompilerParams(collective_id=0, has_side_effects=True, vmem_limit_bytes=67043328),
        cost_estimate=pl.CostEstimate(flops=2 * 10 ** 9, bytes_accessed=30 * 10 ** 6, transcendentals=10 ** 6),
    )(o.reshape(16, n_batch, HEAD), ml, hidden, w_o, w_gate, w_up, w_down, mlp_norm.reshape(-1, HEAD))


def solution(mesh):
    cache_spec = P('dp', 'sp', 'tp', None)
    col_spec = P(None, 'tp')
    row_spec = P('tp', None)
    in_specs = (P(None, 'dp', None), P('dp'), cache_spec, cache_spec, col_spec, col_spec, col_spec, row_spec,
                col_spec, col_spec, row_spec, P(), P(), P(), P())
    out_specs = (P(None, 'dp', None), cache_spec, cache_spec)

    def shard_body(hidden, start_pos, k_cache, v_cache, w_q, w_k, w_v, w_o, w_gate, w_up, w_down, attn_norm, mlp_norm, q_gain, k_gain):
        flat = (k_cache.shape[0], k_cache.shape[1] * k_cache.shape[2], k_cache.shape[3])
        o, ml, k_out, v_out = attend(start_pos, hidden, w_q, w_k, w_v, k_cache.reshape(flat), v_cache.reshape(flat), attn_norm, q_gain, k_gain)
        out = layer(o, ml, hidden, w_o, w_gate, w_up, w_down, mlp_norm)
        return out, k_out.reshape(k_cache.shape), v_out.reshape(v_cache.shape)

    return jax.shard_map(shard_body, mesh=mesh, in_specs=in_specs, out_specs=out_specs, check_vma=False)
```

```python
import functools
import jax
import jax.numpy as jnp
import numpy as np
from jax import lax
from jax.experimental import pallas as pl
from jax.experimental.pallas import tpu as pltpu
from jax.sharding import PartitionSpec as P

ROPE_BASE = 1000000.0
NORM_EPS = 1e-06
NEG_BIG = -1e30
HEAD = 128
CHUNK = 8


def gain_row(ref):
    g = ref[...].astype(jnp.float32)
    return jnp.concatenate([g[j:j + 1] for j in range(g.shape[0])], axis=1)


def attend_kernel(start_hbm, hid_hbm, wq_hbm, wk_hbm, wv_hbm, kc_hbm, vc_hbm, an_hbm, qg_hbm, kg_hbm, freq_hbm,
                  o_hbm, ml_hbm, ko_hbm, vo_hbm,
                  start_ref, an_ref, qg_ref, kg_ref, freq_ref, o_ref, ml_ref, s_sem, o_sem,
                  hid, wq, wk, wv, kbuf, vbuf, nrm, raw, q_s, k_s, v_s, pos_s, ml_s, key_s, sc_s, pr_s,
                  w_sem, h_sem, kin_sem, vin_sem, kout_sem, vout_sem):
    n_steps, n_batch, width = hid.shape
    rows = kbuf.shape[1]
    seq_blk = rows // 2
    n_chunk = n_batch // CHUNK
    n_q = wq.shape[1] // HEAD
    n_kv = wk.shape[1] // HEAD
    blk_start = lax.axis_index('sp') * seq_blk
    scale = HEAD ** -0.5

    small = [pltpu.make_async_copy(a, b, s_sem.at[j]) for j, (a, b) in enumerate((
        (start_hbm, start_ref), (freq_hbm, freq_ref), (an_hbm, an_ref), (qg_hbm, qg_ref), (kg_hbm, kg_ref)))]
    hid_cp = pltpu.make_async_copy(hid_hbm, hid, h_sem)
    for cp in small[:2] + [hid_cp] + small[2:]:
        cp.start()
    w_cps = [pltpu.make_async_copy(a, b, w_sem.at[j]) for j, (a, b) in enumerate(((wq_hbm, wq), (wk_hbm, wk), (wv_hbm, wv)))]
    for cp in w_cps:
        cp.start()

    def kv_in(c):
        sl = pl.ds(c * CHUNK, CHUNK)
        return (pltpu.make_async_copy(kc_hbm.at[sl], kbuf.at[sl], kin_sem.at[c]),
                pltpu.make_async_copy(vc_hbm.at[sl], vbuf.at[sl], vin_sem.at[c]))

    def kv_out(c):
        sl = pl.ds(c * CHUNK, CHUNK)
        return (pltpu.make_async_copy(kbuf.at[sl], ko_hbm.at[sl], kout_sem.at[c]),
                pltpu.make_async_copy(vbuf.at[sl], vo_hbm.at[sl], vout_sem.at[c]))

    @pl.loop(0, n_chunk)
    def _(c):
        a, b = kv_in(c)
        a.start()
        b.start()

    for cp in small:
        cp.wait()

    @pl.loop(0, n_batch)
    def _(b):
        pos_s[pl.ds(b, 1), :] = jnp.full((1, HEAD), start_ref[b].astype(jnp.float32), jnp.float32)

    freq = freq_ref[0:1, :]
    sign = freq_ref[1:2, :]
    ang = pos_s[...] * freq
    cos0 = jnp.cos(ang)
    sin0 = jnp.sin(ang)

    r_id = lax.broadcasted_iota(jnp.int32, (16, rows), 0)
    c_id = lax.broadcasted_iota(jnp.int32, (16, rows), 1)
    same = ((r_id % 4) // 2) == (c_id % 2)
    key_s[...] = jnp.where(same, c_id // 2 - r_id // 4, 1 << 20)

    hid_cp.wait()
    gain = gain_row(an_ref)
    for i in range(n_steps):
        for h in range(0, n_batch, 32):
            x = hid[i, h:h + 32, :].astype(jnp.float32)
            inv = lax.rsqrt(jnp.mean(x * x, axis=-1, keepdims=True) + NORM_EPS)
            nrm[i * n_batch + h:i * n_batch + h + 32, :] = (x * inv * gain).astype(jnp.bfloat16)

    def rope(x, g, cos, sin):
        inv = lax.rsqrt(jnp.mean(x * x, axis=-1, keepdims=True) + NORM_EPS)
        y = x * inv * g
        return y * cos + pltpu.roll(y, HEAD // 2, 1) * sin

    tabs = []
    for i in range(n_steps):
        if i == 0:
            c, s = cos0, sin0
        else:
            ci, si = jnp.cos(freq * float(i)), jnp.sin(freq * float(i))
            c, s = cos0 * ci - sin0 * si, sin0 * ci + cos0 * si
        pos_s_c, pos_s_s = c, s * sign
        tabs.append((pos_s_c, pos_s_s))

    for cp in w_cps:
        cp.wait()
    qg = qg_ref[...].astype(jnp.float32)
    kg = kg_ref[...].astype(jnp.float32)
    nq = n_q * HEAD
    nk = n_kv * HEAD
    raw[:, :nq] = jnp.dot(nrm[...], wq[...], preferred_element_type=jnp.float32)
    raw[:, nq:nq + nk] = jnp.dot(nrm[...], wk[...], preferred_element_type=jnp.float32)
    raw[:, nq + nk:] = jnp.dot(nrm[...], wv[...], preferred_element_type=jnp.float32)
    for i in range(n_steps):
        rs = slice(i * n_batch, (i + 1) * n_batch)
        cos, sin = tabs[i]
        for h in range(n_q):
            q_s[pl.ds(i * n_q + h, n_batch, stride=n_steps * n_q), :] = rope(raw[rs, h * HEAD:(h + 1) * HEAD], qg, cos, sin)
        for h in range(n_kv):
            k_s[pl.ds(i * n_kv + h, n_batch, stride=n_steps * n_kv), :] = rope(
                raw[rs, nq + h * HEAD:nq + (h + 1) * HEAD], kg, cos, sin)
            v_s[pl.ds(i * n_kv + h, n_batch, stride=n_steps * n_kv), :] = raw[rs, nq + nk + h * HEAD:nq + nk + (h + 1) * HEAD]

    row32 = lax.broadcasted_iota(jnp.int32, (32, HEAD), 0)
    eye_r = lax.broadcasted_iota(jnp.int32, (16, HEAD), 0)
    eye_c = lax.broadcasted_iota(jnp.int32, (16, HEAD), 1)
    eye_m = eye_r == eye_c
    eye_l = eye_r + 16 == eye_c
    zero24 = jnp.zeros((24, HEAD), jnp.float32)

    @pl.loop(0, n_chunk)
    def _(c):
        a, b = kv_in(c)
        a.wait()
        b.wait()
        lps = []
        for u in range(CHUNK):
            bb = c * CHUNK + u
            lp = start_ref[bb] - blk_start
            lps.append(lp)
            base = jnp.clip((lp // 8) * 8, 0, seq_blk - 16)
            rel = (lp - base) * 2
            shift = jnp.bitwise_and(rel, 31)
            hit = (row32 >= rel) & (row32 < rel + 8)
            win = pl.ds(pl.multiple_of(base * 2, 16), 32)
            for src, dst in ((k_s, kbuf), (v_s, vbuf)):
                new = src[pl.ds(pl.multiple_of(bb * 8, 8), 8), :]
                new = pltpu.roll(jnp.concatenate([new, zero24], axis=0), shift, 0)
                old = dst[bb, win, :].astype(jnp.float32)
                dst[bb, win, :] = jnp.where(hit, new, old).astype(jnp.bfloat16)
        for u in range(CHUNK):
            bb = c * CHUNK + u
            q = q_s[pl.ds(pl.multiple_of(bb * 16, 16), 16), :].astype(jnp.bfloat16)
            sc_s[u] = lax.dot_general(q, kbuf[bb], (((1,), (1,)), ((), ())), preferred_element_type=jnp.float32)
        tops = []
        for u in range(CHUNK):
            s = jnp.where(key_s[...] <= lps[u], sc_s[u] * scale, NEG_BIG)
            sc_s[u] = s
            tops.append(jnp.maximum(jnp.max(s, axis=-1, keepdims=True), 0.5 * NEG_BIG))
        sums = []
        for u in range(CHUNK):
            p = jnp.exp(sc_s[u] - tops[u])
            sums.append(jnp.sum(p, axis=-1, keepdims=True))
            pr_s[u] = p.astype(jnp.bfloat16)
        for u in range(CHUNK):
            bb = c * CHUNK + u
            o_ref[pl.ds(bb, 16, stride=n_batch), :] = jnp.dot(pr_s[u], vbuf[bb], preferred_element_type=jnp.float32)
        for u in range(CHUNK):
            ml = jnp.where(eye_m, tops[u], 0.0) + jnp.where(eye_l, sums[u], 0.0)
            ml_s[pl.ds(c * CHUNK + u, 1), :] = jnp.sum(ml, axis=0, keepdims=True)
        a, b = kv_out(c)
        a.start()
        b.start()

    for i in range(n_steps):
        ml = ml_s[...]
        ml_ref[i] = ml if i == 0 else pltpu.roll(ml, HEAD - 4 * i, 1)
    outs = [pltpu.make_async_copy(o_ref, o_hbm, o_sem.at[0]), pltpu.make_async_copy(ml_ref, ml_hbm, o_sem.at[1])]
    for cp in outs:
        cp.start()

    @pl.loop(0, n_chunk)
    def _(c):
        a, b = kv_out(c)
        a.wait()
        b.wait()

    for cp in outs:
        cp.wait()


def attend(start_pos, hidden, w_q, w_k, w_v, k_cache, v_cache, attn_norm, q_gain, k_gain):
    n_steps, n_batch, width = hidden.shape
    rows = k_cache.shape[1]
    n_chunk = n_batch // CHUNK
    nq, nk = w_q.shape[1], w_k.shape[1]
    half = HEAD // 2
    f = ROPE_BASE ** (-(np.arange(half, dtype=np.float64) * (2.0 / HEAD)))
    freq = np.stack([np.concatenate([f, f]), np.concatenate([-np.ones(half), np.ones(half)])]).astype(np.float32)
    anyspec = pl.BlockSpec(memory_space=pltpu.HBM)
    return pl.pallas_call(
        attend_kernel,
        name='attend',
        out_shape=(jax.ShapeDtypeStruct((16 * n_batch, HEAD), jnp.float32),
                   jax.ShapeDtypeStruct((n_steps, n_batch, HEAD), jnp.float32),
                   jax.ShapeDtypeStruct(k_cache.shape, jnp.bfloat16),
                   jax.ShapeDtypeStruct(v_cache.shape, jnp.bfloat16)),
        in_specs=[anyspec] * 11,
        out_specs=(anyspec,) * 4,
        scratch_shapes=[
            pltpu.SMEM(start_pos.shape, jnp.int32),
            pltpu.VMEM((width // HEAD, HEAD), jnp.bfloat16),
            pltpu.VMEM((1, HEAD), jnp.bfloat16),
            pltpu.VMEM((1, HEAD), jnp.bfloat16),
            pltpu.VMEM((2, HEAD), jnp.float32),
            pltpu.VMEM((16 * n_batch, HEAD), jnp.float32),
            pltpu.VMEM((n_steps, n_batch, HEAD), jnp.float32),
            pltpu.SemaphoreType.DMA((5,)),
            pltpu.SemaphoreType.DMA((2,)),
            pltpu.VMEM(hidden.shape, jnp.bfloat16),
            pltpu.VMEM(w_q.shape, jnp.bfloat16),
            pltpu.VMEM(w_k.shape, jnp.bfloat16),
            pltpu.VMEM(w_v.shape, jnp.bfloat16),
            pltpu.VMEM(k_cache.shape, jnp.bfloat16),
            pltpu.VMEM(v_cache.shape, jnp.bfloat16),
            pltpu.VMEM((n_steps * n_batch, width), jnp.bfloat16),
            pltpu.VMEM((n_steps * n_batch, nq + 2 * nk), jnp.float32),
            pltpu.VMEM((n_batch * 16, HEAD), jnp.float32),
            pltpu.VMEM((n_batch * 8, HEAD), jnp.float32),
            pltpu.VMEM((n_batch * 8, HEAD), jnp.float32),
            pltpu.VMEM((n_batch, HEAD), jnp.float32),
            pltpu.VMEM((n_batch, HEAD), jnp.float32),
            pltpu.VMEM((16, rows), jnp.int32),
            pltpu.VMEM((CHUNK, 16, rows), jnp.float32),
            pltpu.VMEM((CHUNK, 16, rows), jnp.bfloat16),
            pltpu.SemaphoreType.DMA((3,)),
            pltpu.SemaphoreType.DMA,
            pltpu.SemaphoreType.DMA((n_chunk,)),
            pltpu.SemaphoreType.DMA((n_chunk,)),
            pltpu.SemaphoreType.DMA((n_chunk,)),
            pltpu.SemaphoreType.DMA((n_chunk,)),
        ],
        compiler_params=pltpu.CompilerParams(vmem_limit_bytes=67043328),
        cost_estimate=pl.CostEstimate(flops=2 * 10 ** 9, bytes_accessed=40 * 10 ** 6, transcendentals=10 ** 6),
    )(start_pos, hidden, w_q, w_k, w_v, k_cache, v_cache, attn_norm.reshape(-1, HEAD), q_gain.reshape(1, -1), k_gain.reshape(1, -1), jnp.asarray(freq))


N_COL = 4
N_HALF = 4
LAG = 5
LAG_Y = 8
TILES = 3
SERVE = 1


def layer_kernel(o_hbm, ml_hbm, hid_hbm, wo_hbm, wg_hbm, wu_hbm, wd_hbm, mn_hbm, out_hbm,
                 o_own, ml_own, mn_ref, out_ref, oa, mla, om, mlm, oy, mly, own, ml_mine, attn, hid, wo, wg, wu, wd,
                 p1, e1, x1, r1, m_s, act, p2, e2, x2, ob, yb, pb, pf,
                 ld_sem, out_sem, w_sem, a1_snd, a1_rcv, a2_snd, a2_rcv, es1, er1, xs1, xr1, ts1, tr1,
                 es2, er2, xs2, xr2, ts2, tr2, ps, pr, ys, yr, fs, fr):
    n_steps, n_batch, width = hid_hbm.shape
    n_half = n_batch // N_HALF
    n_col = width // N_COL
    n_piece = N_COL * N_HALF
    tp = lax.axis_index('tp')
    sp = lax.axis_index('sp')
    core = sp % 2
    row = sp // 2
    partner = {'sp': row * 2 + 1 - core}
    across = {'sp': (1 - row) * 2 + core}
    is_mid = (tp % 3) != 0
    is_end = (tp % 3) == 0
    to_mid = {'tp': (tp + 3) // 3}
    to_end = {'tp': (tp - 1) * 3}
    to_other = {'tp': 3 - tp}
    mesh_id = pl.DeviceIdType.MESH

    def remote(src, dst, ssem, rsem, dev):
        return pltpu.make_async_remote_copy(src_ref=src, dst_ref=dst, send_sem=ssem, recv_sem=rsem, device_id=dev, device_id_type=mesh_id)

    send_to = 1 - core
    o_cps, ml_cps = [], []
    for q, step in enumerate(((1 - row) * 2 + send_to, row * 2 + send_to, (1 - row) * 2 + core, row * 2 + core)):
        o_cps.append(pltpu.make_async_copy(o_hbm.at[pl.ds(step * 4, 4)], o_own.at[pl.ds(step * 4, 4)], ld_sem.at[q]))
    ml_cp = pltpu.make_async_copy(ml_hbm, ml_own, ld_sem.at[4])
    hid_cp = pltpu.make_async_copy(hid_hbm.at[sp], hid, ld_sem.at[5])
    mn_cp = pltpu.make_async_copy(mn_hbm, mn_ref, ld_sem.at[6])
    lds = [ml_cp] + o_cps + [hid_cp, mn_cp]
    wts = [pltpu.make_async_copy(a, b, w_sem.at[j]) for j, (a, b) in enumerate(((wo_hbm, wo), (wg_hbm, wg), (wu_hbm, wu), (wd_hbm, wd)))]
    for cp in lds:
        cp.start()

    barrier = pltpu.get_barrier_semaphore()
    for dev in (partner, across):
        pl.semaphore_signal(barrier, inc=1, device_id=dev, device_id_type=mesh_id)

    @pl.when(is_mid)
    def _():
        pl.semaphore_signal(barrier, inc=1, device_id=to_end, device_id_type=mesh_id)
        pl.semaphore_signal(barrier, inc=1, device_id=to_other, device_id_type=mesh_id)
        pl.semaphore_wait(barrier, 4)

    @pl.when(is_end)
    def _():
        pl.semaphore_signal(barrier, inc=1, device_id=to_mid, device_id_type=mesh_id)
        pl.semaphore_wait(barrier, 3)

    ml_cp.wait()
    a1 = []
    for q, jy in enumerate((1 - row, row)):
        step = jy * 2 + 1 - core
        o_cps[q].wait()
        a1.append((remote(ml_own.at[step], mla.at[q], a1_snd.at[2 * q], a1_rcv.at[2 * q], partner),
                   remote(o_own.at[pl.ds(step * 4, 4)], oa.at[q], a1_snd.at[2 * q + 1], a1_rcv.at[2 * q + 1], partner)))
        for cp in a1[-1]:
            cp.start()

    lane = lax.broadcasted_iota(jnp.int32, (n_half, HEAD), 1)

    def weigh(ma, mb):
        top = jnp.maximum(ma, mb)
        wa, wb = jnp.exp(ma - top), jnp.exp(mb - top)
        tot = pltpu.roll(ma, HEAD - 16, 1) * wa + pltpu.roll(mb, HEAD - 16, 1) * wb
        return top, wa, wb, tot

    def merge_core(q, step, dst, mldst):
        for cp in a1[q]:
            cp.wait()
        for h in range(N_HALF):
            rs = pl.ds(h * n_half, n_half)
            top, wa, wb, tot = weigh(ml_own[step, rs, :], mla[q, rs, :])
            mldst[h] = jnp.where(lane < 16, top, pltpu.roll(tot, 16, 1))
            for k in range(4):
                dst[h, k] = o_own[step * 4 + k, rs, :] * wa[:, k:k + 1] + oa[q, k, rs, :] * wb[:, k:k + 1]

    for cp in lds[3:]:
        cp.wait()
    merge_core(0, (1 - row) * 2 + core, om, mlm)
    a2 = []
    for h in range(N_HALF):
        a2.append((remote(mlm.at[h], mly.at[h], a2_snd.at[2 * h], a2_rcv.at[2 * h], across),
                   remote(om.at[h], oy.at[h], a2_snd.at[2 * h + 1], a2_rcv.at[2 * h + 1], across)))
        for cp in a2[-1]:
            cp.start()
    for cp in wts:
        cp.start()
    merge_core(1, row * 2 + core, own, ml_mine)
    wts[0].wait()

    e1_cp = lambda t: remote(p1.at[t], e1.at[t], es1.at[t], er1.at[t], to_mid)
    x1_cp = lambda t: remote(p1.at[t], x1.at[t], xs1.at[t], xr1.at[t], to_other)
    t1_cp = lambda t: remote(r1.at[t], r1.at[t], ts1.at[t], tr1.at[t], to_end)
    e2_cp = lambda t: remote(p2.at[t], e2.at[t], es2.at[t], er2.at[t], to_mid)
    x2_cp = lambda t: remote(p2.at[t], x2.at[t], xs2.at[t], xr2.at[t], to_other)
    t2_cp = lambda t: remote(ob.at[t], ob.at[t], ts2.at[t], tr2.at[t], to_end)
    p_cp = lambda t: remote(ob.at[t], pb.at[t], ps.at[t], pr.at[t], partner)
    y_cp = lambda t: remote(ob.at[t], yb.at[t], ys.at[t], yr.at[t], across)
    f_cp = lambda t: remote(yb.at[t], pf.at[t], fs.at[t], fr.at[t], partner)

    def spread(h, lhs, w, dst, cp, after=None):
        wide = width // 2
        per = N_COL // 2
        for j in range(2):
            d = jnp.dot(lhs, w[:, j * wide:(j + 1) * wide], preferred_element_type=jnp.float32)
            for n in range(per):
                dst[h * N_COL + j * per + n] = d[:, n * n_col:(n + 1) * n_col]

            @pl.when(is_end)
            def _():
                @pl.loop(h * N_COL + j * per, h * N_COL + (j + 1) * per)
                def _(t):
                    cp(t).start()

            if after is not None:
                after(h)

    for h in range(N_HALF):
        for cp in a2[h]:
            cp.wait()
        _, wa, wb, tot = weigh(ml_mine[h], mly[h])
        inv = 1.0 / tot
        for k in range(4):
            val = (own[h, k] * wa[:, k:k + 1] + oy[h, k] * wb[:, k:k + 1]) * inv[:, k:k + 1]
            attn[h, :, k * HEAD:(k + 1) * HEAD] = val.astype(jnp.bfloat16)

        spread(h, attn[h], wo, p1, e1_cp)

    def sum_step(s):
        @pl.when(s < n_piece)
        def _():
            e1_cp(s).wait_recv()
            p1[s] = p1[s] + e1[s]
            x1_cp(s).start()

        @pl.when(s >= LAG)
        def _():
            t = s - LAG
            h = t // N_COL
            rs = pl.ds(pl.multiple_of(h * n_half, n_half), n_half)
            cs = pl.ds(pl.multiple_of((t - h * N_COL) * n_col, n_col), n_col)
            x1_cp(t).wait_recv()
            r = hid[rs, cs].astype(jnp.float32) + (p1[t] + x1[t])
            r1[t] = r.astype(jnp.bfloat16).astype(jnp.float32)
            t1_cp(t).start()

    def sum_steps(lo, hi):
        @pl.when(is_mid)
        def _():
            pl.loop(lo, hi)(sum_step)

    def end_recv(lo, hi):
        @pl.when(is_end)
        def _():
            @pl.loop(lo, hi)
            def _(t):
                t1_cp(t).wait_recv()

    def share(t):
        p_cp(t).start()
        y_cp(t).start()

    def relay(t):
        y_cp(t).wait_recv()
        f_cp(t).start()

    def share_step(s):
        @pl.when(s < n_piece)
        def _():
            e2_cp(s).wait_recv()
            p2[s] = p2[s] + e2[s]
            x2_cp(s).start()

        @pl.when((s >= LAG) & (s < n_piece + LAG))
        def _():
            t = s - LAG
            x2_cp(t).wait_recv()
            o = r1[t] + (p2[t] + x2[t])
            ob[t] = o.astype(jnp.bfloat16).astype(jnp.float32)
            t2_cp(t).start()
            share(t)

        @pl.when(s >= LAG + LAG_Y)
        def _():
            relay(s - LAG - LAG_Y)


    def share_steps(lo, hi):
        @pl.when(is_mid)
        def _():
            pl.loop(lo, hi)(share_step)

    gain = gain_row(mn_ref)
    ffn = wg.shape[1]
    blk = ffn // TILES
    done = [0, 0]

    def serve(h):
        for _ in range(SERVE):
            if done[0] < n_piece + LAG:
                sum_steps(done[0], done[0] + 1)
                done[0] += 1
            elif done[1] < h * N_COL:
                share_steps(done[1], done[1] + 1)
                done[1] += 1

    for h in range(N_HALF):
        stop = max(done[0], (h + 1) * N_COL + LAG)
        if stop > done[0]:
            sum_steps(done[0], stop)
            done[0] = stop
        end_recv(h * N_COL, (h + 1) * N_COL)
        sq = jnp.zeros((n_half, 1), jnp.float32)
        for n in range(N_COL):
            r = r1[h * N_COL + n]
            sq = sq + jnp.sum(r * r, axis=-1, keepdims=True)
        inv = lax.rsqrt(sq / width + NORM_EPS)
        for n in range(N_COL):
            m_s[:, n * n_col:(n + 1) * n_col] = (r1[h * N_COL + n] * inv * gain[:, n * n_col:(n + 1) * n_col]).astype(jnp.bfloat16)
        if h == 0:
            wts[1].wait()
            wts[2].wait()
        for n in range(TILES):
            cs = slice(n * blk, (n + 1) * blk)
            g = jnp.dot(m_s[...], wg[:, cs], preferred_element_type=jnp.float32)
            u = jnp.dot(m_s[...], wu[:, cs], preferred_element_type=jnp.float32)
            act[:, cs] = (jax.nn.silu(g) * u).astype(jnp.bfloat16)
            serve(h)
        if h == 0:
            wts[3].wait()
        spread(h, act[...], wd, p2, e2_cp, serve)

    share_steps(done[1], n_piece + LAG + LAG_Y)

    @pl.when(is_end)
    def _():
        @pl.loop(0, n_piece + LAG_Y)
        def _(s):
            @pl.when(s < n_piece)
            def _():
                t2_cp(s).wait_recv()
                share(s)

            @pl.when(s >= LAG_Y)
            def _():
                relay(s - LAG_Y)

    def put(j, t, val):
        h = t // N_COL
        rs = pl.ds(pl.multiple_of(h * n_half, n_half), n_half)
        cs = pl.ds(pl.multiple_of((t - h * N_COL) * n_col, n_col), n_col)
        out_ref[j, rs, cs] = val.astype(jnp.bfloat16)

    def leave(j, h, k):
        rs = pl.ds(h * n_half, n_half)
        return pltpu.make_async_copy(out_ref.at[j, rs], out_hbm.at[j, rs], out_sem.at[h * 4 + k])

    homes = (sp, row * 2 + 1 - core, (1 - row) * 2 + core, (1 - row) * 2 + 1 - core)
    for h in range(N_HALF):
        @pl.loop(h * N_COL, (h + 1) * N_COL)
        def _(t):
            put(homes[0], t, ob[t])
            p_cp(t).wait_recv()
            put(homes[1], t, pb[t])
            put(homes[2], t, yb[t])
            f_cp(t).wait_recv()
            put(homes[3], t, pf[t])

        for k in range(4):
            leave(homes[k], h, k).start()

    @pl.loop(0, n_piece)
    def _(t):
        p_cp(t).wait_send()
        y_cp(t).wait_send()
        f_cp(t).wait_send()

        @pl.when(is_mid)
        def _():
            x1_cp(t).wait_send()
            t1_cp(t).wait_send()
            x2_cp(t).wait_send()
            t2_cp(t).wait_send()

        @pl.when(is_end)
        def _():
            e1_cp(t).wait_send()
            e2_cp(t).wait_send()

    for h in range(N_HALF):
        for k in range(4):
            leave(homes[k], h, k).wait()


def layer(o, ml, hidden, w_o, w_gate, w_up, w_down, mlp_norm):
    n_steps, n_batch, width = hidden.shape
    n_half = n_batch // N_HALF
    n_col = width // N_COL
    n_piece = N_COL * N_HALF
    vm = pl.BlockSpec(memory_space=pltpu.VMEM)
    anyspec = pl.BlockSpec(memory_space=pltpu.HBM)
    f32, bf16 = jnp.float32, jnp.bfloat16
    piece = pltpu.VMEM((n_piece, n_half, n_col), f32)
    dma = pltpu.SemaphoreType.DMA
    return pl.pallas_call(
        layer_kernel,
        name='layer',
        out_shape=jax.ShapeDtypeStruct(hidden.shape, bf16),
        in_specs=[anyspec] * 8,
        out_specs=anyspec,
        scratch_shapes=[
            pltpu.VMEM((16, n_batch, HEAD), f32),
            pltpu.VMEM((4, n_batch, HEAD), f32),
            pltpu.VMEM((width // HEAD, HEAD), bf16),
            pltpu.VMEM(hidden.shape, bf16),
            pltpu.VMEM((2, 4, n_batch, HEAD), f32),
            pltpu.VMEM((2, n_batch, HEAD), f32),
            pltpu.VMEM((N_HALF, 4, n_half, HEAD), f32),
            pltpu.VMEM((N_HALF, n_half, HEAD), f32),
            pltpu.VMEM((N_HALF, 4, n_half, HEAD), f32),
            pltpu.VMEM((N_HALF, n_half, HEAD), f32),
            pltpu.VMEM((N_HALF, 4, n_half, HEAD), f32),
            pltpu.VMEM((N_HALF, n_half, HEAD), f32),
            pltpu.VMEM((N_HALF, n_half, 4 * HEAD), bf16),
            pltpu.VMEM((n_batch, width), bf16),
            pltpu.VMEM(w_o.shape, bf16),
            pltpu.VMEM(w_gate.shape, bf16),
            pltpu.VMEM(w_up.shape, bf16),
            pltpu.VMEM(w_down.shape, bf16),
            piece, piece, piece, piece,
            pltpu.VMEM((n_half, width), bf16),
            pltpu.VMEM((n_half, w_gate.shape[1]), bf16),
            piece, piece, piece, piece, piece, piece, piece,
            dma((7,)), dma((4 * N_HALF,)), dma((4,)), dma((4,)), dma((4,)), dma((2 * N_HALF,)), dma((2 * N_HALF,)),
        ] + [dma((n_piece,))] * 18,
        compiler_params=pltpu.CompilerParams(collective_id=0, has_side_effects=True, vmem_limit_bytes=67043328),
        cost_estimate=pl.CostEstimate(flops=2 * 10 ** 9, bytes_accessed=30 * 10 ** 6, transcendentals=10 ** 6),
    )(o.reshape(16, n_batch, HEAD), ml, hidden, w_o, w_gate, w_up, w_down, mlp_norm.reshape(-1, HEAD))


def solution(mesh):
    cache_spec = P('dp', 'sp', 'tp', None)
    col_spec = P(None, 'tp')
    row_spec = P('tp', None)
    in_specs = (P(None, 'dp', None), P('dp'), cache_spec, cache_spec, col_spec, col_spec, col_spec, row_spec,
                col_spec, col_spec, row_spec, P(), P(), P(), P())
    out_specs = (P(None, 'dp', None), cache_spec, cache_spec)

    def shard_body(hidden, start_pos, k_cache, v_cache, w_q, w_k, w_v, w_o, w_gate, w_up, w_down, attn_norm, mlp_norm, q_gain, k_gain):
        flat = (k_cache.shape[0], k_cache.shape[1] * k_cache.shape[2], k_cache.shape[3])
        o, ml, k_out, v_out = attend(start_pos, hidden, w_q, w_k, w_v, k_cache.reshape(flat), v_cache.reshape(flat), attn_norm, q_gain, k_gain)
        out = layer(o, ml, hidden, w_o, w_gate, w_up, w_down, mlp_norm)
        return out, k_out.reshape(k_cache.shape), v_out.reshape(v_cache.shape)

    return jax.shard_map(shard_body, mesh=mesh, in_specs=in_specs, out_specs=out_specs, check_vma=False)
```

```python
import functools
import jax
import jax.numpy as jnp
import numpy as np
from jax import lax
from jax.experimental import pallas as pl
from jax.experimental.pallas import tpu as pltpu
from jax.sharding import PartitionSpec as P

ROPE_BASE = 1000000.0
NORM_EPS = 1e-06
NEG_BIG = -1e30
HEAD = 128
CHUNK = 8


def gain_row(ref):
    g = ref[...].astype(jnp.float32)
    return jnp.concatenate([g[j:j + 1] for j in range(g.shape[0])], axis=1)


def attend_kernel(start_hbm, hid_hbm, wq_hbm, wk_hbm, wv_hbm, kc_hbm, vc_hbm, an_hbm, qg_hbm, kg_hbm, freq_hbm,
                  o_hbm, ml_hbm, ko_hbm, vo_hbm,
                  start_ref, an_ref, qg_ref, kg_ref, freq_ref, o_ref, ml_ref, s_sem, o_sem,
                  hid, wq, wk, wv, kbuf, vbuf, nrm, raw, q_s, k_s, v_s, pos_s, ml_s, key_s, sc_s, pr_s,
                  w_sem, h_sem, kin_sem, vin_sem, kout_sem, vout_sem):
    n_steps, n_batch, width = hid.shape
    rows = kbuf.shape[1]
    seq_blk = rows // 2
    n_chunk = n_batch // CHUNK
    n_q = wq.shape[1] // HEAD
    n_kv = wk.shape[1] // HEAD
    blk_start = lax.axis_index('sp') * seq_blk
    scale = HEAD ** -0.5

    small = [pltpu.make_async_copy(a, b, s_sem.at[j]) for j, (a, b) in enumerate((
        (start_hbm, start_ref), (freq_hbm, freq_ref), (an_hbm, an_ref), (qg_hbm, qg_ref), (kg_hbm, kg_ref)))]
    hid_cp = pltpu.make_async_copy(hid_hbm, hid, h_sem)
    for cp in small[:2] + [hid_cp] + small[2:]:
        cp.start()
    w_cps = [pltpu.make_async_copy(a, b, w_sem.at[j]) for j, (a, b) in enumerate(((wq_hbm, wq), (wk_hbm, wk), (wv_hbm, wv)))]
    for cp in w_cps:
        cp.start()

    def kv_in(c):
        sl = pl.ds(c * CHUNK, CHUNK)
        return (pltpu.make_async_copy(kc_hbm.at[sl], kbuf.at[sl], kin_sem.at[c]),
                pltpu.make_async_copy(vc_hbm.at[sl], vbuf.at[sl], vin_sem.at[c]))

    def kv_out(c):
        sl = pl.ds(c * CHUNK, CHUNK)
        return (pltpu.make_async_copy(kbuf.at[sl], ko_hbm.at[sl], kout_sem.at[c]),
                pltpu.make_async_copy(vbuf.at[sl], vo_hbm.at[sl], vout_sem.at[c]))

    @pl.loop(0, n_chunk)
    def _(c):
        a, b = kv_in(c)
        a.start()
        b.start()

    for cp in small:
        cp.wait()

    @pl.loop(0, n_batch)
    def _(b):
        pos_s[pl.ds(b, 1), :] = jnp.full((1, HEAD), start_ref[b].astype(jnp.float32), jnp.float32)

    freq = freq_ref[0:1, :]
    sign = freq_ref[1:2, :]
    ang = pos_s[...] * freq
    cos0 = jnp.cos(ang)
    sin0 = jnp.sin(ang)

    r_id = lax.broadcasted_iota(jnp.int32, (16, rows), 0)
    c_id = lax.broadcasted_iota(jnp.int32, (16, rows), 1)
    same = ((r_id % 4) // 2) == (c_id % 2)
    key_s[...] = jnp.where(same, c_id // 2 - r_id // 4, 1 << 20)

    hid_cp.wait()
    gain = gain_row(an_ref)
    for i in range(n_steps):
        for h in range(0, n_batch, 32):
            x = hid[i, h:h + 32, :].astype(jnp.float32)
            inv = lax.rsqrt(jnp.mean(x * x, axis=-1, keepdims=True) + NORM_EPS)
            nrm[i * n_batch + h:i * n_batch + h + 32, :] = (x * inv * gain).astype(jnp.bfloat16)

    def rope(x, g, cos, sin):
        inv = lax.rsqrt(jnp.mean(x * x, axis=-1, keepdims=True) + NORM_EPS)
        y = x * inv * g
        return y * cos + pltpu.roll(y, HEAD // 2, 1) * sin

    tabs = []
    for i in range(n_steps):
        if i == 0:
            c, s = cos0, sin0
        else:
            ci, si = jnp.cos(freq * float(i)), jnp.sin(freq * float(i))
            c, s = cos0 * ci - sin0 * si, sin0 * ci + cos0 * si
        pos_s_c, pos_s_s = c, s * sign
        tabs.append((pos_s_c, pos_s_s))

    for cp in w_cps:
        cp.wait()
    qg = qg_ref[...].astype(jnp.float32)
    kg = kg_ref[...].astype(jnp.float32)
    nq = n_q * HEAD
    nk = n_kv * HEAD
    raw[:, :nq] = jnp.dot(nrm[...], wq[...], preferred_element_type=jnp.float32)
    raw[:, nq:nq + nk] = jnp.dot(nrm[...], wk[...], preferred_element_type=jnp.float32)
    raw[:, nq + nk:] = jnp.dot(nrm[...], wv[...], preferred_element_type=jnp.float32)
    for i in range(n_steps):
        rs = slice(i * n_batch, (i + 1) * n_batch)
        cos, sin = tabs[i]
        for h in range(n_q):
            q_s[pl.ds(i * n_q + h, n_batch, stride=n_steps * n_q), :] = rope(raw[rs, h * HEAD:(h + 1) * HEAD], qg, cos, sin)
        for h in range(n_kv):
            k_s[pl.ds(i * n_kv + h, n_batch, stride=n_steps * n_kv), :] = rope(
                raw[rs, nq + h * HEAD:nq + (h + 1) * HEAD], kg, cos, sin)
            v_s[pl.ds(i * n_kv + h, n_batch, stride=n_steps * n_kv), :] = raw[rs, nq + nk + h * HEAD:nq + nk + (h + 1) * HEAD]

    row32 = lax.broadcasted_iota(jnp.int32, (32, HEAD), 0)
    eye_r = lax.broadcasted_iota(jnp.int32, (16, HEAD), 0)
    eye_c = lax.broadcasted_iota(jnp.int32, (16, HEAD), 1)
    eye_m = eye_r == eye_c
    eye_l = eye_r + 16 == eye_c
    zero24 = jnp.zeros((24, HEAD), jnp.float32)

    @pl.loop(0, n_chunk)
    def _(c):
        a, b = kv_in(c)
        a.wait()
        b.wait()
        lps = []
        for u in range(CHUNK):
            bb = c * CHUNK + u
            lp = start_ref[bb] - blk_start
            lps.append(lp)
            base = jnp.clip((lp // 8) * 8, 0, seq_blk - 16)
            rel = (lp - base) * 2
            shift = jnp.bitwise_and(rel, 31)
            hit = (row32 >= rel) & (row32 < rel + 8)
            win = pl.ds(pl.multiple_of(base * 2, 16), 32)
            for src, dst in ((k_s, kbuf), (v_s, vbuf)):
                new = src[pl.ds(pl.multiple_of(bb * 8, 8), 8), :]
                new = pltpu.roll(jnp.concatenate([new, zero24], axis=0), shift, 0)
                old = dst[bb, win, :].astype(jnp.float32)
                dst[bb, win, :] = jnp.where(hit, new, old).astype(jnp.bfloat16)
        for u in range(CHUNK):
            bb = c * CHUNK + u
            q = q_s[pl.ds(pl.multiple_of(bb * 16, 16), 16), :].astype(jnp.bfloat16)
            sc_s[u] = lax.dot_general(q, kbuf[bb], (((1,), (1,)), ((), ())), preferred_element_type=jnp.float32)
        tops = []
        for u in range(CHUNK):
            s = jnp.where(key_s[...] <= lps[u], sc_s[u] * scale, NEG_BIG)
            sc_s[u] = s
            tops.append(jnp.maximum(jnp.max(s, axis=-1, keepdims=True), 0.5 * NEG_BIG))
        sums = []
        for u in range(CHUNK):
            p = jnp.exp(sc_s[u] - tops[u])
            sums.append(jnp.sum(p, axis=-1, keepdims=True))
            pr_s[u] = p.astype(jnp.bfloat16)
        for u in range(CHUNK):
            bb = c * CHUNK + u
            o_ref[pl.ds(bb, 16, stride=n_batch), :] = jnp.dot(pr_s[u], vbuf[bb], preferred_element_type=jnp.float32)
        for u in range(CHUNK):
            ml = jnp.where(eye_m, tops[u], 0.0) + jnp.where(eye_l, sums[u], 0.0)
            ml_s[pl.ds(c * CHUNK + u, 1), :] = jnp.sum(ml, axis=0, keepdims=True)
        a, b = kv_out(c)
        a.start()
        b.start()

    for i in range(n_steps):
        ml = ml_s[...]
        ml_ref[i] = ml if i == 0 else pltpu.roll(ml, HEAD - 4 * i, 1)
    outs = [pltpu.make_async_copy(o_ref, o_hbm, o_sem.at[0]), pltpu.make_async_copy(ml_ref, ml_hbm, o_sem.at[1])]
    for cp in outs:
        cp.start()

    @pl.loop(0, n_chunk)
    def _(c):
        a, b = kv_out(c)
        a.wait()
        b.wait()

    for cp in outs:
        cp.wait()


def attend(start_pos, hidden, w_q, w_k, w_v, k_cache, v_cache, attn_norm, q_gain, k_gain):
    n_steps, n_batch, width = hidden.shape
    rows = k_cache.shape[1]
    n_chunk = n_batch // CHUNK
    nq, nk = w_q.shape[1], w_k.shape[1]
    half = HEAD // 2
    f = ROPE_BASE ** (-(np.arange(half, dtype=np.float64) * (2.0 / HEAD)))
    freq = np.stack([np.concatenate([f, f]), np.concatenate([-np.ones(half), np.ones(half)])]).astype(np.float32)
    anyspec = pl.BlockSpec(memory_space=pltpu.HBM)
    return pl.pallas_call(
        attend_kernel,
        name='attend',
        out_shape=(jax.ShapeDtypeStruct((16 * n_batch, HEAD), jnp.float32),
                   jax.ShapeDtypeStruct((n_steps, n_batch, HEAD), jnp.float32),
                   jax.ShapeDtypeStruct(k_cache.shape, jnp.bfloat16),
                   jax.ShapeDtypeStruct(v_cache.shape, jnp.bfloat16)),
        in_specs=[anyspec] * 11,
        out_specs=(anyspec,) * 4,
        scratch_shapes=[
            pltpu.SMEM(start_pos.shape, jnp.int32),
            pltpu.VMEM((width // HEAD, HEAD), jnp.bfloat16),
            pltpu.VMEM((1, HEAD), jnp.bfloat16),
            pltpu.VMEM((1, HEAD), jnp.bfloat16),
            pltpu.VMEM((2, HEAD), jnp.float32),
            pltpu.VMEM((16 * n_batch, HEAD), jnp.float32),
            pltpu.VMEM((n_steps, n_batch, HEAD), jnp.float32),
            pltpu.SemaphoreType.DMA((5,)),
            pltpu.SemaphoreType.DMA((2,)),
            pltpu.VMEM(hidden.shape, jnp.bfloat16),
            pltpu.VMEM(w_q.shape, jnp.bfloat16),
            pltpu.VMEM(w_k.shape, jnp.bfloat16),
            pltpu.VMEM(w_v.shape, jnp.bfloat16),
            pltpu.VMEM(k_cache.shape, jnp.bfloat16),
            pltpu.VMEM(v_cache.shape, jnp.bfloat16),
            pltpu.VMEM((n_steps * n_batch, width), jnp.bfloat16),
            pltpu.VMEM((n_steps * n_batch, nq + 2 * nk), jnp.float32),
            pltpu.VMEM((n_batch * 16, HEAD), jnp.float32),
            pltpu.VMEM((n_batch * 8, HEAD), jnp.float32),
            pltpu.VMEM((n_batch * 8, HEAD), jnp.float32),
            pltpu.VMEM((n_batch, HEAD), jnp.float32),
            pltpu.VMEM((n_batch, HEAD), jnp.float32),
            pltpu.VMEM((16, rows), jnp.int32),
            pltpu.VMEM((CHUNK, 16, rows), jnp.float32),
            pltpu.VMEM((CHUNK, 16, rows), jnp.bfloat16),
            pltpu.SemaphoreType.DMA((3,)),
            pltpu.SemaphoreType.DMA,
            pltpu.SemaphoreType.DMA((n_chunk,)),
            pltpu.SemaphoreType.DMA((n_chunk,)),
            pltpu.SemaphoreType.DMA((n_chunk,)),
            pltpu.SemaphoreType.DMA((n_chunk,)),
        ],
        compiler_params=pltpu.CompilerParams(vmem_limit_bytes=67043328),
        cost_estimate=pl.CostEstimate(flops=2 * 10 ** 9, bytes_accessed=40 * 10 ** 6, transcendentals=10 ** 6),
    )(start_pos, hidden, w_q, w_k, w_v, k_cache, v_cache, attn_norm.reshape(-1, HEAD), q_gain.reshape(1, -1), k_gain.reshape(1, -1), jnp.asarray(freq))


N_COL = 4
N_HALF = 4
LAG = 5
LAG_Y = 8
TILES = 2
SERVE = 2


def layer_kernel(o_hbm, ml_hbm, hid_hbm, wo_hbm, wg_hbm, wu_hbm, wd_hbm, mn_hbm, out_hbm,
                 o_own, ml_own, mn_ref, out_ref, oa, mla, om, mlm, oy, mly, own, ml_mine, attn, hid, wo, wg, wu, wd,
                 p1, e1, x1, r1, m_s, act, p2, e2, x2, ob, yb, pb, pf,
                 ld_sem, out_sem, w_sem, a1_snd, a1_rcv, a2_snd, a2_rcv, es1, er1, xs1, xr1, ts1, tr1,
                 es2, er2, xs2, xr2, ts2, tr2, ps, pr, ys, yr, fs, fr):
    n_steps, n_batch, width = hid_hbm.shape
    n_half = n_batch // N_HALF
    n_col = width // N_COL
    n_piece = N_COL * N_HALF
    tp = lax.axis_index('tp')
    sp = lax.axis_index('sp')
    core = sp % 2
    row = sp // 2
    partner = {'sp': row * 2 + 1 - core}
    across = {'sp': (1 - row) * 2 + core}
    is_mid = (tp % 3) != 0
    is_end = (tp % 3) == 0
    to_mid = {'tp': (tp + 3) // 3}
    to_end = {'tp': (tp - 1) * 3}
    to_other = {'tp': 3 - tp}
    mesh_id = pl.DeviceIdType.MESH

    def remote(src, dst, ssem, rsem, dev):
        return pltpu.make_async_remote_copy(src_ref=src, dst_ref=dst, send_sem=ssem, recv_sem=rsem, device_id=dev, device_id_type=mesh_id)

    barrier = pltpu.get_barrier_semaphore()
    for dev in (partner, across):
        pl.semaphore_signal(barrier, inc=1, device_id=dev, device_id_type=mesh_id)

    @pl.when(is_mid)
    def _():
        pl.semaphore_signal(barrier, inc=1, device_id=to_end, device_id_type=mesh_id)
        pl.semaphore_signal(barrier, inc=1, device_id=to_other, device_id_type=mesh_id)

    @pl.when(is_end)
    def _():
        pl.semaphore_signal(barrier, inc=1, device_id=to_mid, device_id_type=mesh_id)

    send_to = 1 - core
    o_cps, ml_cps = [], []
    for q, step in enumerate(((1 - row) * 2 + send_to, row * 2 + send_to, (1 - row) * 2 + core, row * 2 + core)):
        o_cps.append(pltpu.make_async_copy(o_hbm.at[pl.ds(step * 4, 4)], o_own.at[pl.ds(step * 4, 4)], ld_sem.at[q]))
    ml_cp = pltpu.make_async_copy(ml_hbm, ml_own, ld_sem.at[4])
    hid_cp = pltpu.make_async_copy(hid_hbm.at[sp], hid, ld_sem.at[5])
    mn_cp = pltpu.make_async_copy(mn_hbm, mn_ref, ld_sem.at[6])
    lds = [ml_cp] + o_cps + [hid_cp, mn_cp]
    wts = [pltpu.make_async_copy(a, b, w_sem.at[j]) for j, (a, b) in enumerate(((wo_hbm, wo), (wg_hbm, wg), (wu_hbm, wu), (wd_hbm, wd)))]
    for cp in lds:
        cp.start()

    @pl.when(is_mid)
    def _():
        pl.semaphore_wait(barrier, 4)

    @pl.when(is_end)
    def _():
        pl.semaphore_wait(barrier, 3)

    ml_cp.wait()
    a1 = []
    for q, jy in enumerate((1 - row, row)):
        step = jy * 2 + 1 - core
        o_cps[q].wait()
        a1.append((remote(ml_own.at[step], mla.at[q], a1_snd.at[2 * q], a1_rcv.at[2 * q], partner),
                   remote(o_own.at[pl.ds(step * 4, 4)], oa.at[q], a1_snd.at[2 * q + 1], a1_rcv.at[2 * q + 1], partner)))
        for cp in a1[-1]:
            cp.start()

    lane = lax.broadcasted_iota(jnp.int32, (n_half, HEAD), 1)

    def weigh(ma, mb):
        top = jnp.maximum(ma, mb)
        wa, wb = jnp.exp(ma - top), jnp.exp(mb - top)
        tot = pltpu.roll(ma, HEAD - 16, 1) * wa + pltpu.roll(mb, HEAD - 16, 1) * wb
        return top, wa, wb, tot

    def merge_core(q, step, dst, mldst, send=None):
        for cp in a1[q]:
            cp.wait()
        for h in range(N_HALF):
            rs = pl.ds(h * n_half, n_half)
            top, wa, wb, tot = weigh(ml_own[step, rs, :], mla[q, rs, :])
            mldst[h] = jnp.where(lane < 16, top, pltpu.roll(tot, 16, 1))
            for k in range(4):
                dst[h, k] = o_own[step * 4 + k, rs, :] * wa[:, k:k + 1] + oa[q, k, rs, :] * wb[:, k:k + 1]
            if send is not None:
                for cp in send[h]:
                    cp.start()

    for cp in lds[3:]:
        cp.wait()
    a2 = []
    for h in range(N_HALF):
        a2.append((remote(mlm.at[h], mly.at[h], a2_snd.at[2 * h], a2_rcv.at[2 * h], across),
                   remote(om.at[h], oy.at[h], a2_snd.at[2 * h + 1], a2_rcv.at[2 * h + 1], across)))
    merge_core(0, (1 - row) * 2 + core, om, mlm, a2)
    for cp in wts:
        cp.start()
    merge_core(1, row * 2 + core, own, ml_mine)
    wts[0].wait()

    e1_cp = lambda t: remote(p1.at[t], e1.at[t], es1.at[t], er1.at[t], to_mid)
    x1_cp = lambda t: remote(p1.at[t], x1.at[t], xs1.at[t], xr1.at[t], to_other)
    t1_cp = lambda t: remote(r1.at[t], r1.at[t], ts1.at[t], tr1.at[t], to_end)
    e2_cp = lambda t: remote(p2.at[t], e2.at[t], es2.at[t], er2.at[t], to_mid)
    x2_cp = lambda t: remote(p2.at[t], x2.at[t], xs2.at[t], xr2.at[t], to_other)
    t2_cp = lambda t: remote(ob.at[t], ob.at[t], ts2.at[t], tr2.at[t], to_end)
    p_cp = lambda t: remote(ob.at[t], pb.at[t], ps.at[t], pr.at[t], partner)
    y_cp = lambda t: remote(ob.at[t], yb.at[t], ys.at[t], yr.at[t], across)
    f_cp = lambda t: remote(yb.at[t], pf.at[t], fs.at[t], fr.at[t], partner)

    def spread(h, lhs, w, dst, cp, after=None):
        wide = width // 2
        per = N_COL // 2
        for j in range(2):
            d = jnp.dot(lhs, w[:, j * wide:(j + 1) * wide], preferred_element_type=jnp.float32)
            for n in range(per):
                dst[h * N_COL + j * per + n] = d[:, n * n_col:(n + 1) * n_col]

            @pl.when(is_end)
            def _():
                @pl.loop(h * N_COL + j * per, h * N_COL + (j + 1) * per)
                def _(t):
                    cp(t).start()

            if after is not None:
                after(h)

    for h in range(N_HALF):
        for cp in a2[h]:
            cp.wait()
        _, wa, wb, tot = weigh(ml_mine[h], mly[h])
        inv = 1.0 / tot
        for k in range(4):
            val = (own[h, k] * wa[:, k:k + 1] + oy[h, k] * wb[:, k:k + 1]) * inv[:, k:k + 1]
            attn[h, :, k * HEAD:(k + 1) * HEAD] = val.astype(jnp.bfloat16)

        spread(h, attn[h], wo, p1, e1_cp)

    def sum_step(s):
        @pl.when(s < n_piece)
        def _():
            e1_cp(s).wait_recv()
            p1[s] = p1[s] + e1[s]
            x1_cp(s).start()

        @pl.when(s >= LAG)
        def _():
            t = s - LAG
            h = t // N_COL
            rs = pl.ds(pl.multiple_of(h * n_half, n_half), n_half)
            cs = pl.ds(pl.multiple_of((t - h * N_COL) * n_col, n_col), n_col)
            x1_cp(t).wait_recv()
            r = hid[rs, cs].astype(jnp.float32) + (p1[t] + x1[t])
            r1[t] = r.astype(jnp.bfloat16).astype(jnp.float32)
            t1_cp(t).start()

    def sum_steps(lo, hi):
        @pl.when(is_mid)
        def _():
            pl.loop(lo, hi)(sum_step)

    def end_recv(lo, hi):
        @pl.when(is_end)
        def _():
            @pl.loop(lo, hi)
            def _(t):
                t1_cp(t).wait_recv()

    def share(t):
        p_cp(t).start()
        y_cp(t).start()

    def relay(t):
        y_cp(t).wait_recv()
        f_cp(t).start()

    def share_step(s):
        @pl.when(s < n_piece)
        def _():
            e2_cp(s).wait_recv()
            p2[s] = p2[s] + e2[s]
            x2_cp(s).start()

        @pl.when((s >= LAG) & (s < n_piece + LAG))
        def _():
            t = s - LAG
            x2_cp(t).wait_recv()
            o = r1[t] + (p2[t] + x2[t])
            ob[t] = o.astype(jnp.bfloat16).astype(jnp.float32)
            t2_cp(t).start()
            share(t)

        @pl.when(s >= LAG + LAG_Y)
        def _():
            relay(s - LAG - LAG_Y)


    def share_steps(lo, hi):
        @pl.when(is_mid)
        def _():
            pl.loop(lo, hi)(share_step)

    gain = gain_row(mn_ref)
    ffn = wg.shape[1]
    blk = ffn // TILES
    done = [0, 0]

    def serve(h):
        for _ in range(SERVE):
            if done[0] < n_piece + LAG:
                sum_steps(done[0], done[0] + 1)
                done[0] += 1
            elif done[1] < h * N_COL:
                share_steps(done[1], done[1] + 1)
                done[1] += 1

    for h in range(N_HALF):
        stop = max(done[0], (h + 1) * N_COL + LAG)
        if stop > done[0]:
            sum_steps(done[0], stop)
            done[0] = stop
        end_recv(h * N_COL, (h + 1) * N_COL)
        sq = jnp.zeros((n_half, 1), jnp.float32)
        for n in range(N_COL):
            r = r1[h * N_COL + n]
            sq = sq + jnp.sum(r * r, axis=-1, keepdims=True)
        inv = lax.rsqrt(sq / width + NORM_EPS)
        for n in range(N_COL):
            m_s[:, n * n_col:(n + 1) * n_col] = (r1[h * N_COL + n] * inv * gain[:, n * n_col:(n + 1) * n_col]).astype(jnp.bfloat16)
        if h == 0:
            wts[1].wait()
            wts[2].wait()
        for n in range(TILES):
            cs = slice(n * blk, (n + 1) * blk)
            g = jnp.dot(m_s[...], wg[:, cs], preferred_element_type=jnp.float32)
            u = jnp.dot(m_s[...], wu[:, cs], preferred_element_type=jnp.float32)
            act[:, cs] = (jax.nn.silu(g) * u).astype(jnp.bfloat16)
            serve(h)
        if h == 0:
            wts[3].wait()
        spread(h, act[...], wd, p2, e2_cp, serve)

    share_steps(done[1], n_piece + LAG + LAG_Y)

    @pl.when(is_end)
    def _():
        @pl.loop(0, n_piece + LAG_Y)
        def _(s):
            @pl.when(s < n_piece)
            def _():
                t2_cp(s).wait_recv()
                share(s)

            @pl.when(s >= LAG_Y)
            def _():
                relay(s - LAG_Y)

    def put(j, t, val):
        h = t // N_COL
        rs = pl.ds(pl.multiple_of(h * n_half, n_half), n_half)
        cs = pl.ds(pl.multiple_of((t - h * N_COL) * n_col, n_col), n_col)
        out_ref[j, rs, cs] = val.astype(jnp.bfloat16)

    def leave(j, h, k):
        rs = pl.ds(h * n_half, n_half)
        return pltpu.make_async_copy(out_ref.at[j, rs], out_hbm.at[j, rs], out_sem.at[h * 4 + k])

    homes = (sp, row * 2 + 1 - core, (1 - row) * 2 + core, (1 - row) * 2 + 1 - core)
    for h in range(N_HALF):
        @pl.loop(h * N_COL, (h + 1) * N_COL)
        def _(t):
            put(homes[0], t, ob[t])
            p_cp(t).wait_recv()
            put(homes[1], t, pb[t])
            put(homes[2], t, yb[t])
            f_cp(t).wait_recv()
            put(homes[3], t, pf[t])

        for k in range(4):
            leave(homes[k], h, k).start()

    @pl.loop(0, n_piece)
    def _(t):
        p_cp(t).wait_send()
        y_cp(t).wait_send()
        f_cp(t).wait_send()

        @pl.when(is_mid)
        def _():
            x1_cp(t).wait_send()
            t1_cp(t).wait_send()
            x2_cp(t).wait_send()
            t2_cp(t).wait_send()

        @pl.when(is_end)
        def _():
            e1_cp(t).wait_send()
            e2_cp(t).wait_send()

    for h in range(N_HALF):
        for k in range(4):
            leave(homes[k], h, k).wait()


def layer(o, ml, hidden, w_o, w_gate, w_up, w_down, mlp_norm):
    n_steps, n_batch, width = hidden.shape
    n_half = n_batch // N_HALF
    n_col = width // N_COL
    n_piece = N_COL * N_HALF
    vm = pl.BlockSpec(memory_space=pltpu.VMEM)
    anyspec = pl.BlockSpec(memory_space=pltpu.HBM)
    f32, bf16 = jnp.float32, jnp.bfloat16
    piece = pltpu.VMEM((n_piece, n_half, n_col), f32)
    dma = pltpu.SemaphoreType.DMA
    return pl.pallas_call(
        layer_kernel,
        name='layer',
        out_shape=jax.ShapeDtypeStruct(hidden.shape, bf16),
        in_specs=[anyspec] * 8,
        out_specs=anyspec,
        scratch_shapes=[
            pltpu.VMEM((16, n_batch, HEAD), f32),
            pltpu.VMEM((4, n_batch, HEAD), f32),
            pltpu.VMEM((width // HEAD, HEAD), bf16),
            pltpu.VMEM(hidden.shape, bf16),
            pltpu.VMEM((2, 4, n_batch, HEAD), f32),
            pltpu.VMEM((2, n_batch, HEAD), f32),
            pltpu.VMEM((N_HALF, 4, n_half, HEAD), f32),
            pltpu.VMEM((N_HALF, n_half, HEAD), f32),
            pltpu.VMEM((N_HALF, 4, n_half, HEAD), f32),
            pltpu.VMEM((N_HALF, n_half, HEAD), f32),
            pltpu.VMEM((N_HALF, 4, n_half, HEAD), f32),
            pltpu.VMEM((N_HALF, n_half, HEAD), f32),
            pltpu.VMEM((N_HALF, n_half, 4 * HEAD), bf16),
            pltpu.VMEM((n_batch, width), bf16),
            pltpu.VMEM(w_o.shape, bf16),
            pltpu.VMEM(w_gate.shape, bf16),
            pltpu.VMEM(w_up.shape, bf16),
            pltpu.VMEM(w_down.shape, bf16),
            piece, piece, piece, piece,
            pltpu.VMEM((n_half, width), bf16),
            pltpu.VMEM((n_half, w_gate.shape[1]), bf16),
            piece, piece, piece, piece, piece, piece, piece,
            dma((7,)), dma((4 * N_HALF,)), dma((4,)), dma((4,)), dma((4,)), dma((2 * N_HALF,)), dma((2 * N_HALF,)),
        ] + [dma((n_piece,))] * 18,
        compiler_params=pltpu.CompilerParams(collective_id=0, has_side_effects=True, vmem_limit_bytes=67043328),
        cost_estimate=pl.CostEstimate(flops=2 * 10 ** 9, bytes_accessed=30 * 10 ** 6, transcendentals=10 ** 6),
    )(o.reshape(16, n_batch, HEAD), ml, hidden, w_o, w_gate, w_up, w_down, mlp_norm.reshape(-1, HEAD))


def emit_kernel(src, dst, buf, in_sem, out_sem):
    n = buf.shape[0]
    ins = [pltpu.make_async_copy(src.at[j], buf.at[j], in_sem.at[j]) for j in range(n)]
    outs = [pltpu.make_async_copy(buf.at[j], dst.at[j], out_sem.at[j]) for j in range(n)]
    for cp in ins:
        cp.start()
    for j in range(n):
        ins[j].wait()
        outs[j].start()
    for cp in outs:
        cp.wait()


def emit(x):
    n = x.shape[0]
    anyspec = pl.BlockSpec(memory_space=pltpu.HBM)
    return pl.pallas_call(
        emit_kernel,
        name='emit',
        out_shape=jax.ShapeDtypeStruct(x.shape, x.dtype),
        in_specs=[anyspec],
        out_specs=anyspec,
        scratch_shapes=[pltpu.VMEM(x.shape, x.dtype), pltpu.SemaphoreType.DMA((n,)), pltpu.SemaphoreType.DMA((n,))],
        compiler_params=pltpu.CompilerParams(vmem_limit_bytes=67043328),
        cost_estimate=pl.CostEstimate(flops=0, bytes_accessed=4 * 10 ** 6, transcendentals=0),
    )(x)


def solution(mesh):
    cache_spec = P('dp', 'sp', 'tp', None)
    col_spec = P(None, 'tp')
    row_spec = P('tp', None)
    in_specs = (P(None, 'dp', None), P('dp'), cache_spec, cache_spec, col_spec, col_spec, col_spec, row_spec,
                col_spec, col_spec, row_spec, P(), P(), P(), P())
    out_specs = (P(None, 'dp', None), cache_spec, cache_spec)

    def shard_body(hidden, start_pos, k_cache, v_cache, w_q, w_k, w_v, w_o, w_gate, w_up, w_down, attn_norm, mlp_norm, q_gain, k_gain):
        flat = (k_cache.shape[0], k_cache.shape[1] * k_cache.shape[2], k_cache.shape[3])
        o, ml, k_out, v_out = attend(start_pos, hidden, w_q, w_k, w_v, k_cache.reshape(flat), v_cache.reshape(flat), attn_norm, q_gain, k_gain)
        out = layer(o, ml, hidden, w_o, w_gate, w_up, w_down, mlp_norm)
        return emit(out), k_out.reshape(k_cache.shape), v_out.reshape(v_cache.shape)

    return jax.shard_map(shard_body, mesh=mesh, in_specs=in_specs, out_specs=out_specs, check_vma=False)
```

```python
import functools
import jax
import jax.numpy as jnp
import numpy as np
from jax import lax
from jax.experimental import pallas as pl
from jax.experimental.pallas import tpu as pltpu
from jax.sharding import PartitionSpec as P

ROPE_BASE = 1000000.0
NORM_EPS = 1e-06
NEG_BIG = -3e38
HEAD = 128
CHUNK = 8


def gain_row(ref):
    g = ref[...].astype(jnp.float32)
    return jnp.concatenate([g[j:j + 1] for j in range(g.shape[0])], axis=1)


def attend_kernel(start_hbm, hid_hbm, wq_hbm, wk_hbm, wv_hbm, kc_hbm, vc_hbm, an_hbm, qg_hbm, kg_hbm, freq_hbm,
                  o_hbm, ml_hbm, ko_hbm, vo_hbm,
                  start_ref, an_ref, qg_ref, kg_ref, freq_ref, o_ref, ml_ref, s_sem, o_sem,
                  hid, wq, wk, wv, kbuf, vbuf, nrm, raw, q_s, k_s, v_s, pos_s, ml_s, key_s, sc_s, pr_s,
                  w_sem, h_sem, kin_sem, vin_sem, kout_sem, vout_sem):
    n_steps, n_batch, width = hid.shape
    rows = kbuf.shape[1]
    seq_blk = rows // 2
    n_chunk = n_batch // CHUNK
    n_q = wq.shape[1] // HEAD
    n_kv = wk.shape[1] // HEAD
    blk_start = lax.axis_index('sp') * seq_blk
    scale = HEAD ** -0.5

    small = [pltpu.make_async_copy(a, b, s_sem.at[j]) for j, (a, b) in enumerate((
        (start_hbm, start_ref), (freq_hbm, freq_ref), (an_hbm, an_ref), (qg_hbm, qg_ref), (kg_hbm, kg_ref)))]
    hid_cp = pltpu.make_async_copy(hid_hbm, hid, h_sem)
    for cp in small[:2] + [hid_cp] + small[2:]:
        cp.start()
    w_cps = [pltpu.make_async_copy(a, b, w_sem.at[j]) for j, (a, b) in enumerate(((wq_hbm, wq), (wk_hbm, wk), (wv_hbm, wv)))]
    for cp in w_cps:
        cp.start()

    def kv_in(c):
        sl = pl.ds(c * CHUNK, CHUNK)
        return (pltpu.make_async_copy(kc_hbm.at[sl], kbuf.at[sl], kin_sem.at[c]),
                pltpu.make_async_copy(vc_hbm.at[sl], vbuf.at[sl], vin_sem.at[c]))

    def kv_out(c):
        sl = pl.ds(c * CHUNK, CHUNK)
        return (pltpu.make_async_copy(kbuf.at[sl], ko_hbm.at[sl], kout_sem.at[c]),
                pltpu.make_async_copy(vbuf.at[sl], vo_hbm.at[sl], vout_sem.at[c]))

    @pl.loop(0, n_chunk)
    def _(c):
        a, b = kv_in(c)
        a.start()
        b.start()

    for cp in small:
        cp.wait()

    @pl.loop(0, n_batch)
    def _(b):
        pos_s[pl.ds(b, 1), :] = jnp.full((1, HEAD), start_ref[b].astype(jnp.float32), jnp.float32)

    freq = freq_ref[0:1, :]
    sign = freq_ref[1:2, :]
    ang = pos_s[...] * freq
    cos0 = jnp.cos(ang)
    sin0 = jnp.sin(ang)

    r_id = lax.broadcasted_iota(jnp.int32, (16, rows), 0)
    c_id = lax.broadcasted_iota(jnp.int32, (16, rows), 1)
    same = ((r_id % 4) // 2) == (c_id % 2)
    key_s[...] = jnp.where(same, c_id // 2 - r_id // 4, 1 << 20)

    hid_cp.wait()
    gain = gain_row(an_ref)
    for i in range(n_steps):
        for h in range(0, n_batch, 32):
            x = hid[i, h:h + 32, :].astype(jnp.float32)
            inv = lax.rsqrt(jnp.mean(x * x, axis=-1, keepdims=True) + NORM_EPS)
            nrm[i * n_batch + h:i * n_batch + h + 32, :] = (x * inv * gain).astype(jnp.bfloat16)

    def rope(x, g, cos, sin):
        inv = lax.rsqrt(jnp.mean(x * x, axis=-1, keepdims=True) + NORM_EPS)
        y = x * inv * g
        return y * cos + pltpu.roll(y, HEAD // 2, 1) * sin

    tabs = []
    for i in range(n_steps):
        if i == 0:
            c, s = cos0, sin0
        else:
            ci, si = jnp.cos(freq * float(i)), jnp.sin(freq * float(i))
            c, s = cos0 * ci - sin0 * si, sin0 * ci + cos0 * si
        pos_s_c, pos_s_s = c, s * sign
        tabs.append((pos_s_c, pos_s_s))

    for cp in w_cps:
        cp.wait()
    qg = qg_ref[...].astype(jnp.float32)
    kg = kg_ref[...].astype(jnp.float32)
    nq = n_q * HEAD
    nk = n_kv * HEAD
    raw[:, :nq] = jnp.dot(nrm[...], wq[...], preferred_element_type=jnp.float32)
    raw[:, nq:nq + nk] = jnp.dot(nrm[...], wk[...], preferred_element_type=jnp.float32)
    raw[:, nq + nk:] = jnp.dot(nrm[...], wv[...], preferred_element_type=jnp.float32)
    for i in range(n_steps):
        rs = slice(i * n_batch, (i + 1) * n_batch)
        cos, sin = tabs[i]
        for h in range(n_q):
            q_s[pl.ds(i * n_q + h, n_batch, stride=n_steps * n_q), :] = rope(raw[rs, h * HEAD:(h + 1) * HEAD], qg, cos, sin)
        for h in range(n_kv):
            k_s[pl.ds(i * n_kv + h, n_batch, stride=n_steps * n_kv), :] = rope(
                raw[rs, nq + h * HEAD:nq + (h + 1) * HEAD], kg, cos, sin)
            v_s[pl.ds(i * n_kv + h, n_batch, stride=n_steps * n_kv), :] = raw[rs, nq + nk + h * HEAD:nq + nk + (h + 1) * HEAD]

    row32 = lax.broadcasted_iota(jnp.int32, (32, HEAD), 0)
    eye_r = lax.broadcasted_iota(jnp.int32, (16, HEAD), 0)
    eye_c = lax.broadcasted_iota(jnp.int32, (16, HEAD), 1)
    eye_m = eye_r == eye_c
    eye_l = eye_r + 16 == eye_c
    zero24 = jnp.zeros((24, HEAD), jnp.float32)

    @pl.loop(0, n_chunk)
    def _(c):
        a, b = kv_in(c)
        a.wait()
        b.wait()
        lps = []
        for u in range(CHUNK):
            bb = c * CHUNK + u
            lp = start_ref[bb] - blk_start
            lps.append(lp)
            base = jnp.clip((lp // 8) * 8, 0, seq_blk - 16)
            rel = (lp - base) * 2
            shift = jnp.bitwise_and(rel, 31)
            hit = (row32 >= rel) & (row32 < rel + 8)
            win = pl.ds(pl.multiple_of(base * 2, 16), 32)
            for src, dst in ((k_s, kbuf), (v_s, vbuf)):
                new = src[pl.ds(pl.multiple_of(bb * 8, 8), 8), :]
                new = pltpu.roll(jnp.concatenate([new, zero24], axis=0), shift, 0)
                old = dst[bb, win, :].astype(jnp.float32)
                dst[bb, win, :] = jnp.where(hit, new, old).astype(jnp.bfloat16)
        for u in range(CHUNK):
            bb = c * CHUNK + u
            q = q_s[pl.ds(pl.multiple_of(bb * 16, 16), 16), :].astype(jnp.bfloat16)
            sc_s[u] = lax.dot_general(q, kbuf[bb], (((1,), (1,)), ((), ())), preferred_element_type=jnp.float32)
        tops = []
        for u in range(CHUNK):
            s = jnp.where(key_s[...] <= lps[u], sc_s[u] * scale, NEG_BIG)
            sc_s[u] = s
            tops.append(jnp.maximum(jnp.max(s, axis=-1, keepdims=True), 0.5 * NEG_BIG))
        sums = []
        for u in range(CHUNK):
            p = jnp.exp(sc_s[u] - tops[u])
            sums.append(jnp.sum(p, axis=-1, keepdims=True))
            pr_s[u] = p.astype(jnp.bfloat16)
        for u in range(CHUNK):
            bb = c * CHUNK + u
            o_ref[pl.ds(bb, 16, stride=n_batch), :] = jnp.dot(pr_s[u], vbuf[bb], preferred_element_type=jnp.float32)
        for u in range(CHUNK):
            ml = jnp.where(eye_m, tops[u], 0.0) + jnp.where(eye_l, sums[u], 0.0)
            ml_s[pl.ds(c * CHUNK + u, 1), :] = jnp.sum(ml, axis=0, keepdims=True)
        a, b = kv_out(c)
        a.start()
        b.start()

    for i in range(n_steps):
        ml = ml_s[...]
        ml_ref[i] = ml if i == 0 else pltpu.roll(ml, HEAD - 4 * i, 1)
    outs = [pltpu.make_async_copy(o_ref, o_hbm, o_sem.at[0]), pltpu.make_async_copy(ml_ref, ml_hbm, o_sem.at[1])]
    for cp in outs:
        cp.start()

    @pl.loop(0, n_chunk)
    def _(c):
        a, b = kv_out(c)
        a.wait()
        b.wait()

    for cp in outs:
        cp.wait()


def attend(start_pos, hidden, w_q, w_k, w_v, k_cache, v_cache, attn_norm, q_gain, k_gain):
    n_steps, n_batch, width = hidden.shape
    rows = k_cache.shape[1]
    n_chunk = n_batch // CHUNK
    nq, nk = w_q.shape[1], w_k.shape[1]
    half = HEAD // 2
    f = ROPE_BASE ** (-(np.arange(half, dtype=np.float64) * (2.0 / HEAD)))
    freq = np.stack([np.concatenate([f, f]), np.concatenate([-np.ones(half), np.ones(half)])]).astype(np.float32)
    anyspec = pl.BlockSpec(memory_space=pltpu.HBM)
    return pl.pallas_call(
        attend_kernel,
        name='attend',
        out_shape=(jax.ShapeDtypeStruct((16 * n_batch, HEAD), jnp.float32),
                   jax.ShapeDtypeStruct((n_steps, n_batch, HEAD), jnp.float32),
                   jax.ShapeDtypeStruct(k_cache.shape, jnp.bfloat16),
                   jax.ShapeDtypeStruct(v_cache.shape, jnp.bfloat16)),
        in_specs=[anyspec] * 11,
        out_specs=(anyspec,) * 4,
        scratch_shapes=[
            pltpu.SMEM(start_pos.shape, jnp.int32),
            pltpu.VMEM((width // HEAD, HEAD), jnp.bfloat16),
            pltpu.VMEM((1, HEAD), jnp.bfloat16),
            pltpu.VMEM((1, HEAD), jnp.bfloat16),
            pltpu.VMEM((2, HEAD), jnp.float32),
            pltpu.VMEM((16 * n_batch, HEAD), jnp.float32),
            pltpu.VMEM((n_steps, n_batch, HEAD), jnp.float32),
            pltpu.SemaphoreType.DMA((5,)),
            pltpu.SemaphoreType.DMA((2,)),
            pltpu.VMEM(hidden.shape, jnp.bfloat16),
            pltpu.VMEM(w_q.shape, jnp.bfloat16),
            pltpu.VMEM(w_k.shape, jnp.bfloat16),
            pltpu.VMEM(w_v.shape, jnp.bfloat16),
            pltpu.VMEM(k_cache.shape, jnp.bfloat16),
            pltpu.VMEM(v_cache.shape, jnp.bfloat16),
            pltpu.VMEM((n_steps * n_batch, width), jnp.bfloat16),
            pltpu.VMEM((n_steps * n_batch, nq + 2 * nk), jnp.float32),
            pltpu.VMEM((n_batch * 16, HEAD), jnp.float32),
            pltpu.VMEM((n_batch * 8, HEAD), jnp.float32),
            pltpu.VMEM((n_batch * 8, HEAD), jnp.float32),
            pltpu.VMEM((n_batch, HEAD), jnp.float32),
            pltpu.VMEM((n_batch, HEAD), jnp.float32),
            pltpu.VMEM((16, rows), jnp.int32),
            pltpu.VMEM((CHUNK, 16, rows), jnp.float32),
            pltpu.VMEM((CHUNK, 16, rows), jnp.bfloat16),
            pltpu.SemaphoreType.DMA((3,)),
            pltpu.SemaphoreType.DMA,
            pltpu.SemaphoreType.DMA((n_chunk,)),
            pltpu.SemaphoreType.DMA((n_chunk,)),
            pltpu.SemaphoreType.DMA((n_chunk,)),
            pltpu.SemaphoreType.DMA((n_chunk,)),
        ],
        compiler_params=pltpu.CompilerParams(vmem_limit_bytes=67043328),
        cost_estimate=pl.CostEstimate(flops=2 * 10 ** 9, bytes_accessed=40 * 10 ** 6, transcendentals=10 ** 6),
    )(start_pos, hidden, w_q, w_k, w_v, k_cache, v_cache, attn_norm.reshape(-1, HEAD), q_gain.reshape(1, -1), k_gain.reshape(1, -1), jnp.asarray(freq))


N_COL = 4
N_HALF = 4
LAG = 5
LAG_Y = 8
TILES = 2
SERVE = 2


def layer_kernel(o_hbm, ml_hbm, hid_hbm, wo_hbm, wg_hbm, wu_hbm, wd_hbm, mn_hbm, out_hbm,
                 o_own, ml_own, mn_ref, out_ref, oa, mla, om, mlm, oy, mly, own, ml_mine, attn, hid, wo, wg, wu, wd,
                 p1, e1, x1, r1, m_s, act, p2, e2, x2, ob, yb, pb, pf,
                 ld_sem, out_sem, w_sem, a1_snd, a1_rcv, a2_snd, a2_rcv, es1, er1, xs1, xr1, ts1, tr1,
                 es2, er2, xs2, xr2, ts2, tr2, ps, pr, ys, yr, fs, fr):
    n_steps, n_batch, width = hid_hbm.shape
    n_half = n_batch // N_HALF
    n_col = width // N_COL
    n_piece = N_COL * N_HALF
    tp = lax.axis_index('tp')
    sp = lax.axis_index('sp')
    core = sp % 2
    row = sp // 2
    partner = {'sp': row * 2 + 1 - core}
    across = {'sp': (1 - row) * 2 + core}
    is_mid = (tp % 3) != 0
    is_end = (tp % 3) == 0
    to_mid = {'tp': (tp + 3) // 3}
    to_end = {'tp': (tp - 1) * 3}
    to_other = {'tp': 3 - tp}
    mesh_id = pl.DeviceIdType.MESH

    def remote(src, dst, ssem, rsem, dev):
        return pltpu.make_async_remote_copy(src_ref=src, dst_ref=dst, send_sem=ssem, recv_sem=rsem, device_id=dev, device_id_type=mesh_id)

    barrier = pltpu.get_barrier_semaphore()
    for dev in (partner, across):
        pl.semaphore_signal(barrier, inc=1, device_id=dev, device_id_type=mesh_id)

    @pl.when(is_mid)
    def _():
        pl.semaphore_signal(barrier, inc=1, device_id=to_end, device_id_type=mesh_id)
        pl.semaphore_signal(barrier, inc=1, device_id=to_other, device_id_type=mesh_id)

    @pl.when(is_end)
    def _():
        pl.semaphore_signal(barrier, inc=1, device_id=to_mid, device_id_type=mesh_id)

    send_to = 1 - core
    o_cps, ml_cps = [], []
    for q, step in enumerate(((1 - row) * 2 + send_to, row * 2 + send_to, (1 - row) * 2 + core, row * 2 + core)):
        o_cps.append(pltpu.make_async_copy(o_hbm.at[pl.ds(step * 4, 4)], o_own.at[pl.ds(step * 4, 4)], ld_sem.at[q]))
    ml_cp = pltpu.make_async_copy(ml_hbm, ml_own, ld_sem.at[4])
    hid_cp = pltpu.make_async_copy(hid_hbm.at[sp], hid, ld_sem.at[5])
    mn_cp = pltpu.make_async_copy(mn_hbm, mn_ref, ld_sem.at[6])
    lds = [ml_cp] + o_cps + [hid_cp, mn_cp]
    wts = [pltpu.make_async_copy(a, b, w_sem.at[j]) for j, (a, b) in enumerate(((wo_hbm, wo), (wg_hbm, wg), (wu_hbm, wu), (wd_hbm, wd)))]
    for cp in lds:
        cp.start()

    @pl.when(is_mid)
    def _():
        pl.semaphore_wait(barrier, 4)

    @pl.when(is_end)
    def _():
        pl.semaphore_wait(barrier, 3)

    ml_cp.wait()
    a1 = []
    for q, jy in enumerate((1 - row, row)):
        step = jy * 2 + 1 - core
        o_cps[q].wait()
        a1.append((remote(ml_own.at[step], mla.at[q], a1_snd.at[2 * q], a1_rcv.at[2 * q], partner),
                   remote(o_own.at[pl.ds(step * 4, 4)], oa.at[q], a1_snd.at[2 * q + 1], a1_rcv.at[2 * q + 1], partner)))
        for cp in a1[-1]:
            cp.start()

    lane = lax.broadcasted_iota(jnp.int32, (n_half, HEAD), 1)

    def weigh(ma, mb):
        top = jnp.maximum(ma, mb)
        wa, wb = jnp.exp(ma - top), jnp.exp(mb - top)
        tot = pltpu.roll(ma, HEAD - 16, 1) * wa + pltpu.roll(mb, HEAD - 16, 1) * wb
        return top, wa, wb, tot

    def merge_core(q, step, dst, mldst, send=None):
        for cp in a1[q]:
            cp.wait()
        for h in range(N_HALF):
            rs = pl.ds(h * n_half, n_half)
            top, wa, wb, tot = weigh(ml_own[step, rs, :], mla[q, rs, :])
            mldst[h] = jnp.where(lane < 16, top, pltpu.roll(tot, 16, 1))
            for k in range(4):
                dst[h, k] = o_own[step * 4 + k, rs, :] * wa[:, k:k + 1] + oa[q, k, rs, :] * wb[:, k:k + 1]
            if send is not None:
                for cp in send[h]:
                    cp.start()

    for cp in lds[3:]:
        cp.wait()
    a2 = []
    for h in range(N_HALF):
        a2.append((remote(mlm.at[h], mly.at[h], a2_snd.at[2 * h], a2_rcv.at[2 * h], across),
                   remote(om.at[h], oy.at[h], a2_snd.at[2 * h + 1], a2_rcv.at[2 * h + 1], across)))
    merge_core(0, (1 - row) * 2 + core, om, mlm, a2)
    for cp in wts:
        cp.start()
    merge_core(1, row * 2 + core, own, ml_mine)
    wts[0].wait()

    e1_cp = lambda t: remote(p1.at[t], e1.at[t], es1.at[t], er1.at[t], to_mid)
    x1_cp = lambda t: remote(p1.at[t], x1.at[t], xs1.at[t], xr1.at[t], to_other)
    t1_cp = lambda t: remote(r1.at[t], r1.at[t], ts1.at[t], tr1.at[t], to_end)
    e2_cp = lambda t: remote(p2.at[t], e2.at[t], es2.at[t], er2.at[t], to_mid)
    x2_cp = lambda t: remote(p2.at[t], x2.at[t], xs2.at[t], xr2.at[t], to_other)
    t2_cp = lambda t: remote(ob.at[t], ob.at[t], ts2.at[t], tr2.at[t], to_end)
    p_cp = lambda t: remote(ob.at[t], pb.at[t], ps.at[t], pr.at[t], partner)
    y_cp = lambda t: remote(ob.at[t], yb.at[t], ys.at[t], yr.at[t], across)
    f_cp = lambda t: remote(yb.at[t], pf.at[t], fs.at[t], fr.at[t], partner)

    def spread(h, lhs, w, dst, cp, after=None):
        wide = width // 2
        per = N_COL // 2
        for j in range(2):
            d = jnp.dot(lhs, w[:, j * wide:(j + 1) * wide], preferred_element_type=jnp.float32)
            for n in range(per):
                dst[h * N_COL + j * per + n] = d[:, n * n_col:(n + 1) * n_col]

            @pl.when(is_end)
            def _():
                @pl.loop(h * N_COL + j * per, h * N_COL + (j + 1) * per)
                def _(t):
                    cp(t).start()

            if after is not None:
                after(h)

    for h in range(N_HALF):
        for cp in a2[h]:
            cp.wait()
        _, wa, wb, tot = weigh(ml_mine[h], mly[h])
        inv = 1.0 / tot
        for k in range(4):
            val = (own[h, k] * wa[:, k:k + 1] + oy[h, k] * wb[:, k:k + 1]) * inv[:, k:k + 1]
            attn[h, :, k * HEAD:(k + 1) * HEAD] = val.astype(jnp.bfloat16)

        spread(h, attn[h], wo, p1, e1_cp)

    def sum_step(s):
        @pl.when(s < n_piece)
        def _():
            e1_cp(s).wait_recv()
            p1[s] = p1[s] + e1[s]
            x1_cp(s).start()

        @pl.when(s >= LAG)
        def _():
            t = s - LAG
            h = t // N_COL
            rs = pl.ds(pl.multiple_of(h * n_half, n_half), n_half)
            cs = pl.ds(pl.multiple_of((t - h * N_COL) * n_col, n_col), n_col)
            x1_cp(t).wait_recv()
            r = hid[rs, cs].astype(jnp.float32) + (p1[t] + x1[t])
            r1[t] = r.astype(jnp.bfloat16).astype(jnp.float32)
            t1_cp(t).start()

    def sum_steps(lo, hi):
        @pl.when(is_mid)
        def _():
            pl.loop(lo, hi)(sum_step)

    def end_recv(lo, hi):
        @pl.when(is_end)
        def _():
            @pl.loop(lo, hi)
            def _(t):
                t1_cp(t).wait_recv()

    def share(t):
        y_cp(t).start()
        p_cp(t).start()

    def relay(t):
        y_cp(t).wait_recv()
        f_cp(t).start()

    def share_step(s):
        @pl.when(s < n_piece)
        def _():
            e2_cp(s).wait_recv()
            p2[s] = p2[s] + e2[s]
            x2_cp(s).start()

        @pl.when((s >= LAG) & (s < n_piece + LAG))
        def _():
            t = s - LAG
            x2_cp(t).wait_recv()
            o = r1[t] + (p2[t] + x2[t])
            ob[t] = o.astype(jnp.bfloat16).astype(jnp.float32)
            t2_cp(t).start()
            share(t)

        @pl.when(s >= LAG + LAG_Y)
        def _():
            relay(s - LAG - LAG_Y)


    def share_steps(lo, hi):
        @pl.when(is_mid)
        def _():
            pl.loop(lo, hi)(share_step)

    gain = gain_row(mn_ref)
    ffn = wg.shape[1]
    blk = ffn // TILES
    done = [0, 0]

    def serve(h):
        for _ in range(SERVE):
            if done[0] < n_piece + LAG:
                sum_steps(done[0], done[0] + 1)
                done[0] += 1
            elif done[1] < h * N_COL:
                share_steps(done[1], done[1] + 1)
                done[1] += 1

    for h in range(N_HALF):
        stop = max(done[0], (h + 1) * N_COL + LAG)
        if stop > done[0]:
            sum_steps(done[0], stop)
            done[0] = stop
        end_recv(h * N_COL, (h + 1) * N_COL)
        sq = jnp.zeros((n_half, 1), jnp.float32)
        for n in range(N_COL):
            r = r1[h * N_COL + n]
            sq = sq + jnp.sum(r * r, axis=-1, keepdims=True)
        inv = lax.rsqrt(sq / width + NORM_EPS)
        for n in range(N_COL):
            m_s[:, n * n_col:(n + 1) * n_col] = (r1[h * N_COL + n] * inv * gain[:, n * n_col:(n + 1) * n_col]).astype(jnp.bfloat16)
        if h == 0:
            wts[1].wait()
            wts[2].wait()
        for n in range(TILES):
            cs = slice(n * blk, (n + 1) * blk)
            g = jnp.dot(m_s[...], wg[:, cs], preferred_element_type=jnp.float32)
            u = jnp.dot(m_s[...], wu[:, cs], preferred_element_type=jnp.float32)
            act[:, cs] = (jax.nn.silu(g) * u).astype(jnp.bfloat16)
            serve(h)
        if h == 0:
            wts[3].wait()
        spread(h, act[...], wd, p2, e2_cp, serve)

    share_steps(done[1], n_piece + LAG + LAG_Y)

    @pl.when(is_end)
    def _():
        @pl.loop(0, n_piece + LAG_Y)
        def _(s):
            @pl.when(s < n_piece)
            def _():
                t2_cp(s).wait_recv()
                share(s)

            @pl.when(s >= LAG_Y)
            def _():
                relay(s - LAG_Y)

    def put(j, t, val):
        h = t // N_COL
        rs = pl.ds(pl.multiple_of(h * n_half, n_half), n_half)
        cs = pl.ds(pl.multiple_of((t - h * N_COL) * n_col, n_col), n_col)
        out_ref[j, rs, cs] = val.astype(jnp.bfloat16)

    def leave(j, h, k):
        rs = pl.ds(h * n_half, n_half)
        return pltpu.make_async_copy(out_ref.at[j, rs], out_hbm.at[j, rs], out_sem.at[h * 4 + k])

    homes = (sp, row * 2 + 1 - core, (1 - row) * 2 + core, (1 - row) * 2 + 1 - core)
    for h in range(N_HALF):
        @pl.loop(h * N_COL, (h + 1) * N_COL)
        def _(t):
            put(homes[0], t, ob[t])
            p_cp(t).wait_recv()
            put(homes[1], t, pb[t])
            put(homes[2], t, yb[t])
            f_cp(t).wait_recv()
            put(homes[3], t, pf[t])

        for k in range(4):
            leave(homes[k], h, k).start()

    @pl.loop(0, n_piece)
    def _(t):
        p_cp(t).wait_send()
        y_cp(t).wait_send()
        f_cp(t).wait_send()

        @pl.when(is_mid)
        def _():
            x1_cp(t).wait_send()
            t1_cp(t).wait_send()
            x2_cp(t).wait_send()
            t2_cp(t).wait_send()

        @pl.when(is_end)
        def _():
            e1_cp(t).wait_send()
            e2_cp(t).wait_send()

    for h in range(N_HALF):
        for k in range(4):
            leave(homes[k], h, k).wait()


def layer(o, ml, hidden, w_o, w_gate, w_up, w_down, mlp_norm):
    n_steps, n_batch, width = hidden.shape
    n_half = n_batch // N_HALF
    n_col = width // N_COL
    n_piece = N_COL * N_HALF
    vm = pl.BlockSpec(memory_space=pltpu.VMEM)
    anyspec = pl.BlockSpec(memory_space=pltpu.HBM)
    f32, bf16 = jnp.float32, jnp.bfloat16
    piece = pltpu.VMEM((n_piece, n_half, n_col), f32)
    dma = pltpu.SemaphoreType.DMA
    return pl.pallas_call(
        layer_kernel,
        name='layer',
        out_shape=jax.ShapeDtypeStruct(hidden.shape, bf16),
        in_specs=[anyspec] * 8,
        out_specs=anyspec,
        scratch_shapes=[
            pltpu.VMEM((16, n_batch, HEAD), f32),
            pltpu.VMEM((4, n_batch, HEAD), f32),
            pltpu.VMEM((width // HEAD, HEAD), bf16),
            pltpu.VMEM(hidden.shape, bf16),
            pltpu.VMEM((2, 4, n_batch, HEAD), f32),
            pltpu.VMEM((2, n_batch, HEAD), f32),
            pltpu.VMEM((N_HALF, 4, n_half, HEAD), f32),
            pltpu.VMEM((N_HALF, n_half, HEAD), f32),
            pltpu.VMEM((N_HALF, 4, n_half, HEAD), f32),
            pltpu.VMEM((N_HALF, n_half, HEAD), f32),
            pltpu.VMEM((N_HALF, 4, n_half, HEAD), f32),
            pltpu.VMEM((N_HALF, n_half, HEAD), f32),
            pltpu.VMEM((N_HALF, n_half, 4 * HEAD), bf16),
            pltpu.VMEM((n_batch, width), bf16),
            pltpu.VMEM(w_o.shape, bf16),
            pltpu.VMEM(w_gate.shape, bf16),
            pltpu.VMEM(w_up.shape, bf16),
            pltpu.VMEM(w_down.shape, bf16),
            piece, piece, piece, piece,
            pltpu.VMEM((n_half, width), bf16),
            pltpu.VMEM((n_half, w_gate.shape[1]), bf16),
            piece, piece, piece, piece, piece, piece, piece,
            dma((7,)), dma((4 * N_HALF,)), dma((4,)), dma((4,)), dma((4,)), dma((2 * N_HALF,)), dma((2 * N_HALF,)),
        ] + [dma((n_piece,))] * 18,
        compiler_params=pltpu.CompilerParams(collective_id=0, has_side_effects=True, vmem_limit_bytes=67043328),
        cost_estimate=pl.CostEstimate(flops=2 * 10 ** 9, bytes_accessed=30 * 10 ** 6, transcendentals=10 ** 6),
    )(o.reshape(16, n_batch, HEAD), ml, hidden, w_o, w_gate, w_up, w_down, mlp_norm.reshape(-1, HEAD))


def emit_kernel(src, dst, buf, in_sem, out_sem):
    n = buf.shape[0]
    ins = [pltpu.make_async_copy(src.at[j], buf.at[j], in_sem.at[j]) for j in range(n)]
    outs = [pltpu.make_async_copy(buf.at[j], dst.at[j], out_sem.at[j]) for j in range(n)]
    for cp in ins:
        cp.start()
    for j in range(n):
        ins[j].wait()
        outs[j].start()
    for cp in outs:
        cp.wait()


def emit(x):
    n = x.shape[0]
    anyspec = pl.BlockSpec(memory_space=pltpu.HBM)
    return pl.pallas_call(
        emit_kernel,
        name='emit',
        out_shape=jax.ShapeDtypeStruct(x.shape, x.dtype),
        in_specs=[anyspec],
        out_specs=anyspec,
        scratch_shapes=[pltpu.VMEM(x.shape, x.dtype), pltpu.SemaphoreType.DMA((n,)), pltpu.SemaphoreType.DMA((n,))],
        compiler_params=pltpu.CompilerParams(vmem_limit_bytes=67043328),
        cost_estimate=pl.CostEstimate(flops=0, bytes_accessed=4 * 10 ** 6, transcendentals=0),
    )(x)


def solution(mesh):
    cache_spec = P('dp', 'sp', 'tp', None)
    col_spec = P(None, 'tp')
    row_spec = P('tp', None)
    in_specs = (P(None, 'dp', None), P('dp'), cache_spec, cache_spec, col_spec, col_spec, col_spec, row_spec,
                col_spec, col_spec, row_spec, P(), P(), P(), P())
    out_specs = (P(None, 'dp', None), cache_spec, cache_spec)

    def shard_body(hidden, start_pos, k_cache, v_cache, w_q, w_k, w_v, w_o, w_gate, w_up, w_down, attn_norm, mlp_norm, q_gain, k_gain):
        flat = (k_cache.shape[0], k_cache.shape[1] * k_cache.shape[2], k_cache.shape[3])
        o, ml, k_out, v_out = attend(start_pos, hidden, w_q, w_k, w_v, k_cache.reshape(flat), v_cache.reshape(flat), attn_norm, q_gain, k_gain)
        out = layer(o, ml, hidden, w_o, w_gate, w_up, w_down, mlp_norm)
        return emit(out), k_out.reshape(k_cache.shape), v_out.reshape(v_cache.shape)

    return jax.shard_map(shard_body, mesh=mesh, in_specs=in_specs, out_specs=out_specs, check_vma=False)
```

```python
import functools
import jax
import jax.numpy as jnp
import numpy as np
from jax import lax
from jax.experimental import pallas as pl
from jax.experimental.pallas import tpu as pltpu
from jax.sharding import PartitionSpec as P

ROPE_BASE = 1000000.0
NORM_EPS = 1e-06
NEG_BIG = -3e38
HEAD = 128
CHUNK = 8


def gain_row(ref):
    g = ref[...].astype(jnp.float32)
    return jnp.concatenate([g[j:j + 1] for j in range(g.shape[0])], axis=1)


def attend_kernel(start_hbm, hid_hbm, wq_hbm, wk_hbm, wv_hbm, kc_hbm, vc_hbm, an_hbm, qg_hbm, kg_hbm, freq_hbm,
                  o_hbm, ml_hbm, ko_hbm, vo_hbm,
                  start_ref, an_ref, qg_ref, kg_ref, freq_ref, o_ref, ml_ref, s_sem, o_sem,
                  hid, wq, wk, wv, kbuf, vbuf, nrm, raw, q_s, k_s, v_s, pos_s, ml_s, key_s, sc_s, pr_s,
                  w_sem, h_sem, kin_sem, vin_sem, kout_sem, vout_sem):
    n_steps, n_batch, width = hid.shape
    rows = kbuf.shape[1]
    seq_blk = rows // 2
    n_chunk = n_batch // CHUNK
    n_q = wq.shape[1] // HEAD
    n_kv = wk.shape[1] // HEAD
    blk_start = lax.axis_index('sp') * seq_blk
    scale = HEAD ** -0.5

    small = [pltpu.make_async_copy(a, b, s_sem.at[j]) for j, (a, b) in enumerate((
        (start_hbm, start_ref), (freq_hbm, freq_ref), (an_hbm, an_ref), (qg_hbm, qg_ref), (kg_hbm, kg_ref)))]
    hid_cp = pltpu.make_async_copy(hid_hbm, hid, h_sem)
    for cp in small[:2] + [hid_cp] + small[2:]:
        cp.start()
    w_cps = [pltpu.make_async_copy(a, b, w_sem.at[j]) for j, (a, b) in enumerate(((wq_hbm, wq), (wk_hbm, wk), (wv_hbm, wv)))]
    for cp in w_cps:
        cp.start()

    def kv_in(c):
        sl = pl.ds(c * CHUNK, CHUNK)
        return (pltpu.make_async_copy(kc_hbm.at[sl], kbuf.at[sl], kin_sem.at[c]),
                pltpu.make_async_copy(vc_hbm.at[sl], vbuf.at[sl], vin_sem.at[c]))

    def kv_out(c):
        sl = pl.ds(c * CHUNK, CHUNK)
        return (pltpu.make_async_copy(kbuf.at[sl], ko_hbm.at[sl], kout_sem.at[c]),
                pltpu.make_async_copy(vbuf.at[sl], vo_hbm.at[sl], vout_sem.at[c]))

    @pl.loop(0, n_chunk)
    def _(c):
        a, b = kv_in(c)
        a.start()
        b.start()

    for cp in small:
        cp.wait()

    @pl.loop(0, n_batch)
    def _(b):
        pos_s[pl.ds(b, 1), :] = jnp.full((1, HEAD), start_ref[b].astype(jnp.float32), jnp.float32)

    freq = freq_ref[0:1, :]
    sign = freq_ref[1:2, :]
    ang = pos_s[...] * freq
    cos0 = jnp.cos(ang)
    sin0 = jnp.sin(ang)

    r_id = lax.broadcasted_iota(jnp.int32, (16, rows), 0)
    c_id = lax.broadcasted_iota(jnp.int32, (16, rows), 1)
    same = ((r_id % 4) // 2) == (c_id % 2)
    key_s[...] = jnp.where(same, c_id // 2 - r_id // 4, 1 << 20)

    hid_cp.wait()
    gain = gain_row(an_ref)
    for i in range(n_steps):
        for h in range(0, n_batch, 32):
            x = hid[i, h:h + 32, :].astype(jnp.float32)
            inv = lax.rsqrt(jnp.mean(x * x, axis=-1, keepdims=True) + NORM_EPS)
            nrm[i * n_batch + h:i * n_batch + h + 32, :] = (x * inv * gain).astype(jnp.bfloat16)

    def rope(x, g, cos, sin):
        inv = lax.rsqrt(jnp.mean(x * x, axis=-1, keepdims=True) + NORM_EPS)
        y = x * inv * g
        return y * cos + pltpu.roll(y, HEAD // 2, 1) * sin

    tabs = []
    for i in range(n_steps):
        if i == 0:
            c, s = cos0, sin0
        else:
            ci, si = jnp.cos(freq * float(i)), jnp.sin(freq * float(i))
            c, s = cos0 * ci - sin0 * si, sin0 * ci + cos0 * si
        pos_s_c, pos_s_s = c, s * sign
        tabs.append((pos_s_c, pos_s_s))

    for cp in w_cps:
        cp.wait()
    qg = qg_ref[...].astype(jnp.float32)
    kg = kg_ref[...].astype(jnp.float32)
    nq = n_q * HEAD
    nk = n_kv * HEAD
    raw[:, :nq] = jnp.dot(nrm[...], wq[...], preferred_element_type=jnp.float32)
    raw[:, nq:nq + nk] = jnp.dot(nrm[...], wk[...], preferred_element_type=jnp.float32)
    raw[:, nq + nk:] = jnp.dot(nrm[...], wv[...], preferred_element_type=jnp.float32)
    for i in range(n_steps):
        rs = slice(i * n_batch, (i + 1) * n_batch)
        cos, sin = tabs[i]
        for h in range(n_q):
            q_s[pl.ds(i * n_q + h, n_batch, stride=n_steps * n_q), :] = rope(raw[rs, h * HEAD:(h + 1) * HEAD], qg, cos, sin)
        for h in range(n_kv):
            k_s[pl.ds(i * n_kv + h, n_batch, stride=n_steps * n_kv), :] = rope(
                raw[rs, nq + h * HEAD:nq + (h + 1) * HEAD], kg, cos, sin)
            v_s[pl.ds(i * n_kv + h, n_batch, stride=n_steps * n_kv), :] = raw[rs, nq + nk + h * HEAD:nq + nk + (h + 1) * HEAD]

    row32 = lax.broadcasted_iota(jnp.int32, (32, HEAD), 0)
    eye_r = lax.broadcasted_iota(jnp.int32, (16, HEAD), 0)
    eye_c = lax.broadcasted_iota(jnp.int32, (16, HEAD), 1)
    eye_m = eye_r == eye_c
    eye_l = eye_r + 16 == eye_c
    zero24 = jnp.zeros((24, HEAD), jnp.float32)

    @pl.loop(0, n_chunk)
    def _(c):
        a, b = kv_in(c)
        a.wait()
        b.wait()
        lps = []
        for u in range(CHUNK):
            bb = c * CHUNK + u
            lp = start_ref[bb] - blk_start
            lps.append(lp)
            base = jnp.clip((lp // 8) * 8, 0, seq_blk - 16)
            rel = (lp - base) * 2
            shift = jnp.bitwise_and(rel, 31)
            hit = (row32 >= rel) & (row32 < rel + 8)
            win = pl.ds(pl.multiple_of(base * 2, 16), 32)
            for src, dst in ((k_s, kbuf), (v_s, vbuf)):
                new = src[pl.ds(pl.multiple_of(bb * 8, 8), 8), :]
                new = pltpu.roll(jnp.concatenate([new, zero24], axis=0), shift, 0)
                old = dst[bb, win, :].astype(jnp.float32)
                dst[bb, win, :] = jnp.where(hit, new, old).astype(jnp.bfloat16)
        for u in range(CHUNK):
            bb = c * CHUNK + u
            q = q_s[pl.ds(pl.multiple_of(bb * 16, 16), 16), :].astype(jnp.bfloat16)
            sc_s[u] = lax.dot_general(q, kbuf[bb], (((1,), (1,)), ((), ())), preferred_element_type=jnp.float32)
        tops = []
        for u in range(CHUNK):
            s = jnp.where(key_s[...] <= lps[u], sc_s[u] * scale, NEG_BIG)
            sc_s[u] = s
            tops.append(jnp.maximum(jnp.max(s, axis=-1, keepdims=True), 0.5 * NEG_BIG))
        sums = []
        for u in range(CHUNK):
            p = jnp.exp(sc_s[u] - tops[u])
            sums.append(jnp.sum(p, axis=-1, keepdims=True))
            pr_s[u] = p.astype(jnp.bfloat16)
        for u in range(CHUNK):
            bb = c * CHUNK + u
            o_ref[pl.ds(bb, 16, stride=n_batch), :] = jnp.dot(pr_s[u], vbuf[bb], preferred_element_type=jnp.float32)
        for u in range(CHUNK):
            ml = jnp.where(eye_m, tops[u], 0.0) + jnp.where(eye_l, sums[u], 0.0)
            ml_s[pl.ds(c * CHUNK + u, 1), :] = jnp.sum(ml, axis=0, keepdims=True)
        a, b = kv_out(c)
        a.start()
        b.start()

    for i in range(n_steps):
        ml = ml_s[...]
        ml_ref[i] = ml if i == 0 else pltpu.roll(ml, HEAD - 4 * i, 1)
    outs = [pltpu.make_async_copy(o_ref, o_hbm, o_sem.at[0]), pltpu.make_async_copy(ml_ref, ml_hbm, o_sem.at[1])]
    for cp in outs:
        cp.start()

    @pl.loop(0, n_chunk)
    def _(c):
        a, b = kv_out(c)
        a.wait()
        b.wait()

    for cp in outs:
        cp.wait()


def attend(start_pos, hidden, w_q, w_k, w_v, k_cache, v_cache, attn_norm, q_gain, k_gain):
    n_steps, n_batch, width = hidden.shape
    rows = k_cache.shape[1]
    n_chunk = n_batch // CHUNK
    nq, nk = w_q.shape[1], w_k.shape[1]
    half = HEAD // 2
    f = ROPE_BASE ** (-(np.arange(half, dtype=np.float64) * (2.0 / HEAD)))
    freq = np.stack([np.concatenate([f, f]), np.concatenate([-np.ones(half), np.ones(half)])]).astype(np.float32)
    anyspec = pl.BlockSpec(memory_space=pltpu.HBM)
    return pl.pallas_call(
        attend_kernel,
        name='attend',
        out_shape=(jax.ShapeDtypeStruct((16 * n_batch, HEAD), jnp.float32),
                   jax.ShapeDtypeStruct((n_steps, n_batch, HEAD), jnp.float32),
                   jax.ShapeDtypeStruct(k_cache.shape, jnp.bfloat16),
                   jax.ShapeDtypeStruct(v_cache.shape, jnp.bfloat16)),
        in_specs=[anyspec] * 11,
        out_specs=(anyspec,) * 4,
        scratch_shapes=[
            pltpu.SMEM(start_pos.shape, jnp.int32),
            pltpu.VMEM((width // HEAD, HEAD), jnp.bfloat16),
            pltpu.VMEM((1, HEAD), jnp.bfloat16),
            pltpu.VMEM((1, HEAD), jnp.bfloat16),
            pltpu.VMEM((2, HEAD), jnp.float32),
            pltpu.VMEM((16 * n_batch, HEAD), jnp.float32),
            pltpu.VMEM((n_steps, n_batch, HEAD), jnp.float32),
            pltpu.SemaphoreType.DMA((5,)),
            pltpu.SemaphoreType.DMA((2,)),
            pltpu.VMEM(hidden.shape, jnp.bfloat16),
            pltpu.VMEM(w_q.shape, jnp.bfloat16),
            pltpu.VMEM(w_k.shape, jnp.bfloat16),
            pltpu.VMEM(w_v.shape, jnp.bfloat16),
            pltpu.VMEM(k_cache.shape, jnp.bfloat16),
            pltpu.VMEM(v_cache.shape, jnp.bfloat16),
            pltpu.VMEM((n_steps * n_batch, width), jnp.bfloat16),
            pltpu.VMEM((n_steps * n_batch, nq + 2 * nk), jnp.float32),
            pltpu.VMEM((n_batch * 16, HEAD), jnp.float32),
            pltpu.VMEM((n_batch * 8, HEAD), jnp.float32),
            pltpu.VMEM((n_batch * 8, HEAD), jnp.float32),
            pltpu.VMEM((n_batch, HEAD), jnp.float32),
            pltpu.VMEM((n_batch, HEAD), jnp.float32),
            pltpu.VMEM((16, rows), jnp.int32),
            pltpu.VMEM((CHUNK, 16, rows), jnp.float32),
            pltpu.VMEM((CHUNK, 16, rows), jnp.bfloat16),
            pltpu.SemaphoreType.DMA((3,)),
            pltpu.SemaphoreType.DMA,
            pltpu.SemaphoreType.DMA((n_chunk,)),
            pltpu.SemaphoreType.DMA((n_chunk,)),
            pltpu.SemaphoreType.DMA((n_chunk,)),
            pltpu.SemaphoreType.DMA((n_chunk,)),
        ],
        compiler_params=pltpu.CompilerParams(vmem_limit_bytes=67043328),
        cost_estimate=pl.CostEstimate(flops=2 * 10 ** 9, bytes_accessed=40 * 10 ** 6, transcendentals=10 ** 6),
    )(start_pos, hidden, w_q, w_k, w_v, k_cache, v_cache, attn_norm.reshape(-1, HEAD), q_gain.reshape(1, -1), k_gain.reshape(1, -1), jnp.asarray(freq))


N_COL = 4
N_HALF = 4
LAG = 5
LAG_Y = 8
TILES = 2
SERVE = 2


def layer_kernel(o_hbm, ml_hbm, hid_hbm, wo_hbm, wg_hbm, wu_hbm, wd_hbm, mn_hbm, out_hbm,
                 o_own, ml_own, mn_ref, out_ref, oa, mla, om, mlm, oy, mly, own, ml_mine, attn, hid, wo, wg, wu, wd,
                 p1, e1, x1, r1, m_s, act, p2, e2, x2, ob, yb, pb, pf,
                 ld_sem, out_sem, w_sem, a1_snd, a1_rcv, a2_snd, a2_rcv, es1, er1, xs1, xr1, ts1, tr1,
                 es2, er2, xs2, xr2, ts2, tr2, ps, pr, ys, yr, fs, fr):
    n_steps, n_batch, width = hid_hbm.shape
    n_half = n_batch // N_HALF
    n_col = width // N_COL
    n_piece = N_COL * N_HALF
    tp = lax.axis_index('tp')
    sp = lax.axis_index('sp')
    core = sp % 2
    row = sp // 2
    partner = {'sp': row * 2 + 1 - core}
    across = {'sp': (1 - row) * 2 + core}
    is_mid = (tp % 3) != 0
    is_end = (tp % 3) == 0
    to_mid = {'tp': (tp + 3) // 3}
    to_end = {'tp': (tp - 1) * 3}
    to_other = {'tp': 3 - tp}
    mesh_id = pl.DeviceIdType.MESH

    def remote(src, dst, ssem, rsem, dev):
        return pltpu.make_async_remote_copy(src_ref=src, dst_ref=dst, send_sem=ssem, recv_sem=rsem, device_id=dev, device_id_type=mesh_id)

    barrier = pltpu.get_barrier_semaphore()
    for dev in (partner, across):
        pl.semaphore_signal(barrier, inc=1, device_id=dev, device_id_type=mesh_id)

    @pl.when(is_mid)
    def _():
        pl.semaphore_signal(barrier, inc=1, device_id=to_end, device_id_type=mesh_id)
        pl.semaphore_signal(barrier, inc=1, device_id=to_other, device_id_type=mesh_id)

    @pl.when(is_end)
    def _():
        pl.semaphore_signal(barrier, inc=1, device_id=to_mid, device_id_type=mesh_id)

    send_to = 1 - core
    o_cps, ml_cps = [], []
    for q, step in enumerate(((1 - row) * 2 + send_to, row * 2 + send_to, (1 - row) * 2 + core, row * 2 + core)):
        o_cps.append(pltpu.make_async_copy(o_hbm.at[pl.ds(step * 4, 4)], o_own.at[pl.ds(step * 4, 4)], ld_sem.at[q]))
    ml_cp = pltpu.make_async_copy(ml_hbm, ml_own, ld_sem.at[4])
    hid_cp = pltpu.make_async_copy(hid_hbm.at[sp], hid, ld_sem.at[5])
    mn_cp = pltpu.make_async_copy(mn_hbm, mn_ref, ld_sem.at[6])
    lds = [ml_cp] + o_cps + [hid_cp, mn_cp]
    wts = [pltpu.make_async_copy(a, b, w_sem.at[j]) for j, (a, b) in enumerate(((wo_hbm, wo), (wg_hbm, wg), (wu_hbm, wu), (wd_hbm, wd)))]
    for cp in lds:
        cp.start()

    @pl.when(is_mid)
    def _():
        pl.semaphore_wait(barrier, 4)

    @pl.when(is_end)
    def _():
        pl.semaphore_wait(barrier, 3)

    ml_cp.wait()
    a1 = []
    for q, jy in enumerate((1 - row, row)):
        step = jy * 2 + 1 - core
        o_cps[q].wait()
        a1.append((remote(ml_own.at[step], mla.at[q], a1_snd.at[2 * q], a1_rcv.at[2 * q], partner),
                   remote(o_own.at[pl.ds(step * 4, 4)], oa.at[q], a1_snd.at[2 * q + 1], a1_rcv.at[2 * q + 1], partner)))
        for cp in a1[-1]:
            cp.start()

    lane = lax.broadcasted_iota(jnp.int32, (n_half, HEAD), 1)

    def weigh(ma, mb):
        top = jnp.maximum(ma, mb)
        wa, wb = jnp.exp(ma - top), jnp.exp(mb - top)
        tot = pltpu.roll(ma, HEAD - 16, 1) * wa + pltpu.roll(mb, HEAD - 16, 1) * wb
        return top, wa, wb, tot

    def merge_core(q, step, dst, mldst, send=None):
        for cp in a1[q]:
            cp.wait()
        for h in range(N_HALF):
            rs = pl.ds(h * n_half, n_half)
            top, wa, wb, tot = weigh(ml_own[step, rs, :], mla[q, rs, :])
            mldst[h] = jnp.where(lane < 16, top, pltpu.roll(tot, 16, 1))
            for k in range(4):
                dst[h, k] = o_own[step * 4 + k, rs, :] * wa[:, k:k + 1] + oa[q, k, rs, :] * wb[:, k:k + 1]
            if send is not None:
                for cp in send[h]:
                    cp.start()

    for cp in lds[3:]:
        cp.wait()
    a2 = []
    for h in range(N_HALF):
        a2.append((remote(mlm.at[h], mly.at[h], a2_snd.at[2 * h], a2_rcv.at[2 * h], across),
                   remote(om.at[h], oy.at[h], a2_snd.at[2 * h + 1], a2_rcv.at[2 * h + 1], across)))
    merge_core(0, (1 - row) * 2 + core, om, mlm, a2)
    for cp in wts:
        cp.start()
    merge_core(1, row * 2 + core, own, ml_mine)
    wts[0].wait()

    e1_cp = lambda t: remote(p1.at[t], e1.at[t], es1.at[t], er1.at[t], to_mid)
    x1_cp = lambda t: remote(p1.at[t], x1.at[t], xs1.at[t], xr1.at[t], to_other)
    t1_cp = lambda t: remote(r1.at[t], r1.at[t], ts1.at[t], tr1.at[t], to_end)
    e2_cp = lambda t: remote(p2.at[t], e2.at[t], es2.at[t], er2.at[t], to_mid)
    x2_cp = lambda t: remote(p2.at[t], x2.at[t], xs2.at[t], xr2.at[t], to_other)
    t2_cp = lambda t: remote(ob.at[t], ob.at[t], ts2.at[t], tr2.at[t], to_end)
    p_cp = lambda t: remote(ob.at[t], pb.at[t], ps.at[t], pr.at[t], partner)
    y_cp = lambda t: remote(ob.at[t], yb.at[t], ys.at[t], yr.at[t], across)
    f_cp = lambda t: remote(yb.at[t], pf.at[t], fs.at[t], fr.at[t], partner)

    def spread(h, lhs, w, dst, cp, after=None):
        wide = width // 2
        per = N_COL // 2
        for j in range(2):
            d = jnp.dot(lhs, w[:, j * wide:(j + 1) * wide], preferred_element_type=jnp.float32)
            for n in range(per):
                dst[h * N_COL + j * per + n] = d[:, n * n_col:(n + 1) * n_col]

            @pl.when(is_end)
            def _():
                @pl.loop(h * N_COL + j * per, h * N_COL + (j + 1) * per)
                def _(t):
                    cp(t).start()

            if after is not None:
                after(h)

    for h in range(N_HALF):
        for cp in a2[h]:
            cp.wait()
        _, wa, wb, tot = weigh(ml_mine[h], mly[h])
        inv = 1.0 / tot
        for k in range(4):
            val = (own[h, k] * wa[:, k:k + 1] + oy[h, k] * wb[:, k:k + 1]) * inv[:, k:k + 1]
            attn[h, :, k * HEAD:(k + 1) * HEAD] = val.astype(jnp.bfloat16)

        spread(h, attn[h], wo, p1, e1_cp)

    def sum_step(s, lag):
        @pl.when(s < n_piece)
        def _():
            e1_cp(s).wait_recv()
            p1[s] = p1[s] + e1[s]
            x1_cp(s).start()

        if lag is None:
            return

        @pl.when(s >= lag)
        def _():
            t = s - lag
            h = t // N_COL
            rs = pl.ds(pl.multiple_of(h * n_half, n_half), n_half)
            cs = pl.ds(pl.multiple_of((t - h * N_COL) * n_col, n_col), n_col)
            x1_cp(t).wait_recv()
            r = hid[rs, cs].astype(jnp.float32) + (p1[t] + x1[t])
            r1[t] = r.astype(jnp.bfloat16).astype(jnp.float32)
            t1_cp(t).start()

    def sum_steps(lo, hi, lag=LAG):
        @pl.when(is_mid)
        def _():
            pl.loop(lo, hi)(lambda s: sum_step(s, lag))

    def end_recv(lo, hi):
        @pl.when(is_end)
        def _():
            @pl.loop(lo, hi)
            def _(t):
                t1_cp(t).wait_recv()

    def share(t):
        y_cp(t).start()
        p_cp(t).start()

    def relay(t):
        y_cp(t).wait_recv()
        f_cp(t).start()

    def share_step(s):
        @pl.when(s < n_piece)
        def _():
            e2_cp(s).wait_recv()
            p2[s] = p2[s] + e2[s]
            x2_cp(s).start()

        @pl.when((s >= LAG) & (s < n_piece + LAG))
        def _():
            t = s - LAG
            x2_cp(t).wait_recv()
            o = r1[t] + (p2[t] + x2[t])
            ob[t] = o.astype(jnp.bfloat16).astype(jnp.float32)
            t2_cp(t).start()
            share(t)

        @pl.when(s >= LAG + LAG_Y)
        def _():
            relay(s - LAG - LAG_Y)


    def share_steps(lo, hi):
        @pl.when(is_mid)
        def _():
            pl.loop(lo, hi)(share_step)

    gain = gain_row(mn_ref)
    ffn = wg.shape[1]
    blk = ffn // TILES
    done = [0, 0]
    early = N_COL + LAG - 1

    def serve(h):
        for _ in range(SERVE):
            if done[0] < n_piece + LAG:
                sum_steps(done[0], done[0] + 1, None if done[0] == early else LAG)
                done[0] += 1
            elif done[1] < h * N_COL:
                share_steps(done[1], done[1] + 1)
                done[1] += 1

    for h in range(N_HALF):
        stop = early if h == 0 else max(done[0], (h + 1) * N_COL + LAG)
        if stop > done[0]:
            sum_steps(done[0], stop, LAG - 1 if h == 0 else LAG)
            done[0] = stop
        end_recv(h * N_COL, (h + 1) * N_COL)
        sq = jnp.zeros((n_half, 1), jnp.float32)
        for n in range(N_COL):
            r = r1[h * N_COL + n]
            sq = sq + jnp.sum(r * r, axis=-1, keepdims=True)
        inv = lax.rsqrt(sq / width + NORM_EPS)
        for n in range(N_COL):
            m_s[:, n * n_col:(n + 1) * n_col] = (r1[h * N_COL + n] * inv * gain[:, n * n_col:(n + 1) * n_col]).astype(jnp.bfloat16)
        if h == 0:
            wts[1].wait()
            wts[2].wait()
        for n in range(TILES):
            cs = slice(n * blk, (n + 1) * blk)
            g = jnp.dot(m_s[...], wg[:, cs], preferred_element_type=jnp.float32)
            u = jnp.dot(m_s[...], wu[:, cs], preferred_element_type=jnp.float32)
            act[:, cs] = (jax.nn.silu(g) * u).astype(jnp.bfloat16)
            serve(h)
        if h == 0:
            wts[3].wait()
        spread(h, act[...], wd, p2, e2_cp, serve)

    share_steps(done[1], n_piece + LAG + LAG_Y)

    @pl.when(is_end)
    def _():
        @pl.loop(0, n_piece + LAG_Y)
        def _(s):
            @pl.when(s < n_piece)
            def _():
                t2_cp(s).wait_recv()
                share(s)

            @pl.when(s >= LAG_Y)
            def _():
                relay(s - LAG_Y)

    def put(j, t, val):
        h = t // N_COL
        rs = pl.ds(pl.multiple_of(h * n_half, n_half), n_half)
        cs = pl.ds(pl.multiple_of((t - h * N_COL) * n_col, n_col), n_col)
        out_ref[j, rs, cs] = val.astype(jnp.bfloat16)

    def leave(j, h, k):
        rs = pl.ds(h * n_half, n_half)
        return pltpu.make_async_copy(out_ref.at[j, rs], out_hbm.at[j, rs], out_sem.at[h * 4 + k])

    homes = (sp, row * 2 + 1 - core, (1 - row) * 2 + core, (1 - row) * 2 + 1 - core)
    for h in range(N_HALF):
        @pl.loop(h * N_COL, (h + 1) * N_COL)
        def _(t):
            put(homes[0], t, ob[t])
            p_cp(t).wait_recv()
            put(homes[1], t, pb[t])
            put(homes[2], t, yb[t])
            f_cp(t).wait_recv()
            put(homes[3], t, pf[t])

        for k in range(4):
            leave(homes[k], h, k).start()

    @pl.loop(0, n_piece)
    def _(t):
        p_cp(t).wait_send()
        y_cp(t).wait_send()
        f_cp(t).wait_send()

        @pl.when(is_mid)
        def _():
            x1_cp(t).wait_send()
            t1_cp(t).wait_send()
            x2_cp(t).wait_send()
            t2_cp(t).wait_send()

        @pl.when(is_end)
        def _():
            e1_cp(t).wait_send()
            e2_cp(t).wait_send()

    for h in range(N_HALF):
        for k in range(4):
            leave(homes[k], h, k).wait()


def layer(o, ml, hidden, w_o, w_gate, w_up, w_down, mlp_norm):
    n_steps, n_batch, width = hidden.shape
    n_half = n_batch // N_HALF
    n_col = width // N_COL
    n_piece = N_COL * N_HALF
    vm = pl.BlockSpec(memory_space=pltpu.VMEM)
    anyspec = pl.BlockSpec(memory_space=pltpu.HBM)
    f32, bf16 = jnp.float32, jnp.bfloat16
    piece = pltpu.VMEM((n_piece, n_half, n_col), f32)
    dma = pltpu.SemaphoreType.DMA
    return pl.pallas_call(
        layer_kernel,
        name='layer',
        out_shape=jax.ShapeDtypeStruct(hidden.shape, bf16),
        in_specs=[anyspec] * 8,
        out_specs=anyspec,
        scratch_shapes=[
            pltpu.VMEM((16, n_batch, HEAD), f32),
            pltpu.VMEM((4, n_batch, HEAD), f32),
            pltpu.VMEM((width // HEAD, HEAD), bf16),
            pltpu.VMEM(hidden.shape, bf16),
            pltpu.VMEM((2, 4, n_batch, HEAD), f32),
            pltpu.VMEM((2, n_batch, HEAD), f32),
            pltpu.VMEM((N_HALF, 4, n_half, HEAD), f32),
            pltpu.VMEM((N_HALF, n_half, HEAD), f32),
            pltpu.VMEM((N_HALF, 4, n_half, HEAD), f32),
            pltpu.VMEM((N_HALF, n_half, HEAD), f32),
            pltpu.VMEM((N_HALF, 4, n_half, HEAD), f32),
            pltpu.VMEM((N_HALF, n_half, HEAD), f32),
            pltpu.VMEM((N_HALF, n_half, 4 * HEAD), bf16),
            pltpu.VMEM((n_batch, width), bf16),
            pltpu.VMEM(w_o.shape, bf16),
            pltpu.VMEM(w_gate.shape, bf16),
            pltpu.VMEM(w_up.shape, bf16),
            pltpu.VMEM(w_down.shape, bf16),
            piece, piece, piece, piece,
            pltpu.VMEM((n_half, width), bf16),
            pltpu.VMEM((n_half, w_gate.shape[1]), bf16),
            piece, piece, piece, piece, piece, piece, piece,
            dma((7,)), dma((4 * N_HALF,)), dma((4,)), dma((4,)), dma((4,)), dma((2 * N_HALF,)), dma((2 * N_HALF,)),
        ] + [dma((n_piece,))] * 18,
        compiler_params=pltpu.CompilerParams(collective_id=0, has_side_effects=True, vmem_limit_bytes=67043328),
        cost_estimate=pl.CostEstimate(flops=2 * 10 ** 9, bytes_accessed=30 * 10 ** 6, transcendentals=10 ** 6),
    )(o.reshape(16, n_batch, HEAD), ml, hidden, w_o, w_gate, w_up, w_down, mlp_norm.reshape(-1, HEAD))


def emit_kernel(src, dst, buf, in_sem, out_sem):
    n = buf.shape[0]
    ins = [pltpu.make_async_copy(src.at[j], buf.at[j], in_sem.at[j]) for j in range(n)]
    outs = [pltpu.make_async_copy(buf.at[j], dst.at[j], out_sem.at[j]) for j in range(n)]
    for cp in ins:
        cp.start()
    for j in range(n):
        ins[j].wait()
        outs[j].start()
    for cp in outs:
        cp.wait()


def emit(x):
    n = x.shape[0]
    anyspec = pl.BlockSpec(memory_space=pltpu.HBM)
    return pl.pallas_call(
        emit_kernel,
        name='emit',
        out_shape=jax.ShapeDtypeStruct(x.shape, x.dtype),
        in_specs=[anyspec],
        out_specs=anyspec,
        scratch_shapes=[pltpu.VMEM(x.shape, x.dtype), pltpu.SemaphoreType.DMA((n,)), pltpu.SemaphoreType.DMA((n,))],
        compiler_params=pltpu.CompilerParams(vmem_limit_bytes=67043328),
        cost_estimate=pl.CostEstimate(flops=0, bytes_accessed=4 * 10 ** 6, transcendentals=0),
    )(x)


def solution(mesh):
    cache_spec = P('dp', 'sp', 'tp', None)
    col_spec = P(None, 'tp')
    row_spec = P('tp', None)
    in_specs = (P(None, 'dp', None), P('dp'), cache_spec, cache_spec, col_spec, col_spec, col_spec, row_spec,
                col_spec, col_spec, row_spec, P(), P(), P(), P())
    out_specs = (P(None, 'dp', None), cache_spec, cache_spec)

    def shard_body(hidden, start_pos, k_cache, v_cache, w_q, w_k, w_v, w_o, w_gate, w_up, w_down, attn_norm, mlp_norm, q_gain, k_gain):
        flat = (k_cache.shape[0], k_cache.shape[1] * k_cache.shape[2], k_cache.shape[3])
        o, ml, k_out, v_out = attend(start_pos, hidden, w_q, w_k, w_v, k_cache.reshape(flat), v_cache.reshape(flat), attn_norm, q_gain, k_gain)
        out = layer(o, ml, hidden, w_o, w_gate, w_up, w_down, mlp_norm)
        return emit(out), k_out.reshape(k_cache.shape), v_out.reshape(v_cache.shape)

    return jax.shard_map(shard_body, mesh=mesh, in_specs=in_specs, out_specs=out_specs, check_vma=False)
```
